128 devices in a mesh: dp: 8 (over y, core), tensor: 16 (over x, z).
Axes of the slice: x: 4, y: 4, z: 4, core: 2. Of those that a mesh axis runs over, the one named last changes fastest.
Arguments:
- ref_hidden: bfloat16 [2304, 4608], P('dp', 'tensor'), may hold values from -6 to 6
- pol_hidden: bfloat16 [2304, 4608], P('dp', 'tensor'), may hold values from -6 to 6
- readout: bfloat16 [2304, 4608], P('dp', 'tensor'), may hold values from -0.019897461 to 0.019897461
- lengths: int32 [24], P('dp'), may hold values from 16 to 96, as said below
- pairing: int32 [24], replicated, may hold values from 0 to 23, each once
- pre_gain: float32 [4608], replicated, may hold values from 0.25 to 1.75
- post_gain: float32 [4608], replicated, may hold values from 0.25 to 1.75
- w_query: bfloat16 [4608, 4096], P('dp', 'tensor'), may hold values from -0.09375 to 0.09375
- w_key: bfloat16 [4608, 2048], P('dp', 'tensor'), may hold values from -3 to 3
- value_projection: bfloat16 [4608, 2048], P('dp', 'tensor'), may hold values from -0.09375 to 0.09375
- w_out: bfloat16 [4608, 4096], P('dp', 'tensor'), may hold values from -0.09375 to 0.09375
- a_query: bfloat16 [4608, 64], P('dp'), may hold values from -0.09375 to 0.09375
- a_value: bfloat16 [4608, 64], P('dp'), may hold values from -0.09375 to 0.09375
- query_second_factor: bfloat16 [64, 4096], P(None, 'tensor'), may hold values from -0.75 to 0.75
- value_second_factor: bfloat16 [64, 2048], P(None, 'tensor'), may hold values from -0.75 to 0.75
Outputs:
- policy_out: bfloat16 [2304, 4608], P('dp', 'tensor')
- reference_out: bfloat16 [2304, 4608], P('dp', 'tensor')
- dpo_loss: float32 [], replicated
- grad_hidden: bfloat16 [2304, 4608], P('dp', 'tensor')
- grad_a: float32 [4608, 128], P('dp')
- query_factor_gradient: float32 [64, 4096], P(None, 'tensor')
- value_factor_gradient: float32 [64, 2048], P(None, 'tensor')
The draws below stay inside these ranges and needn't reach their ends.
Inputs may be any that keep to these rules, and one draw needn't show every extreme that they name: `lengths`: every sequence has at least one valid token and some sequence is full. `pairing`: entries 2k and 2k + 1 name the chosen and the rejected sequence of pair k; every sequence appears once.
All inputs are finite; a program needn't handle non-finite values.
Results may differ from the reference program's by a relative error of at most 0.0233.
The reference program's roundings to bfloat16 on the way count: a program that leaves them out, or rounds other values in their place, can miss the bound.
Values may be sent and summed in bfloat16 or wider, within the bound.
A program may use at most 128 MiB of HBM per device.

```python
import jax
import jax.numpy as jnp
from jax import lax

MODEL_WIDTH = 4608
HQ = 32
KEY_VALUE_HEADS = 16
HEAD_SIZE = 128
ADAPTER_RANK = 64
SEQUENCE_SLOTS = 96
SEQUENCE_COUNT = 24
TOKEN_SLOTS = 2304
N_TENSOR = 16


def draw_lengths(key, part):
    first_key = jax.random.fold_in(key, 11)
    second_key = jax.random.fold_in(key, 12)
    lowest = max(1, SEQUENCE_SLOTS // 6)
    drawn = jax.random.randint(first_key, (SEQUENCE_COUNT,), lowest, SEQUENCE_SLOTS + 1)
    target_row = jax.random.randint(second_key, (), 0, SEQUENCE_COUNT)
    return jnp.where(jnp.arange(SEQUENCE_COUNT) == target_row, SEQUENCE_SLOTS, drawn).astype(jnp.int32)


def key_head_scales(scale_random_key, lowest, highest):
    uniform_sample = jax.random.uniform(scale_random_key, (KEY_VALUE_HEADS,), jnp.float32)
    spread_heads = jnp.exp(jnp.log(lowest) + uniform_sample * (jnp.log(highest) - jnp.log(lowest)))
    return (spread_heads[:, None] * jnp.ones((1, HEAD_SIZE), jnp.float32)).reshape(KEY_VALUE_HEADS * HEAD_SIZE)


def draw_w_key(key, part):
    scale_random_key = jax.random.fold_in(key, 21)
    entry_random_key = jax.random.fold_in(key, 22)
    spread_heads = key_head_scales(scale_random_key, 1.0, 8.0)
    table_entries = jax.random.truncated_normal(entry_random_key, -3.0, 3.0, (MODEL_WIDTH, KEY_VALUE_HEADS * HEAD_SIZE), jnp.float32)
    return (table_entries * spread_heads[None, :] * float(MODEL_WIDTH) ** (-0.5)).astype(jnp.bfloat16)


def steps_of(own_key, dims, cuts, least, high):
    level = 1.0
    for dim, parts in cuts:
        steps = jax.random.uniform(jax.random.fold_in(jax.random.fold_in(own_key, 6), dim), (parts,), jnp.float32, least / len(cuts), high / len(cuts))
        level = level * jnp.repeat(jnp.exp(steps), dims[dim] // parts).reshape((-1,) + (1,) * (len(dims) - 1 - dim))
    return level


def gaussian(key, extent, deviation, limit, split=(), kind=jnp.bfloat16):
    entries = deviation * jax.random.normal(key, extent, jnp.float32)
    if split:
        entries = entries * steps_of(key, extent, split, -0.22, 0.18)
    return jnp.clip(entries, -limit, limit).astype(kind)


def setup_inputs(seed: int = 0) -> dict:
    splits = jax.random.split(jax.random.key(seed), 16)
    return {
        "ref_hidden": gaussian(splits[0], (TOKEN_SLOTS, MODEL_WIDTH), 1.0, 6.0, ((0, 8), (1, 16))),
        "pol_hidden": gaussian(splits[1], (TOKEN_SLOTS, MODEL_WIDTH), 1.0, 6.0, ((0, 8), (1, 16))),
        "readout": gaussian(splits[2], (TOKEN_SLOTS, MODEL_WIDTH), 0.003, 0.019897461, ((0, 8), (1, 16))),
        "lengths": draw_lengths(jax.random.fold_in(splits[15], 71), 0),
        "pairing": jax.random.permutation(splits[4], SEQUENCE_COUNT).astype(jnp.int32),
        "pre_gain": jnp.clip(1.0 + 0.15 * jax.random.normal(splits[5], (MODEL_WIDTH,), jnp.float32), 0.25, 1.75),
        "post_gain": jnp.clip(1.0 + 0.15 * jax.random.normal(splits[6], (MODEL_WIDTH,), jnp.float32), 0.25, 1.75),
        "w_query": gaussian(splits[7], (MODEL_WIDTH, HQ * HEAD_SIZE), MODEL_WIDTH ** -0.5, 0.09375, ((0, 8), (1, 16))),
        "w_key": draw_w_key(jax.random.fold_in(splits[15], 71), 0),
        "value_projection": gaussian(splits[9], (MODEL_WIDTH, KEY_VALUE_HEADS * HEAD_SIZE), MODEL_WIDTH ** -0.5, 0.09375, ((0, 8), (1, 16))),
        "w_out": gaussian(splits[10], (MODEL_WIDTH, HQ * HEAD_SIZE), (HQ * HEAD_SIZE) ** -0.5, 0.09375, ((0, 8), (1, 16))),
        "a_query": gaussian(splits[11], (MODEL_WIDTH, ADAPTER_RANK), MODEL_WIDTH ** -0.5, 0.09375, ((0, 8),)),
        "a_value": gaussian(splits[12], (MODEL_WIDTH, ADAPTER_RANK), MODEL_WIDTH ** -0.5, 0.09375, ((0, 8),)),
        "query_second_factor": gaussian(splits[13], (ADAPTER_RANK, HQ * HEAD_SIZE), ADAPTER_RANK ** -0.5, 0.75, ((1, 16),)),
        "value_second_factor": gaussian(splits[14], (ADAPTER_RANK, KEY_VALUE_HEADS * HEAD_SIZE), ADAPTER_RANK ** -0.5, 0.75, ((1, 16),)),
    }


NORM_EPS = 1e-06
SOFT_CAP = 50.0
ADAPTER_SCALE = 0.5
DPO_BETA = 0.5
LOSS_SCALE = 256.0
ROPE_BASE = 10000.0

def query_scale():
    return float(MODEL_WIDTH // HQ) ** (-0.5)

def apply_rotation(value_rows, direction):
    length = value_rows.shape[1]
    head_depth = value_rows.shape[3]
    middle = head_depth // 2
    spacing = ROPE_BASE ** (-2.0 * jnp.arange(middle, dtype=jnp.float32) / head_depth)
    angles = jnp.arange(length, dtype=jnp.float32)[:, None] * spacing[None, :]
    cosine = jnp.cos(angles)[None, :, None, :]
    sine_part = direction * jnp.sin(angles)[None, :, None, :]
    leading = value_rows[..., :middle]
    trailing = value_rows[..., middle:]
    return jnp.concatenate([leading * cosine - trailing * sine_part, trailing * cosine + leading * sine_part], axis=-1)

def allowed_mask(lengths, length):
    places = jnp.arange(length)
    causal = places[None, :] <= places[:, None]
    living = places[None, :] < lengths[:, None]
    return causal[None, None, None, :, :] & living[:, None, None, None, :]

def attend(query_rows, rotated_keys, value_rows, lengths):
    seqs_here, length, q_heads, head_depth = query_rows.shape
    kv_heads = rotated_keys.shape[2]
    grouped_heads = query_rows.reshape(seqs_here, length, kv_heads, q_heads // kv_heads, head_depth)
    scores = jnp.einsum('sqkgd,spkd->skgqp', grouped_heads.astype(jnp.float32), rotated_keys.astype(jnp.float32)) * query_scale()
    capped = SOFT_CAP * jnp.tanh(scores / SOFT_CAP)
    allowed = allowed_mask(lengths, length)
    weights = jnp.where(allowed, jnp.exp(capped), 0.0)
    probabilities = weights / lax.optimization_barrier(jnp.sum(weights, axis=-1, keepdims=True))
    probs_low = probabilities.astype(jnp.bfloat16)
    mixed_out = jnp.einsum('skgqp,spkd->sqkgd', probs_low.astype(jnp.float32), value_rows.astype(jnp.float32))
    return (mixed_out.astype(jnp.bfloat16).reshape(seqs_here, length, q_heads, head_depth), probs_low, probabilities, capped)

def attend_back(grad_mixed, query_rows, rotated_keys, value_rows, probs_low, probabilities, capped):
    seqs_here, length, q_heads, head_depth = query_rows.shape
    kv_heads = rotated_keys.shape[2]
    shape_five = (seqs_here, length, kv_heads, q_heads // kv_heads, head_depth)
    grouped_heads = query_rows.reshape(shape_five).astype(jnp.float32)
    grad_grouped = grad_mixed.reshape(shape_five).astype(jnp.float32)
    grad_probs = jnp.einsum('sqkgd,spkd->skgqp', grad_grouped, value_rows.astype(jnp.float32))
    value_rows_gradient = jnp.einsum('skgqp,sqkgd->spkd', probs_low.astype(jnp.float32), grad_grouped)
    centered = grad_probs - lax.optimization_barrier(jnp.sum(grad_probs * probabilities, axis=-1, keepdims=True))
    grad_scores = (probabilities * centered * (1.0 - (capped / SOFT_CAP) ** 2) * query_scale()).astype(jnp.bfloat16)
    grad_scores = grad_scores.astype(jnp.float32)
    query_rows_gradient = jnp.einsum('skgqp,spkd->sqkgd', grad_scores, rotated_keys.astype(jnp.float32)).reshape(seqs_here, length, q_heads, head_depth)
    key_rows_gradient = jnp.einsum('skgqp,sqkgd->spkd', grad_scores, grouped_heads)
    return (query_rows_gradient, key_rows_gradient, value_rows_gradient)

def normalize(hidden, gain):
    wide_rows = hidden.astype(jnp.float32)
    pre_scale = lax.rsqrt(lax.optimization_barrier(jnp.sum(wide_rows * wide_rows, axis=1, keepdims=True)) / MODEL_WIDTH + NORM_EPS)
    return ((wide_rows * pre_scale * gain).astype(jnp.bfloat16), pre_scale)

def attention_layer(hidden, normed, lengths, post_gain, w_query, w_key, value_projection, w_out, adapters):
    query_rows = jnp.dot(normed, w_query, preferred_element_type=jnp.float32)
    keys_before_rotation = jnp.dot(normed, w_key, preferred_element_type=jnp.float32)
    value_rows = jnp.dot(normed, value_projection, preferred_element_type=jnp.float32)
    low_rank_update = None
    if adapters is not None:
        a_query, a_value, query_second_factor, value_second_factor = adapters
        low_rank_update = jnp.dot(normed, jnp.concatenate([a_query, a_value], axis=1), preferred_element_type=jnp.float32).astype(jnp.bfloat16)
        query_rows = query_rows + ADAPTER_SCALE * jnp.dot(low_rank_update[:, :ADAPTER_RANK], query_second_factor, preferred_element_type=jnp.float32)
        value_rows = value_rows + ADAPTER_SCALE * jnp.dot(low_rank_update[:, ADAPTER_RANK:], value_second_factor, preferred_element_type=jnp.float32)
    query_rows = apply_rotation(query_rows.reshape(SEQUENCE_COUNT, SEQUENCE_SLOTS, HQ, HEAD_SIZE), 1.0).astype(jnp.bfloat16)
    rotated_keys = apply_rotation(keys_before_rotation.reshape(SEQUENCE_COUNT, SEQUENCE_SLOTS, KEY_VALUE_HEADS, HEAD_SIZE), 1.0).astype(jnp.bfloat16)
    value_rows = value_rows.reshape(SEQUENCE_COUNT, SEQUENCE_SLOTS, KEY_VALUE_HEADS, HEAD_SIZE).astype(jnp.bfloat16)
    mixed_out, probs_low, probabilities, capped = attend(query_rows, rotated_keys, value_rows, lengths)
    flat_mixed = mixed_out.reshape(TOKEN_SLOTS, HQ * HEAD_SIZE)
    group_cols = HQ * HEAD_SIZE // N_TENSOR
    contract_cols = (((1,), (1,)), ((), ()))

    def add_group(index_g, running):
        start = (index_g * group_cols).astype(jnp.int32)
        columns = lax.dynamic_slice_in_dim(flat_mixed, start, group_cols, 1)
        w_columns = lax.dynamic_slice_in_dim(w_out, start, group_cols, 1)
        term_low = lax.dot_general(columns, w_columns, contract_cols, preferred_element_type=jnp.float32).astype(jnp.bfloat16)
        return running + lax.optimization_barrier(term_low).astype(jnp.float32)
    summed = lax.fori_loop(jnp.int32(0), jnp.int32(N_TENSOR), add_group, jnp.zeros((TOKEN_SLOTS, MODEL_WIDTH), jnp.float32))
    post_scale = lax.rsqrt(lax.optimization_barrier(jnp.sum(summed * summed, axis=1, keepdims=True)) / MODEL_WIDTH + NORM_EPS)
    result = hidden.astype(jnp.float32) + summed * post_scale * post_gain
    saved = (low_rank_update, query_rows, rotated_keys, value_rows, probs_low, probabilities, capped, summed, post_scale)
    return (result, saved)

def block_hook(grads, factor):
    grouped_heads = grads.astype(jnp.float32).reshape(TOKEN_SLOTS, N_TENSOR, -1)
    grouped_factors = factor.astype(jnp.float32).reshape(ADAPTER_RANK, N_TENSOR, -1)
    split_pieces = (ADAPTER_SCALE * jnp.einsum('fei,kei->fek', grouped_heads, grouped_factors)).astype(jnp.bfloat16)
    return lax.optimization_barrier(jnp.sum(lax.optimization_barrier(split_pieces).astype(jnp.float32), axis=1))

def reference(ref_hidden, pol_hidden, readout, lengths, pairing, pre_gain, post_gain, w_query, w_key, value_projection, w_out, a_query, a_value, query_second_factor, value_second_factor):
    ref_normed, ref_scale = normalize(ref_hidden, pre_gain)
    ref_result, ref_saved = attention_layer(ref_hidden, ref_normed, lengths, post_gain, w_query, w_key, value_projection, w_out, None)
    pol_normed, pol_scale = normalize(pol_hidden, pre_gain)
    pol_result, pol_saved = attention_layer(pol_hidden, pol_normed, lengths, post_gain, w_query, w_key, value_projection, w_out, (a_query, a_value, query_second_factor, value_second_factor))
    readout_wide = readout.astype(jnp.float32)
    living = (jnp.arange(SEQUENCE_SLOTS)[None, :] < lengths[:, None]).astype(jnp.float32)

    def sequence_score(result):
        return lax.optimization_barrier(jnp.sum(lax.optimization_barrier(jnp.sum(result * readout_wide, axis=1)).reshape(SEQUENCE_COUNT, SEQUENCE_SLOTS) * living, axis=1))
    ratios = sequence_score(pol_result) - sequence_score(ref_result)
    chosen = pairing[0::2]
    rejected = pairing[1::2]
    margins = DPO_BETA * (ratios[chosen] - ratios[rejected])
    dpo_loss = jnp.sum(jax.nn.softplus(-margins))
    pair_pull = DPO_BETA * LOSS_SCALE * jax.nn.sigmoid(-margins)
    coefficients = jnp.zeros((SEQUENCE_COUNT,), jnp.float32).at[chosen].add(-pair_pull).at[rejected].add(pair_pull)
    grad_result = (coefficients[:, None] * living).reshape(TOKEN_SLOTS, 1) * readout_wide
    low_rank_update, query_rows, rotated_keys, value_rows, probs_low, probabilities, capped, summed, post_scale = pol_saved
    post_dot = lax.optimization_barrier(jnp.sum(summed * post_gain * grad_result, axis=1, keepdims=True))
    grad_summed = post_scale * post_gain * grad_result - summed * post_scale ** 3 * post_dot / MODEL_WIDTH
    grad_wide = grad_summed.astype(jnp.bfloat16)
    grad_mixed = jnp.dot(grad_wide, w_out, preferred_element_type=jnp.float32).astype(jnp.bfloat16)
    grad_q_rot, rotated_key_gradient, value_head_gradient = attend_back(grad_mixed.reshape(SEQUENCE_COUNT, SEQUENCE_SLOTS, HQ, HEAD_SIZE), query_rows, rotated_keys, value_rows, probs_low, probabilities, capped)
    query_rows_gradient = apply_rotation(grad_q_rot, -1.0).reshape(TOKEN_SLOTS, HQ * HEAD_SIZE).astype(jnp.bfloat16)
    key_rows_gradient = apply_rotation(rotated_key_gradient, -1.0).reshape(TOKEN_SLOTS, KEY_VALUE_HEADS * HEAD_SIZE).astype(jnp.bfloat16)
    value_rows_gradient = value_head_gradient.reshape(TOKEN_SLOTS, KEY_VALUE_HEADS * HEAD_SIZE).astype(jnp.bfloat16)
    rows_contraction = (((0,), (0,)), ((), ()))
    contract_cols = (((1,), (1,)), ((), ()))
    query_factor_gradient = ADAPTER_SCALE * lax.dot_general(low_rank_update[:, :ADAPTER_RANK], query_rows_gradient, rows_contraction, preferred_element_type=jnp.float32)
    value_factor_gradient = ADAPTER_SCALE * lax.dot_general(low_rank_update[:, ADAPTER_RANK:], value_rows_gradient, rows_contraction, preferred_element_type=jnp.float32)
    adapter_grad = jnp.concatenate([block_hook(query_rows_gradient, query_second_factor), block_hook(value_rows_gradient, value_second_factor)], axis=1)
    grad_a = lax.dot_general(pol_normed.astype(jnp.float32), adapter_grad, rows_contraction, precision=lax.Precision.HIGHEST)
    a_both = jnp.concatenate([a_query, a_value], axis=1).astype(jnp.float32)
    grad_normed = lax.dot_general(query_rows_gradient, w_query, contract_cols, preferred_element_type=jnp.float32)
    grad_normed = grad_normed + lax.dot_general(key_rows_gradient, w_key, contract_cols, preferred_element_type=jnp.float32)
    grad_normed = grad_normed + lax.dot_general(value_rows_gradient, value_projection, contract_cols, preferred_element_type=jnp.float32)
    grad_normed = grad_normed + lax.dot_general(adapter_grad, a_both, contract_cols, precision=lax.Precision.HIGHEST)
    narrow = pol_hidden.astype(jnp.float32)
    pre_dot = lax.optimization_barrier(jnp.sum(narrow * pre_gain * grad_normed, axis=1, keepdims=True))
    grad_hidden = grad_result + pol_scale * pre_gain * grad_normed - narrow * pol_scale ** 3 * pre_dot / MODEL_WIDTH
    return (pol_result.astype(jnp.bfloat16), ref_result.astype(jnp.bfloat16), dpo_loss, grad_hidden.astype(jnp.bfloat16), grad_a, query_factor_gradient, value_factor_gradient)
```

```python
import jax
import jax.numpy as jnp
import numpy as np
from jax import lax
from jax.experimental import pallas as pl
from jax.experimental.pallas import tpu as pltpu
from jax.sharding import Mesh
from jax.sharding import PartitionSpec as P

DP = ("dp_0", "dp_1")
TENSOR = ("tensor_0", "tensor_1")
MESH = pl.DeviceIdType.MESH

WIDTH = 4608
TOK = 288
LENGTH = 96
HEAD = 128
RANK = 64
NORM_EPS = 1e-06
SOFT_CAP = 50.0
ADAPTER_SCALE = 0.5
DPO_BETA = 0.5
LOSS_SCALE = 256.0
ROPE_BASE = 10000.0
QUERY_SCALE = float(WIDTH // 32) ** (-0.5)

GROUP = 80
SHARD = 2 * TOK + GROUP
MAIN = 4096
RINGS = ((0, 1), (0, -1), (1, 1), (1, -1))

F32 = jnp.float32
BF16 = jnp.bfloat16
NT = (((1,), (1,)), ((), ()))
TN = (((0,), (0,)), ((), ()))


def dot(a, b, dims=(((1,), (0,)), ((), ())), precision=None):
    return lax.dot_general(a, b, dims, preferred_element_type=F32, precision=precision)


def aligned(start, multiple):
    return start if isinstance(start, int) else pl.multiple_of(start, multiple)


def back(position, hops, direction):
    return lax.rem(position - hops * direction + 8, 4)


def chunks_of(rows):
    tiles = rows // 16
    sizes = [16 * (tiles // 4 + (1 if k < tiles % 4 else 0)) for k in range(4)]
    return sizes, [sum(sizes[:k]) for k in range(4)]


class Ring:
    def __init__(self, rows, send, recv):
        self.rows = rows
        self.sizes, self.starts = chunks_of(rows)
        self.send, self.recv = send, recv
        self.at = (lax.axis_index("tensor_0"), lax.axis_index("tensor_1"))

    def place(self, k, first, second):
        primary, way = RINGS[k]
        a = back(self.at[primary], first, way)
        b = back(self.at[1 - primary], second, way)
        px, pz = (a, b) if primary == 0 else (b, a)
        return aligned((4 * px + pz) * self.rows + self.starts[k], 16)

    def next_on(self, k, secondary):
        primary, way = RINGS[k]
        axis = 1 - primary if secondary else primary
        return {TENSOR[axis]: back(self.at[axis], -1, way)}

    def remote(self, source, target, k, number, device):
        return pltpu.make_async_remote_copy(
            src_ref=source,
            dst_ref=target,
            send_sem=self.send.at[k, number],
            recv_sem=self.recv.at[k, number],
            device_id=device,
            device_id_type=MESH,
        )


class Gather(Ring):
    def __init__(self, buffer, rows, send, recv):
        super().__init__(rows, send, recv)
        self.buffer = buffer

    def piece(self, k, j, s):
        return self.buffer.at[pl.ds(self.place(k, j, s), self.sizes[k]), :]

    def number(self, secondary, j, s):
        return 3 + 3 * j + s if secondary else j

    def copy(self, k, secondary, j, s):
        piece = self.piece(k, j, s)
        return self.remote(piece, piece, k, self.number(secondary, j, s), self.next_on(k, secondary))

    def start(self, secondary, j, s):
        for k in range(4):
            self.copy(k, secondary, j, s).start()

    def wait(self, k, secondary, j, s):
        piece = self.piece(k, j, s + 1) if secondary else self.piece(k, j + 1, s)
        self.remote(piece, piece, k, self.number(secondary, j, s), self.next_on(k, secondary)).wait_recv()

    def wave(self, w):
        if w == 0:
            self.start(False, 0, 0)
            self.start(True, 0, 0)
            return
        if w <= 3:
            for k in range(4):
                self.wait(k, False, w - 1, 0)
                if w < 3:
                    self.copy(k, False, w, 0).start()
                self.copy(k, True, w, 0).start()
        for s in range(3):
            j = w - 1 - s
            if 0 <= j <= 3:
                for k in range(4):
                    self.wait(k, True, j, s)
                    if s < 2:
                        self.copy(k, True, j, s + 1).start()

    def drain(self):
        for k in range(4):
            for j in range(3):
                self.copy(k, False, j, 0).wait_send()
            for j in range(4):
                for s in range(3):
                    self.copy(k, True, j, s).wait_send()


class Scatter(Ring):
    def __init__(self, partial, landing, rows, send, recv):
        super().__init__(rows, send, recv)
        self.partial, self.landing = partial, landing

    def piece(self, k, first, second):
        return self.partial.at[pl.ds(self.place(k, first, second), self.sizes[k]), :]

    def slot(self, k, number):
        return self.landing.at[pl.ds(15 * self.starts[k] + number * self.sizes[k], self.sizes[k]), :]

    def outer(self, k, j, s):
        number = 3 * j + s
        return self.remote(self.piece(k, j + 1, s + 1), self.slot(k, number), k, number, self.next_on(k, True))

    def inner(self, k, s):
        return self.remote(self.piece(k, s + 1, 0), self.slot(k, 12 + s), k, 12 + s, self.next_on(k, False))

    def add(self, k, number, first, second):
        piece, slot = self.piece(k, first, second), self.slot(k, number)
        piece[...] = (piece[...].astype(F32) + slot[...].astype(F32)).astype(BF16)

    def begin(self):
        for j in range(4):
            for k in range(4):
                self.outer(k, j, 0).start()

    def run(self, result):
        for s in range(3):
            self.turn(s, result)

    def turn(self, s, result):
        for j in range(4):
            for k in range(4):
                self.outer(k, j, s).wait_recv()
                self.add(k, 3 * j + s, j + 1, s + 2)
                if s < 2:
                    self.outer(k, j, s + 1).start()
                    continue
                if j == 0:
                    self.inner(k, 0).start()
                    continue
                self.inner(k, j - 1).wait_recv()
                if j < 3:
                    self.add(k, 12 + j - 1, j + 1, 0)
                    self.inner(k, j).start()
                else:
                    own = self.piece(k, 0, 0)[...].astype(F32) + self.slot(k, 14)[...].astype(F32)
                    result[pl.ds(self.starts[k], self.sizes[k]), :] = own

    def drain(self):
        for k in range(4):
            for j in range(4):
                for s in range(3):
                    self.outer(k, j, s).wait_send()
            for s in range(3):
                self.inner(k, s).wait_send()


class Weights:
    def __init__(self, w_in, w_back, y_send, y_recv, d_send, d_recv):
        self.w_in, self.w_back = w_in, w_back
        self.sems = (y_send, y_recv, d_send, d_recv)
        self.y, self.core = lax.axis_index("dp_0"), lax.axis_index("dp_1")

    def block(self, hops, half, part, core):
        way = 1 - 2 * half
        tile = 2 * (2 * back(self.y, hops, way) + core) + half
        ref = self.w_in if part < 2 else self.w_back
        if part % 2 == 0:
            return ref.at[pl.ds(aligned(256 * tile, 256), 256), :]
        return ref.at[pl.ds(aligned(MAIN + 32 * tile, 32), 32), :]

    def round(self, s, half, part, arriving=False):
        ref = self.block(s + 1 if arriving else s, half, part, self.core)
        return pltpu.make_async_remote_copy(
            src_ref=ref,
            dst_ref=ref,
            send_sem=self.sems[0].at[half, s, part],
            recv_sem=self.sems[1].at[half, s, part],
            device_id={"dp_0": back(self.y, -1, 1 - 2 * half)},
            device_id_type=MESH,
        )

    def across(self, i, half, part, arriving=False):
        ref = self.block(i, half, part, 1 - self.core if arriving else self.core)
        return pltpu.make_async_remote_copy(
            src_ref=ref,
            dst_ref=ref,
            send_sem=self.sems[2].at[half, i, part],
            recv_sem=self.sems[3].at[half, i, part],
            device_id={"dp_1": 1 - self.core},
            device_id_type=MESH,
        )

    def step(self, s, parts):
        for half in range(2):
            for part in parts:
                if s > 0:
                    self.round(s - 1, half, part, True).wait_recv()
                if s < 3:
                    self.round(s, half, part).start()
                self.across(s, half, part).start()

    def arrive(self, parts):
        for half in range(2):
            for part in parts:
                for i in range(4):
                    self.across(i, half, part, True).wait_recv()

    def drain(self):
        for half in range(2):
            for part in range(4):
                for s in range(3):
                    self.round(s, half, part).wait_send()
                for i in range(4):
                    self.across(i, half, part).wait_send()


class Exchange:
    def __init__(self, buffer, rows, count, me, device_of, send, recv, source=None, spread=False):
        self.buffer, self.rows, self.count, self.me = buffer, rows, count, me
        self.device_of, self.send, self.recv = device_of, send, recv
        self.source = buffer if source is None else source
        self.spread = spread

    def slot(self, i):
        return self.buffer.at[pl.ds(aligned(i * self.rows, 8), self.rows), :]

    def copy(self, delta):
        peer = lax.rem(self.me + delta, self.count)
        origin = peer if self.spread else self.me
        return pltpu.make_async_remote_copy(
            src_ref=self.source.at[pl.ds(aligned(origin * self.rows, 8), self.rows), :],
            dst_ref=self.slot(self.me),
            send_sem=self.send.at[delta],
            recv_sem=self.recv.at[delta],
            device_id=self.device_of(peer),
            device_id_type=MESH,
        )

    def start(self):
        for delta in range(1, self.count):
            self.copy(delta).start()

    def wait(self):
        for delta in range(1, self.count):
            arrived = self.slot(lax.rem(self.me - delta + self.count, self.count))
            pltpu.make_async_remote_copy(
                src_ref=arrived,
                dst_ref=arrived,
                send_sem=self.send.at[delta],
                recv_sem=self.recv.at[delta],
                device_id=self.device_of(lax.rem(self.me + delta, self.count)),
                device_id_type=MESH,
            ).wait_recv()

    def total(self):
        value = self.buffer[0 : self.rows, :].astype(F32)
        for i in range(1, self.count):
            value = value + self.buffer[self.rows * i : self.rows * i + self.rows, :].astype(F32)
        return value

    def drain(self):
        for delta in range(1, self.count):
            self.copy(delta).wait_send()


def in_tensor(i):
    return {"tensor_0": lax.div(i, 4), "tensor_1": lax.rem(i, 4)}


def in_data(i):
    return {"dp_0": lax.div(i, 2), "dp_1": lax.rem(i, 2)}


def greet(peers):
    barrier = pltpu.get_barrier_semaphore()
    for peer in peers:
        pl.semaphore_signal(barrier, inc=1, device_id=peer, device_id_type=MESH)
    pl.semaphore_wait(barrier, len(peers))


def pack_tail(tail):
    last = jnp.concatenate([tail[240:288], jnp.zeros((32, 32), tail.dtype)], axis=0)
    return jnp.concatenate([tail[0:80], tail[80:160], tail[160:240], last], axis=1)


GROUPS = ((0, 80), (80, 80), (160, 80), (240, 48))


def unpack_features(buffer, rows, offset, target, row_offset):
    def main(t, carry):
        base = aligned(t * rows + offset, 16)
        for half in range(2):
            target[pl.ds(row_offset, TOK), pl.ds(aligned(256 * t + 128 * half, 128), 128)] = buffer[
                pl.ds(aligned(base + TOK * half, 16), TOK), :
            ]
        return carry

    lax.fori_loop(0, 16, main, 0)

    def tail(q, carry):
        tails = [
            buffer[pl.ds(aligned((4 * q + j) * rows + offset + 2 * TOK, 16), GROUP), :] for j in range(4)
        ]
        for g, (start, size) in enumerate(GROUPS):
            joined = jnp.concatenate([t[:size, 32 * g : 32 * g + 32] for t in tails], axis=1)
            target[pl.ds(row_offset + start, size), pl.ds(aligned(MAIN + 128 * q, 128), 128)] = joined
        return carry

    lax.fori_loop(0, 4, tail, 0)


def unpack_result(packed, offset, target):
    for half in range(2):
        target[:, 128 * half : 128 * half + 128] = packed[offset + TOK * half : offset + TOK * half + TOK, :]
    for g, (start, size) in enumerate(GROUPS):
        base = offset + 2 * TOK
        target[start : start + size, 256:288] = packed[base : base + size, 32 * g : 32 * g + 32]


def pack_hidden(hidden, buffer, base):
    for half in range(2):
        buffer[pl.ds(aligned(base + TOK * half, 16), TOK), :] = hidden[:, 128 * half : 128 * half + 128].astype(
            BF16
        )
    buffer[pl.ds(aligned(base + 2 * TOK, 16), GROUP), :] = pack_tail(hidden[:, 256:288]).astype(BF16)


def gain_tile(gain, c):
    if c < 32:
        return gain[c // 2 : c // 2 + 1, 128 * (c % 2) : 128 * (c % 2) + 128]
    return jnp.concatenate([gain[4 * (c - 32) + j : 4 * (c - 32) + j + 1, 256:288] for j in range(4)], axis=1)


def normalize(normed, scale_ref, gain_ref, models):
    def rows(i, carry):
        at = pl.ds(aligned(96 * i, 96), 96)
        squares = jnp.zeros((96, 128), F32)
        for c in range(36):
            x = normed[at, 128 * c : 128 * c + 128].astype(F32)
            squares = squares + x * x
        scale = lax.rsqrt(jnp.sum(squares, axis=1, keepdims=True) / WIDTH + NORM_EPS)
        scale_ref[at, :] = jnp.broadcast_to(scale, (96, 128))
        for c in range(36):
            x = normed[at, 128 * c : 128 * c + 128].astype(F32)
            normed[at, 128 * c : 128 * c + 128] = (x * scale * gain_tile(gain_ref, c)).astype(BF16)
        return carry

    lax.fori_loop(0, 3 * models, rows, 0)


def rope(x, cosine, sine):
    return x * cosine + pltpu.roll(x, 64, 1) * sine


def allowed_here(length):
    query = lax.broadcasted_iota(jnp.int32, (LENGTH, LENGTH), 0)
    key = lax.broadcasted_iota(jnp.int32, (LENGTH, LENGTH), 1)
    return (key <= query) & (key < length)


def columns_to_rows(scratch, columns):
    lane = lax.broadcasted_iota(jnp.int32, (TOK, 128), 1)
    table = jnp.zeros((TOK, 128), F32)
    for k, column in enumerate(columns):
        table = jnp.where(lane == k, column, table)
    scratch[0:TOK, :] = table
    scratch[TOK:384, :] = jnp.zeros((384 - TOK, 128), F32)
    return jnp.transpose(scratch[...])[0:8, :]


def rows_to_columns(scratch, rows):
    missing = 128 - sum(row.shape[0] for row in rows)
    filled = jnp.concatenate(list(rows) + [jnp.zeros((missing, 384), F32)], axis=0)
    scratch[...] = jnp.transpose(filled)


SCRATCH = {
    "hidden_buf": ((32 * SHARD, 128), BF16),
    "w_in": ((WIDTH, 640), BF16),
    "w_back": ((WIDTH, 256), BF16),
    "normed": ((2 * TOK, WIDTH), BF16),
    "scale": ((2 * TOK, 128), F32),
    "acc": ((2 * TOK, 640), F32),
    "linear": ((TOK, 640), F32),
    "low": ((TOK, 128), BF16),
    "heads": ((2 * TOK, 512), BF16),
    "mixed": ((2 * TOK, 256), BF16),
    "probs": ((2 * TOK, 256), F32),
    "capped": ((2 * TOK, 256), F32),
    "partial": ((32 * SHARD, 128), BF16),
    "landing": ((30 * SHARD, 128), BF16),
    "result": ((2 * SHARD, 128), F32),
    "summed": ((2, TOK, TOK), F32),
    "table": ((384, 128), F32),
    "stats": ((16 * 8, 384), F32),
    "scores": ((8 * 8, 128), F32),
    "grad_buf": ((16 * SHARD, 128), BF16),
    "grad_mixed": ((TOK, 256), F32),
    "grads": ((TOK, 640), BF16),
    "partial_back": ((16 * SHARD, 128), BF16),
    "landing_back": ((15 * SHARD, 128), BF16),
    "hooks": ((384, 128), F32),
    "hook_parts": ((384, 128), F32),
    "hook_whole": ((384, 128), F32),
    "stats_back": ((16 * 8, 384), F32),
    "factors": ((8 * 64, 384), BF16),
    "a_terms": ((WIDTH, 128), BF16),
    "a_across": ((4 * 576, 128), BF16),
    "a_pairs": ((4 * 576, 128), BF16),
    "a_round": ((4 * 576, 128), BF16),
}
SEMAPHORES = {
    "gather": (4, 15),
    "scatter": (4, 15),
    "gather_back": (4, 15),
    "scatter_back": (4, 15),
    "y": (2, 3, 4),
    "d": (2, 4, 4),
    "stats": (16,),
    "scores": (8,),
    "hooks": (16,),
    "hook_whole": (16,),
    "stats_back": (16,),
    "factors": (8,),
    "across": (4,),
    "round": (4,),
}


class Refs:
    pass


def step_body(*refs):
    names = INPUTS + OUTPUTS + list(SCRATCH)
    r = Refs()
    for name, ref in zip(names, refs):
        setattr(r, name, ref)
    sems = refs[len(names) :]
    send = dict(zip(SEMAPHORES, sems[0::2]))
    recv = dict(zip(SEMAPHORES, sems[1::2]))

    x, z = lax.axis_index("tensor_0"), lax.axis_index("tensor_1")
    y, core = lax.axis_index("dp_0"), lax.axis_index("dp_1")
    mine, rank = 4 * x + z, 2 * y + core
    base = mine * 2 * SHARD
    pack_hidden(r.ref_hidden[...], r.hidden_buf, base)
    pack_hidden(r.pol_hidden[...], r.hidden_buf, base + SHARD)
    for half in range(2):
        tile = 2 * rank + half
        for start, size, to in ((0, 256, 256 * tile), (256, 32, MAIN + 32 * tile)):
            here, there = pl.ds(288 * half + start, size), pl.ds(aligned(to, 32), size)
            r.w_in[there, 0:256] = r.w_query[here, :]
            r.w_in[there, 256:384] = r.w_key[here, :]
            r.w_in[there, 384:512] = r.w_value[here, :]
            r.w_in[there, 512:640] = jnp.concatenate([r.a_query[here, :], r.a_value[here, :]], axis=1)
            r.w_back[there, :] = r.w_out[here, :]
    greet(
        [in_tensor(lax.rem(mine + i, 16)) for i in range(1, 16)]
        + [in_data(lax.rem(rank + i, 8)) for i in range(1, 8)]
    )

    gather = Gather(r.hidden_buf, 2 * SHARD, send["gather"], recv["gather"])
    weights = Weights(r.w_in, r.w_back, send["y"], recv["y"], send["d"], recv["d"])
    gather.wave(0)
    weights.step(0, (0, 1))
    gather.wave(1)
    gather.wave(2)
    weights.step(1, (0, 1))
    gather.wave(3)
    gather.wave(4)
    weights.step(2, (0, 1))
    weights.step(0, (2, 3))
    gather.wave(5)
    gather.wave(6)
    unpack_features(r.hidden_buf, 2 * SHARD, 0, r.normed, 0)
    unpack_features(r.hidden_buf, 2 * SHARD, SHARD, r.normed, TOK)
    normalize(r.normed, r.scale, r.pre_gain, 2)
    weights.step(3, (0, 1))
    weights.arrive((0, 1))

    acc = r.acc
    acc[...] = jnp.zeros_like(acc)

    def project(i, carry):
        at = pl.ds(aligned(512 * i, 512), 512)
        acc[...] += dot(r.normed[:, at], r.w_in[at, :])
        return carry

    lax.fori_loop(0, 9, project, 0)
    weights.step(1, (2, 3))

    r.linear[...] = acc[TOK : 2 * TOK, :]
    r.low[...] = acc[TOK : 2 * TOK, 512:640].astype(BF16)
    query_factor = jnp.concatenate([r.b_query[...], jnp.zeros((RANK, 256), BF16)], axis=0)
    value_factor = jnp.concatenate([jnp.zeros((RANK, 128), BF16), r.b_value[...]], axis=0)
    acc[TOK : 2 * TOK, 0:256] += ADAPTER_SCALE * dot(r.low[...], query_factor)
    acc[TOK : 2 * TOK, 384:512] += ADAPTER_SCALE * dot(r.low[...], value_factor)

    def attend(i, carry):
        at = pl.ds(aligned(96 * i, 96), 96)
        cos, sin = r.cosine[...], r.sine[...]
        key = rope(acc[at, 256:384], cos, sin).astype(BF16)
        value = acc[at, 384:512].astype(BF16)
        allowed = allowed_here(r.lengths[lax.rem(i, 3)])
        r.heads[at, 256:384] = key
        r.heads[at, 384:512] = value
        for g in range(2):
            query = rope(acc[at, 128 * g : 128 * g + 128], cos, sin).astype(BF16)
            r.heads[at, 128 * g : 128 * g + 128] = query
            scores = dot(query, key, NT) * QUERY_SCALE
            cap = SOFT_CAP * jnp.tanh(scores / SOFT_CAP)
            weight = jnp.where(allowed, jnp.exp(cap), 0.0)
            prob = weight / jnp.sum(weight, axis=1, keepdims=True)
            r.probs[at, 128 * g : 128 * g + 96] = prob
            r.capped[at, 128 * g : 128 * g + 96] = cap
            r.mixed[at, 128 * g : 128 * g + 128] = dot(prob.astype(BF16), value).astype(BF16)
        return carry

    lax.fori_loop(0, 6, attend, 0)
    weights.step(2, (2, 3))
    weights.step(3, (2, 3))
    weights.arrive((2, 3))
    partial_products(r.mixed, r.w_back, r.partial, 2)

    scatter = Scatter(r.partial, r.landing, 2 * SHARD, send["scatter"], recv["scatter"])
    scatter.begin()
    scatter.run(r.result)
    for m in range(2):
        unpack_result(r.result, m * SHARD, r.summed.at[m])

    post_gain = r.post_gain[pl.ds(mine, 1), :]
    pre_gain = r.pre_gain[pl.ds(mine, 1), :]
    columns = [[], [], []]
    for m, hidden in enumerate((r.ref_hidden, r.pol_hidden)):
        summed, readout = r.summed[m], r.readout[...].astype(F32)
        columns[0].append(jnp.sum(summed * summed, axis=1, keepdims=True))
        columns[1].append(jnp.sum(summed * post_gain * readout, axis=1, keepdims=True))
        columns[2].append(jnp.sum(hidden[...].astype(F32) * readout, axis=1, keepdims=True))
    stats = Exchange(r.stats, 8, 16, mine, in_tensor, send["stats"], recv["stats"])
    r.stats[pl.ds(aligned(8 * mine, 8), 8), :] = columns_to_rows(r.table, sum(columns, []))
    stats.start()
    stats.wait()
    totals = stats.total()
    post_scale = lax.rsqrt(totals[0:2] / WIDTH + NORM_EPS)
    lane = lax.broadcasted_iota(jnp.int32, (1, 384), 1)
    lengths = [r.lengths[s] for s in range(3)]
    living = jnp.zeros((1, 384), F32)
    for s in range(3):
        living = jnp.where((lane >= 96 * s) & (lane < 96 * s + lengths[s]), 1.0, living)
    token_scores = (totals[4:6] + post_scale * totals[2:4]) * living
    row8 = lax.broadcasted_iota(jnp.int32, (8, 128), 0)
    lane8 = lax.broadcasted_iota(jnp.int32, (8, 128), 1)
    tile = jnp.zeros((8, 128), F32)
    for m in range(2):
        for s in range(3):
            inside = (lane >= 96 * s) & (lane < 96 * s + 96)
            score = jnp.sum(jnp.where(inside, token_scores[m : m + 1], 0.0), axis=1, keepdims=True)
            tile = jnp.where((row8 == m) & (lane8 == 3 * rank + s), score, tile)
    scores = Exchange(r.scores, 8, 8, rank, in_data, send["scores"], recv["scores"])
    r.scores[pl.ds(aligned(8 * rank, 8), 8), :] = tile
    scores.start()
    scores.wait()
    everyone = scores.total()
    ratio = everyone[1:2] - everyone[0:1]
    row32 = lax.broadcasted_iota(jnp.int32, (32, 128), 0)
    lane32 = lax.broadcasted_iota(jnp.int32, (32, 128), 1)
    named = jnp.full((32, 128), -1, jnp.int32)
    for k in range(24):
        named = jnp.where(row32 == k, r.pairing[k], named)
    chosen = named == lane32
    even = lax.rem(row32, 2) == 0
    picked = jnp.broadcast_to(jnp.sum(jnp.where(chosen, ratio, 0.0), axis=1, keepdims=True), (32, 128))
    other = jnp.where(even, pltpu.roll(picked, 31, 0), pltpu.roll(picked, 1, 0))
    margin = DPO_BETA * jnp.where(even, picked - other, other - picked)
    loss = jnp.maximum(-margin, 0.0) + jnp.log1p(jnp.exp(-jnp.abs(margin)))
    counted = even & (row32 < 24) & (lane32 == 0)
    total_loss = jnp.sum(jnp.where(counted, loss, 0.0), axis=(0, 1), keepdims=True)
    r.loss[...] = jnp.broadcast_to(total_loss, (8, 128))
    pull = DPO_BETA * LOSS_SCALE / (1.0 + jnp.exp(margin))
    signed = jnp.where(even, -pull, pull)
    coefficients = jnp.sum(jnp.where(chosen, signed, 0.0), axis=0, keepdims=True)
    lane128 = lax.broadcasted_iota(jnp.int32, (1, 128), 1)
    coefficient = jnp.zeros((1, 384), F32)
    for s in range(3):
        own = jnp.sum(jnp.where(lane128 == 3 * rank + s, coefficients, 0.0), axis=1, keepdims=True)
        coefficient = jnp.where((lane >= 96 * s) & (lane < 96 * s + 96), own, coefficient)
    coefficient = coefficient * living
    scale_pol = post_scale[1:2]
    shrink = scale_pol * scale_pol * scale_pol * (coefficient * totals[3:4]) / WIDTH
    rows_to_columns(r.table, [post_scale, coefficient, shrink])
    grad_result = r.table[0:TOK, 2:3] * r.readout[...].astype(F32)
    grad_summed = r.table[0:TOK, 1:2] * post_gain * grad_result - r.summed[1] * r.table[0:TOK, 3:4]
    pack_hidden(grad_summed, r.grad_buf, mine * SHARD)

    back_gather = Gather(r.grad_buf, SHARD, send["gather_back"], recv["gather_back"])
    back_gather.wave(0)
    for m, (hidden, out) in enumerate(((r.ref_hidden, r.ref_out), (r.pol_hidden, r.pol_out))):
        out[...] = (hidden[...].astype(F32) + r.summed[m] * r.table[0:TOK, m : m + 1] * post_gain).astype(BF16)
    for w in range(1, 7):
        back_gather.wave(w)
    unpack_features(r.grad_buf, SHARD, 0, r.normed, 0)

    r.grad_mixed[...] = jnp.zeros_like(r.grad_mixed)

    def mix_back(i, carry):
        at = pl.ds(aligned(512 * i, 512), 512)
        r.grad_mixed[...] += dot(r.normed[0:TOK, at], r.w_back[at, :])
        return carry

    lax.fori_loop(0, 9, mix_back, 0)

    def attend_back(i, carry):
        here = pl.ds(aligned(96 * i, 96), 96)
        at = pl.ds(aligned(TOK + 96 * i, 96), 96)
        cos, sin = r.cosine[...], r.sine[...]
        key, value = r.heads[at, 256:384], r.heads[at, 384:512]
        key_grad = jnp.zeros((96, HEAD), F32)
        value_grad = jnp.zeros((96, HEAD), F32)
        for g in range(2):
            query = r.heads[at, 128 * g : 128 * g + 128]
            incoming = r.grad_mixed[here, 128 * g : 128 * g + 128].astype(BF16)
            prob = r.probs[at, 128 * g : 128 * g + 96]
            cap = r.capped[at, 128 * g : 128 * g + 96] / SOFT_CAP
            grad_probs = dot(incoming, value, NT)
            value_grad = value_grad + dot(prob.astype(BF16), incoming, TN)
            centered = grad_probs - jnp.sum(grad_probs * prob, axis=1, keepdims=True)
            grad_scores = (prob * centered * (1.0 - cap * cap) * QUERY_SCALE).astype(BF16)
            query_grad = dot(grad_scores, key)
            key_grad = key_grad + dot(grad_scores, query, TN)
            r.grads[here, 128 * g : 128 * g + 128] = rope(query_grad, cos, -sin).astype(BF16)
        r.grads[here, 256:384] = rope(key_grad, cos, -sin).astype(BF16)
        r.grads[here, 384:512] = value_grad.astype(BF16)
        return carry

    lax.fori_loop(0, 3, attend_back, 0)

    query_factor = jnp.concatenate([r.b_query[...], jnp.zeros((RANK, 256), BF16)], axis=0)
    value_factor = jnp.concatenate([jnp.zeros((RANK, 128), BF16), r.b_value[...]], axis=0)
    hook = dot(r.grads[:, 0:256], query_factor, NT) + dot(r.grads[:, 384:512], value_factor, NT)
    r.grads[:, 512:640] = (ADAPTER_SCALE * hook).astype(BF16)
    r.hooks[0:TOK, :] = r.grads[:, 512:640].astype(F32)
    r.hooks[TOK:384, :] = jnp.zeros((384 - TOK, 128), F32)
    hooks = Exchange(r.hook_parts, 24, 16, mine, in_tensor, send["hooks"], recv["hooks"], r.hooks, True)
    own_rows = pl.ds(aligned(24 * mine, 8), 24)
    r.hook_parts[own_rows, :] = r.hooks[own_rows, :]
    hooks.start()
    pull_back = jnp.sum(r.grads[...].astype(F32) * r.linear[...], axis=1, keepdims=True)
    stats_back = Exchange(r.stats_back, 8, 16, mine, in_tensor, send["stats_back"], recv["stats_back"])
    r.summed[0, :, 0:128] = r.table[0:TOK, :]
    r.stats_back[pl.ds(aligned(8 * mine, 8), 8), :] = columns_to_rows(r.table, [pull_back])
    stats_back.start()
    factor_terms = ADAPTER_SCALE * dot(r.low[...], r.grads[:, 0:512], TN)
    own_factor = pl.ds(aligned(64 * rank, 64), 64)
    r.factors[own_factor, 0:256] = factor_terms[0:64, 0:256].astype(BF16)
    r.factors[own_factor, 256:384] = factor_terms[64:128, 384:512].astype(BF16)
    factors = Exchange(r.factors, 64, 8, rank, in_data, send["factors"], recv["factors"])
    factors.start()
    partial_products(r.grads, r.w_in, r.partial_back, 1)
    back_scatter = Scatter(
        r.partial_back, r.landing_back, SHARD, send["scatter_back"], recv["scatter_back"]
    )
    back_scatter.begin()

    hooks.wait()
    r.hook_whole[own_rows, :] = hooks.total()
    hook_whole = Exchange(
        r.hook_whole, 24, 16, mine, in_tensor, send["hook_whole"], recv["hook_whole"]
    )
    hook_whole.start()
    back_scatter.turn(0, r.result)
    hook_whole.wait()
    hook_low = r.hook_whole[0:TOK, :].astype(BF16)

    def adapter_main(t, carry):
        term = dot(r.normed[TOK : 2 * TOK, pl.ds(aligned(256 * t, 256), 256)], hook_low, TN)
        r.a_terms[pl.ds(aligned(288 * t, 32), 256), :] = term.astype(BF16)
        return carry

    lax.fori_loop(0, 16, adapter_main, 0)

    def adapter_tail(q, carry):
        term = dot(r.normed[TOK : 2 * TOK, pl.ds(aligned(MAIN + 128 * q, 128), 128)], hook_low, TN)
        for j in range(4):
            at = aligned(288 * (4 * q + j) + 256, 32)
            r.a_terms[pl.ds(at, 32), :] = term[32 * j : 32 * j + 32, :].astype(BF16)
        return carry

    lax.fori_loop(0, 4, adapter_tail, 0)

    def across(i):
        return pltpu.make_async_remote_copy(
            src_ref=r.a_terms.at[pl.ds(aligned(576 * (2 * i + 1 - core), 64), 576), :],
            dst_ref=r.a_across.at[pl.ds(576 * i, 576), :],
            send_sem=send["across"].at[i],
            recv_sem=recv["across"].at[i],
            device_id={"dp_1": 1 - core},
            device_id_type=MESH,
        )

    def round_y(i):
        to = lax.rem(y + i, 4)
        return pltpu.make_async_remote_copy(
            src_ref=r.a_pairs.at[pl.ds(aligned(576 * to, 64), 576), :],
            dst_ref=r.a_round.at[pl.ds(576 * i, 576), :],
            send_sem=send["round"].at[i],
            recv_sem=recv["round"].at[i],
            device_id={"dp_0": to},
            device_id_type=MESH,
        )

    for i in range(4):
        across(i).start()
    back_scatter.turn(1, r.result)
    for i in range(4):
        across(i).wait_recv()
        own = r.a_terms[pl.ds(aligned(576 * (2 * i + core), 64), 576), :].astype(F32)
        pair = own + r.a_across[576 * i : 576 * i + 576, :].astype(F32)
        r.a_pairs[576 * i : 576 * i + 576, :] = pair.astype(BF16)
    for i in range(1, 4):
        round_y(i).start()
    back_scatter.turn(2, r.result)

    stats_back.wait()
    rows_to_columns(r.table, [stats_back.total()])
    unpack_result(r.result, 0, r.summed.at[1])
    pre_scale = r.scale[TOK : 2 * TOK, 0:1]
    shrink_back = pre_scale * pre_scale * r.table[0:TOK, 0:1] / WIDTH
    grad_result = r.summed[0, :, 2:3] * r.readout[...].astype(F32)
    hidden = r.pol_hidden[...].astype(F32)
    r.grad_hidden[...] = (
        grad_result + pre_scale * pre_gain * r.summed[1] - hidden * shrink_back
    ).astype(BF16)
    factors.wait()
    factor_total = factors.total()
    r.query_grad[...] = factor_total[:, 0:256]
    r.value_grad[...] = factor_total[:, 256:384]
    whole = r.a_pairs[pl.ds(aligned(576 * y, 64), 576), :].astype(F32)
    for i in range(1, 4):
        round_y(i).wait_recv()
        whole = whole + r.a_round[576 * i : 576 * i + 576, :].astype(F32)
    r.grad_a[...] = whole
    for ring in (gather, weights, scatter, back_gather, back_scatter):
        ring.drain()
    for exchange in (stats, scores, hooks, hook_whole, stats_back, factors):
        exchange.drain()
    for i in range(4):
        across(i).wait_send()
    for i in range(1, 4):
        round_y(i).wait_send()


def partial_products(rows, matrix, partial, models):
    def main(t, carry):
        product = dot(rows[...], matrix[pl.ds(aligned(256 * t, 256), 256), :], NT).astype(BF16)
        for m in range(models):
            for half in range(2):
                at = aligned((t * models + m) * SHARD + TOK * half, 16)
                partial[pl.ds(at, TOK), :] = product[m * TOK : m * TOK + TOK, 128 * half : 128 * half + 128]
        return carry

    lax.fori_loop(0, 16, main, 0)

    def tail(q, carry):
        product = dot(rows[...], matrix[pl.ds(aligned(MAIN + 128 * q, 128), 128), :], NT).astype(BF16)
        for m in range(models):
            for j in range(4):
                at = aligned(((4 * q + j) * models + m) * SHARD + 2 * TOK, 16)
                partial[pl.ds(at, GROUP), :] = pack_tail(product[m * TOK : m * TOK + TOK, 32 * j : 32 * j + 32])
        return carry

    lax.fori_loop(0, 4, tail, 0)


def rotation_tables():
    spacing = ROPE_BASE ** (-2.0 * np.arange(64, dtype=np.float32) / HEAD)
    angles = np.arange(LENGTH, dtype=np.float32)[:, None] * spacing.astype(np.float32)[None, :]
    cosine, sine = np.cos(angles), np.sin(angles)
    return (
        np.concatenate([cosine, cosine], axis=1).astype(np.float32),
        np.concatenate([-sine, sine], axis=1).astype(np.float32),
    )


INPUTS = [
    "lengths", "pairing", "ref_hidden", "pol_hidden", "readout", "w_query", "w_key", "w_value", "w_out", "a_query",
    "a_value", "b_query", "b_value", "pre_gain", "post_gain", "cosine", "sine",
]
OUTPUTS = ["pol_out", "ref_out", "loss", "grad_hidden", "grad_a", "query_grad", "value_grad"]


def body(
    ref_hidden,
    pol_hidden,
    readout,
    lengths,
    pairing,
    pre_gain,
    post_gain,
    w_query,
    w_key,
    value_projection,
    w_out,
    a_query,
    a_value,
    query_second_factor,
    value_second_factor,
):
    vmem, smem = pl.BlockSpec(memory_space=pltpu.VMEM), pl.BlockSpec(memory_space=pltpu.SMEM)
    cosine, sine = rotation_tables()
    semaphores = [pltpu.SemaphoreType.DMA(shape) for shape in SEMAPHORES.values() for _ in range(2)]
    tile = jax.ShapeDtypeStruct((TOK, TOK), BF16)
    results = pl.pallas_call(
        step_body,
        out_shape=(
            tile,
            tile,
            jax.ShapeDtypeStruct((8, 128), F32),
            tile,
            jax.ShapeDtypeStruct((576, 128), F32),
            jax.ShapeDtypeStruct((RANK, 256), F32),
            jax.ShapeDtypeStruct((RANK, 128), F32),
        ),
        in_specs=[smem, smem] + [vmem] * (len(INPUTS) - 2),
        out_specs=(vmem,) * len(OUTPUTS),
        scratch_shapes=[pltpu.VMEM(shape, kind) for shape, kind in SCRATCH.values()] + semaphores,
        compiler_params=pltpu.CompilerParams(
            collective_id=0, has_side_effects=True, vmem_limit_bytes=62 * 1024 * 1024
        ),
    )(
        lengths,
        pairing,
        ref_hidden,
        pol_hidden,
        readout,
        w_query,
        w_key,
        value_projection,
        w_out,
        a_query,
        a_value,
        query_second_factor,
        value_second_factor,
        pre_gain.reshape(16, TOK),
        post_gain.reshape(16, TOK),
        jnp.asarray(cosine),
        jnp.asarray(sine),
    )
    pol_out, ref_out, loss, grad_hidden, grad_a, query_grad, value_grad = results
    return (pol_out, ref_out, loss[0, 0], grad_hidden, grad_a, query_grad, value_grad)


def solution(mesh):
    torus = Mesh(mesh.devices.reshape(4, 2, 4, 4), ("dp_0", "dp_1", "tensor_0", "tensor_1"))
    split, rows, columns = P(DP, TENSOR), P(DP, None), P(None, TENSOR)
    return jax.shard_map(
        body,
        mesh=torus,
        in_specs=(split, split, split, P(DP), P(), P(), P(), split, split, split, split, rows, rows, columns, columns),
        out_specs=(split, split, P(), split, rows, columns, columns),
        check_vma=False,
    )
```

```python
import jax
import jax.numpy as jnp
import numpy as np
from jax import lax
from jax.experimental import pallas as pl
from jax.experimental.pallas import tpu as pltpu
from jax.sharding import Mesh
from jax.sharding import PartitionSpec as P

DP = ("dp_0", "dp_1")
TENSOR = ("tensor_0", "tensor_1")
MESH = pl.DeviceIdType.MESH

WIDTH = 4608
TOK = 288
LENGTH = 96
HEAD = 128
RANK = 64
NORM_EPS = 1e-06
SOFT_CAP = 50.0
ADAPTER_SCALE = 0.5
DPO_BETA = 0.5
LOSS_SCALE = 256.0
ROPE_BASE = 10000.0
QUERY_SCALE = float(WIDTH // 32) ** (-0.5)

GROUP = 80
SHARD = 2 * TOK + GROUP
MAIN = 4096
RINGS = ((0, 1), (0, -1), (1, 1), (1, -1))

ORDER = (2, 1, 3, 0)

F32 = jnp.float32
BF16 = jnp.bfloat16
NT = (((1,), (1,)), ((), ()))
TN = (((0,), (0,)), ((), ()))


def dot(a, b, dims=(((1,), (0,)), ((), ())), precision=None):
    return lax.dot_general(a, b, dims, preferred_element_type=F32, precision=precision)


def aligned(start, multiple):
    return start if isinstance(start, int) else pl.multiple_of(start, multiple)


def back(position, hops, direction):
    return lax.rem(position - hops * direction + 8, 4)


def chunks_of(rows):
    tiles = rows // 16
    sizes = [16 * (tiles // 4 + (1 if k < tiles % 4 else 0)) for k in range(4)]
    return sizes, [sum(sizes[:k]) for k in range(4)]


class Ring:
    def __init__(self, rows, send, recv):
        self.rows = rows
        self.sizes, self.starts = chunks_of(rows)
        self.send, self.recv = send, recv
        self.at = (lax.axis_index("tensor_0"), lax.axis_index("tensor_1"))

    def place(self, k, first, second):
        primary, way = RINGS[k]
        a = back(self.at[primary], first, way)
        b = back(self.at[1 - primary], second, way)
        px, pz = (a, b) if primary == 0 else (b, a)
        return aligned((4 * px + pz) * self.rows + self.starts[k], 16)

    def next_on(self, k, secondary, behind=False):
        primary, way = RINGS[k]
        axis = 1 - primary if secondary else primary
        return {TENSOR[axis]: back(self.at[axis], 1 if behind else -1, way)}

    def remote(self, source, target, k, number, device):
        return pltpu.make_async_remote_copy(
            src_ref=source,
            dst_ref=target,
            send_sem=self.send.at[k, number],
            recv_sem=self.recv.at[k, number],
            device_id=device,
            device_id_type=MESH,
        )


class Gather(Ring):
    def __init__(self, buffer, rows, send, recv):
        super().__init__(rows, send, recv)
        self.buffer = buffer

    def piece(self, k, j, s):
        return self.buffer.at[pl.ds(self.place(k, j, s), self.sizes[k]), :]

    def first(self, k, number):
        piece = self.piece(k, 1 if number == 1 else 0, 0)
        return self.remote(piece, piece, k, number, self.next_on(k, False, number == 2))

    def second(self, k, j, s):
        piece = self.piece(k, j, s)
        return self.remote(piece, piece, k, 3 + 3 * j + s, self.next_on(k, True))

    def begin(self):
        for k in range(4):
            self.first(k, 0).start()
            self.first(k, 2).start()
        for k in range(4):
            self.second(k, 0, 0).start()

    def await_first(self, number):
        j = number + 1
        for k in range(4):
            piece = self.piece(k, j, 0)
            self.remote(piece, piece, k, number, self.next_on(k, False)).wait_recv()
            if number == 0:
                self.first(k, 1).start()
            self.second(k, j, 0).start()

    def await_second(self, j, s):
        for k in range(4):
            piece = self.piece(k, j, s + 1)
            self.remote(piece, piece, k, 3 + 3 * j + s, self.next_on(k, True)).wait_recv()
            if s < 2:
                self.second(k, j, s + 1).start()

    def steps(self):
        self.await_first(0)
        yield
        self.await_first(2)
        yield
        self.await_second(0, 0)
        yield
        self.await_first(1)
        yield
        for j, s in ((1, 0), (3, 0), (0, 1), (2, 0), (1, 1), (3, 1), (0, 2), (2, 1), (1, 2), (3, 2), (2, 2)):
            self.await_second(j, s)
            yield

    def drain(self):
        for k in range(4):
            for number in range(3):
                self.first(k, number).wait_send()
            for j in range(4):
                for s in range(3):
                    self.second(k, j, s).wait_send()


class Scatter(Ring):
    def __init__(self, partial, landing, rows, send, recv):
        super().__init__(rows, send, recv)
        self.partial, self.landing = partial, landing

    def piece(self, k, first, second):
        return self.partial.at[pl.ds(self.place(k, first, second), self.sizes[k]), :]

    def slot(self, k, number):
        return self.landing.at[pl.ds(15 * self.starts[k] + number * self.sizes[k], self.sizes[k]), :]

    def outer(self, k, j, s):
        number = 3 * j + s
        return self.remote(self.piece(k, ORDER[j], s + 1), self.slot(k, number), k, number, self.next_on(k, True))

    def inner(self, k, number):
        piece = self.piece(k, (2, 3, 1)[number - 12], 0)
        return self.remote(piece, self.slot(k, number), k, number, self.next_on(k, False, number == 14))

    def add(self, k, number, first, second):
        piece, slot = self.piece(k, first, second), self.slot(k, number)
        piece[...] = (piece[...].astype(F32) + slot[...].astype(F32)).astype(BF16)

    def begin(self):
        for j in range(4):
            for k in range(4):
                self.outer(k, j, 0).start()

    def steps(self, result):
        for s in range(3):
            for j in range(4):
                for k in range(4):
                    self.outer(k, j, s).wait_recv()
                    self.add(k, 3 * j + s, ORDER[j], s + 2)
                    if s < 2:
                        self.outer(k, j, s + 1).start()
                    elif j == 0:
                        self.inner(k, 12).start()
                    elif j == 1:
                        self.inner(k, 14).start()
                    elif j == 2:
                        self.inner(k, 12).wait_recv()
                        self.add(k, 12, 3, 0)
                        self.inner(k, 13).start()
                yield
        for k in range(4):
            own = self.piece(k, 0, 0)[...].astype(F32)
            for number in (14, 13):
                self.inner(k, number).wait_recv()
                own = own + self.slot(k, number)[...].astype(F32)
            result[pl.ds(self.starts[k], self.sizes[k]), :] = own
        yield

    def drain(self):
        for k in range(4):
            for j in range(4):
                for s in range(3):
                    self.outer(k, j, s).wait_send()
            for number in range(12, 15):
                self.inner(k, number).wait_send()


class Weights:
    def __init__(self, w_in, w_back, y_send, y_recv, d_send, d_recv):
        self.w_in, self.w_back = w_in, w_back
        self.sems = (y_send, y_recv, d_send, d_recv)
        self.y, self.core = lax.axis_index("dp_0"), lax.axis_index("dp_1")

    def block(self, hops, half, part, core):
        way = 1 - 2 * half
        tile = 2 * (2 * back(self.y, hops, way) + core) + half
        if part < 2:
            return self.w_in.at[pl.ds(aligned(256 * tile + 128 * part, 128), 128), :]
        if part == 3:
            return self.w_back.at[pl.ds(aligned(256 * tile, 256), 256), :]
        ref = self.w_in if part == 2 else self.w_back
        return ref.at[pl.ds(aligned(MAIN + 32 * tile, 32), 32), :]

    def round(self, s, half, part, arriving=False):
        ref = self.block(s + 1 if arriving else s, half, part, self.core)
        return pltpu.make_async_remote_copy(
            src_ref=ref,
            dst_ref=ref,
            send_sem=self.sems[0].at[half, s, part],
            recv_sem=self.sems[1].at[half, s, part],
            device_id={"dp_0": back(self.y, -1, 1 - 2 * half)},
            device_id_type=MESH,
        )

    def across(self, i, half, part, arriving=False):
        ref = self.block(i, half, part, 1 - self.core if arriving else self.core)
        return pltpu.make_async_remote_copy(
            src_ref=ref,
            dst_ref=ref,
            send_sem=self.sems[2].at[half, i, part],
            recv_sem=self.sems[3].at[half, i, part],
            device_id={"dp_1": 1 - self.core},
            device_id_type=MESH,
        )

    def step(self, s, parts):
        for part in parts:
            for half in range(2):
                if s > 0:
                    self.round(s - 1, half, part, True).wait_recv()
                if s < 3:
                    self.round(s, half, part).start()
                self.across(s, half, part).start()

    def arrive(self, parts):
        for half in range(2):
            for part in parts:
                for i in range(4):
                    self.across(i, half, part, True).wait_recv()

    def drain(self):
        for half in range(2):
            for part in range(5):
                for s in range(3):
                    self.round(s, half, part).wait_send()
                for i in range(4):
                    self.across(i, half, part).wait_send()


class Exchange:
    def __init__(self, buffer, rows, count, me, device_of, send, recv, source=None, spread=False):
        self.buffer, self.rows, self.count, self.me = buffer, rows, count, me
        self.device_of, self.send, self.recv = device_of, send, recv
        self.source = buffer if source is None else source
        self.spread = spread

    def slot(self, i):
        return self.buffer.at[pl.ds(aligned(i * self.rows, 8), self.rows), :]

    def copy(self, delta):
        peer = lax.rem(self.me + delta, self.count)
        origin = peer if self.spread else self.me
        return pltpu.make_async_remote_copy(
            src_ref=self.source.at[pl.ds(aligned(origin * self.rows, 8), self.rows), :],
            dst_ref=self.slot(self.me),
            send_sem=self.send.at[delta],
            recv_sem=self.recv.at[delta],
            device_id=self.device_of(peer),
            device_id_type=MESH,
        )

    def start(self):
        for delta in range(1, self.count):
            self.copy(delta).start()

    def wait(self):
        for delta in range(1, self.count):
            arrived = self.slot(lax.rem(self.me - delta + self.count, self.count))
            pltpu.make_async_remote_copy(
                src_ref=arrived,
                dst_ref=arrived,
                send_sem=self.send.at[delta],
                recv_sem=self.recv.at[delta],
                device_id=self.device_of(lax.rem(self.me + delta, self.count)),
                device_id_type=MESH,
            ).wait_recv()

    def total(self):
        value = self.buffer[0 : self.rows, :].astype(F32)
        for i in range(1, self.count):
            value = value + self.buffer[self.rows * i : self.rows * i + self.rows, :].astype(F32)
        return value

    def drain(self):
        for delta in range(1, self.count):
            self.copy(delta).wait_send()


def in_tensor(i):
    return {"tensor_0": lax.div(i, 4), "tensor_1": lax.rem(i, 4)}


def in_data(i):
    return {"dp_0": lax.div(i, 2), "dp_1": lax.rem(i, 2)}


def together(main, filler, ratio):
    for number, _ in enumerate(main):
        for _ in range(ratio if isinstance(ratio, int) else ratio[number]):
            next(filler, None)
    for _ in filler:
        pass


def greet(peers):
    barrier = pltpu.get_barrier_semaphore()
    for peer in peers:
        pl.semaphore_signal(barrier, inc=1, device_id=peer, device_id_type=MESH)
    pl.semaphore_wait(barrier, len(peers))


def pack_tail(tail):
    last = jnp.concatenate([tail[240:288], jnp.zeros((32, 32), tail.dtype)], axis=0)
    return jnp.concatenate([tail[0:80], tail[80:160], tail[160:240], last], axis=1)


GROUPS = ((0, 80), (80, 80), (160, 80), (240, 48))


def unpack_features(buffer, rows, offset, target, row_offset):
    def main(t, carry):
        base = aligned(t * rows + offset, 16)
        for half in range(2):
            target[pl.ds(row_offset, TOK), pl.ds(aligned(256 * t + 128 * half, 128), 128)] = buffer[
                pl.ds(aligned(base + TOK * half, 16), TOK), :
            ]
        return carry

    lax.fori_loop(0, 16, main, 0)

    def tail(q, carry):
        tails = [
            buffer[pl.ds(aligned((4 * q + j) * rows + offset + 2 * TOK, 16), GROUP), :] for j in range(4)
        ]
        for g, (start, size) in enumerate(GROUPS):
            joined = jnp.concatenate([t[:size, 32 * g : 32 * g + 32] for t in tails], axis=1)
            target[pl.ds(row_offset + start, size), pl.ds(aligned(MAIN + 128 * q, 128), 128)] = joined
        return carry

    lax.fori_loop(0, 4, tail, 0)


def unpack_result(packed, offset, target):
    for half in range(2):
        target[:, 128 * half : 128 * half + 128] = packed[offset + TOK * half : offset + TOK * half + TOK, :]
    for g, (start, size) in enumerate(GROUPS):
        base = offset + 2 * TOK
        target[start : start + size, 256:288] = packed[base : base + size, 32 * g : 32 * g + 32]


def pack_hidden(hidden, buffer, base):
    for half in range(2):
        buffer[pl.ds(aligned(base + TOK * half, 16), TOK), :] = hidden[:, 128 * half : 128 * half + 128].astype(
            BF16
        )
    buffer[pl.ds(aligned(base + 2 * TOK, 16), GROUP), :] = pack_tail(hidden[:, 256:288]).astype(BF16)


def feature_lanes(gain, start, count):
    pieces = []
    while count:
        row, lane = divmod(start, 128)
        size = min(count, 128 - lane)
        pieces.append(gain[row : row + 1, lane : lane + size])
        start, count = start + size, count - size
    return pieces[0] if len(pieces) == 1 else jnp.concatenate(pieces, axis=1)


def order_gain(gain, target):
    for c in range(32):
        target[c : c + 1, :] = feature_lanes(gain, 288 * (c // 2) + 128 * (c % 2), 128)
    for q in range(4):
        tails = [feature_lanes(gain, 288 * (4 * q + j) + 256, 32) for j in range(4)]
        target[32 + q : 33 + q, :] = jnp.concatenate(tails, axis=1)


def own_gain(ordered, mine):
    tail = ordered[pl.ds(32 + lax.div(mine, 4), 1), :]
    picked = jnp.zeros((1, 32), F32)
    for j in range(4):
        picked = jnp.where(lax.rem(mine, 4) == j, tail[:, 32 * j : 32 * j + 32], picked)
    return jnp.concatenate([ordered[pl.ds(2 * mine, 1), :], ordered[pl.ds(2 * mine + 1, 1), :], picked], axis=1)


def normalize(normed, scale_ref, gain_ref, offset):
    def rows(i, carry):
        at = pl.ds(aligned(offset + 96 * i, 96), 96)
        squares = jnp.zeros((96, 128), F32)
        for c in range(36):
            x = normed[at, 128 * c : 128 * c + 128].astype(F32)
            squares = squares + x * x
        scale = lax.rsqrt(jnp.sum(squares, axis=1, keepdims=True) / WIDTH + NORM_EPS)
        scale_ref[at, :] = jnp.broadcast_to(scale, (96, 128))
        for c in range(36):
            x = normed[at, 128 * c : 128 * c + 128].astype(F32)
            normed[at, 128 * c : 128 * c + 128] = (x * scale * gain_ref[c : c + 1, :]).astype(BF16)
        return carry

    lax.fori_loop(0, 3, rows, 0)


def rope(x, cosine, sine):
    return x * cosine + pltpu.roll(x, 64, 1) * sine


def allowed_here(length):
    query = lax.broadcasted_iota(jnp.int32, (LENGTH, LENGTH), 0)
    key = lax.broadcasted_iota(jnp.int32, (LENGTH, LENGTH), 1)
    return (key <= query) & (key < length)


def columns_to_rows(scratch, columns):
    lane = lax.broadcasted_iota(jnp.int32, (TOK, 128), 1)
    table = jnp.zeros((TOK, 128), F32)
    for k, column in enumerate(columns):
        table = jnp.where(lane == k, column, table)
    scratch[0:TOK, :] = table
    scratch[TOK:384, :] = jnp.zeros((384 - TOK, 128), F32)
    return jnp.transpose(scratch[...])[0:8, :]


def rows_to_columns(scratch, rows):
    missing = 128 - sum(row.shape[0] for row in rows)
    filled = jnp.concatenate(list(rows) + [jnp.zeros((missing, 384), F32)], axis=0)
    scratch[...] = jnp.transpose(filled)


SCRATCH = {
    "hidden_buf": ((32 * SHARD, 128), BF16),
    "w_in": ((WIDTH, 640), BF16),
    "w_back": ((WIDTH, 256), BF16),
    "normed": ((2 * TOK, WIDTH), BF16),
    "scale": ((2 * TOK, 128), F32),
    "acc": ((2 * TOK, 640), F32),
    "linear": ((TOK, 640), F32),
    "low": ((TOK, 128), BF16),
    "heads": ((2 * TOK, 512), BF16),
    "mixed": ((2 * TOK, 256), BF16),
    "probs": ((2 * TOK, 256), F32),
    "capped": ((2 * TOK, 256), F32),
    "partial": ((16 * SHARD, 128), BF16),
    "partial_pol": ((16 * SHARD, 128), BF16),
    "landing": ((15 * SHARD, 128), BF16),
    "landing_pol": ((15 * SHARD, 128), BF16),
    "result": ((2, SHARD, 128), F32),
    "summed": ((2, TOK, TOK), F32),
    "table": ((384, 128), F32),
    "coefficient": ((384, 128), F32),
    "ref_stats": ((16 * 8, 384), F32),
    "pol_stats": ((16 * 16, 128), F32),
    "pre_ordered": ((40, 128), F32),
    "post_ordered": ((40, 128), F32),
    "scores": ((8 * 8, 128), F32),
    "grad_buf": ((16 * SHARD, 128), BF16),
    "grad_mixed": ((TOK, 256), F32),
    "grads": ((TOK, 640), BF16),
    "partial_back": ((16 * SHARD, 128), BF16),
    "landing_back": ((15 * SHARD, 128), BF16),
    "hooks": ((384, 128), F32),
    "hook_parts": ((384, 128), F32),
    "hook_whole": ((384, 128), F32),
    "stats_back": ((16 * 8, 384), F32),
    "factors": ((8 * 64, 384), BF16),
    "a_terms": ((WIDTH, 128), BF16),
    "a_across": ((4 * 576, 128), BF16),
    "a_pairs": ((4 * 576, 128), BF16),
    "a_round": ((4 * 576, 128), BF16),
}
SEMAPHORES = {
    "gather": (4, 15),
    "scatter_ref": (4, 15),
    "scatter_pol": (4, 15),
    "gather_back": (4, 15),
    "scatter_back": (4, 15),
    "y": (2, 3, 5),
    "d": (2, 4, 5),
    "ref_stats": (16,),
    "pol_stats": (16,),
    "scores": (8,),
    "hooks": (16,),
    "hook_whole": (16,),
    "stats_back": (16,),
    "factors": (8,),
    "across": (4,),
    "round": (4,),
}


class Refs:
    pass


def step_body(*refs):
    names = INPUTS + OUTPUTS + list(SCRATCH)
    r = Refs()
    for name, ref in zip(names, refs):
        setattr(r, name, ref)
    sems = refs[len(names) :]
    send = dict(zip(SEMAPHORES, sems[0::2]))
    recv = dict(zip(SEMAPHORES, sems[1::2]))

    x, z = lax.axis_index("tensor_0"), lax.axis_index("tensor_1")
    y, core = lax.axis_index("dp_0"), lax.axis_index("dp_1")
    mine, rank = 4 * x + z, 2 * y + core
    pack_hidden(r.ref_hidden[...], r.hidden_buf, mine * 2 * SHARD)
    pack_hidden(r.pol_hidden[...], r.hidden_buf, mine * 2 * SHARD + SHARD)
    a_both = jnp.concatenate([r.a_query[...].astype(F32), r.a_value[...].astype(F32)], axis=0)
    a_both = jnp.transpose(jnp.concatenate([a_both, jnp.zeros((128, 64), F32)], axis=1))
    for half in range(2):
        tile = 2 * rank + half
        for start, size, to in ((0, 256, 256 * tile), (256, 32, MAIN + 32 * tile)):
            here, there = pl.ds(288 * half + start, size), pl.ds(aligned(to, 32), size)
            r.w_in[there, 0:256] = r.w_query[here, :]
            r.w_in[there, 256:384] = r.w_key[here, :]
            r.w_in[there, 384:512] = r.w_value[here, :]
            r.w_in[there, 512:640] = a_both[288 * half + start : 288 * half + start + size, :].astype(BF16)
            r.w_back[there, :] = r.w_out[here, :]
    greet(
        [in_tensor(lax.rem(mine + i, 16)) for i in range(1, 16)]
        + [in_data(lax.rem(rank + i, 8)) for i in range(1, 8)]
    )

    gather = Gather(r.hidden_buf, 2 * SHARD, send["gather"], recv["gather"])
    weights = Weights(r.w_in, r.w_back, send["y"], recv["y"], send["d"], recv["d"])

    def weight_steps():
        for s in range(1, 3):
            weights.step(s, (0,))
            yield
            weights.step(s, (1,))
            if s == 1:
                weights.step(s, (2,))
            yield
        weights.step(2, (2,))
        weights.step(0, (3, 4))
        yield
        for part in range(3):
            weights.step(3, (part,))
            yield
        weights.step(1, (3, 4))
        yield

    gather.begin()
    weights.step(0, (0, 1, 2))
    gain = r.pre_ordered
    order_gain(r.pre_gain, gain)
    order_gain(r.post_gain, r.post_ordered)
    pre_gain, post_gain = own_gain(gain, mine), own_gain(r.post_ordered, mine)
    together(gather.steps(), weight_steps(), (0, 1, 1, 0, 1, 1, 0, 1, 1, 0, 1, 1, 0, 1, 0))

    def project(m):
        rows = slice(m * TOK, m * TOK + TOK)
        for i in range(3):
            total = None
            for c in range(3 * i, 3 * i + 3):
                term = dot(r.normed[rows, 512 * c : 512 * c + 512], r.w_in[512 * c : 512 * c + 512, :])
                total = term if total is None else total + term
            r.acc[rows, :] = total if i == 0 else r.acc[rows, :] + total
            yield

    def attend(m):
        for i in range(3):
            at = slice(m * TOK + 96 * i, m * TOK + 96 * i + 96)
            cos, sin = r.cosine[...], r.sine[...]
            key = rope(r.acc[at, 256:384], cos, sin).astype(BF16)
            value = r.acc[at, 384:512].astype(BF16)
            allowed = allowed_here(r.lengths[i])
            r.heads[at, 256:384] = key
            r.heads[at, 384:512] = value
            for g in range(2):
                query = rope(r.acc[at, 128 * g : 128 * g + 128], cos, sin).astype(BF16)
                r.heads[at, 128 * g : 128 * g + 128] = query
                scores = dot(query, key, NT) * QUERY_SCALE
                cap = SOFT_CAP * jnp.tanh(scores / SOFT_CAP)
                weight = jnp.where(allowed, jnp.exp(cap), 0.0)
                prob = weight / jnp.sum(weight, axis=1, keepdims=True)
                r.probs[at, 128 * g : 128 * g + 96] = prob
                r.capped[at, 128 * g : 128 * g + 96] = cap
                r.mixed[at, 128 * g : 128 * g + 128] = dot(prob.astype(BF16), value).astype(BF16)
            yield

    unpack_features(r.hidden_buf, 2 * SHARD, 0, r.normed, 0)
    normalize(r.normed, r.scale, gain, 0)
    weights.arrive((0, 1, 2))
    weights.step(2, (3, 4))
    for _ in project(0):
        pass
    for _ in attend(0):
        pass
    weights.step(3, (3, 4))
    weights.arrive((3, 4))
    for _ in partial_products(r.mixed.at[0:TOK], r.w_back, r.partial):
        pass
    ref_scatter = Scatter(r.partial, r.landing, SHARD, send["scatter_ref"], recv["scatter_ref"])
    ref_scatter.begin()
    pol_scatter = Scatter(r.partial_pol, r.landing_pol, SHARD, send["scatter_pol"], recv["scatter_pol"])

    def policy():
        unpack_features(r.hidden_buf, 2 * SHARD, SHARD, r.normed, TOK)
        yield
        normalize(r.normed, r.scale, gain, TOK)
        yield
        yield from project(1)
        r.linear[...] = r.acc[TOK : 2 * TOK, :]
        r.low[...] = r.acc[TOK : 2 * TOK, 512:640].astype(BF16)
        query_factor = jnp.concatenate([r.b_query[...], jnp.zeros((RANK, 256), BF16)], axis=0)
        value_factor = jnp.concatenate([jnp.zeros((RANK, 128), BF16), r.b_value[...]], axis=0)
        r.acc[TOK : 2 * TOK, 0:256] += ADAPTER_SCALE * dot(r.low[...], query_factor)
        r.acc[TOK : 2 * TOK, 384:512] += ADAPTER_SCALE * dot(r.low[...], value_factor)
        yield
        yield from attend(1)
        yield from partial_products(r.mixed.at[TOK : 2 * TOK], r.w_back, r.partial_pol)
        pol_scatter.begin()
        yield

    def token_sums(m, hidden):
        unpack_result(r.result.at[m], 0, r.summed.at[m])
        summed, readout = r.summed[m], r.readout[...].astype(F32)
        return [
            jnp.sum(summed * summed, axis=1, keepdims=True),
            jnp.sum(summed * post_gain * readout, axis=1, keepdims=True),
            jnp.sum(hidden[...].astype(F32) * readout, axis=1, keepdims=True),
        ]

    ref_stats = Exchange(r.ref_stats, 8, 16, mine, in_tensor, send["ref_stats"], recv["ref_stats"])
    pol_stats = Exchange(r.pol_stats, 16, 16, mine, in_tensor, send["pol_stats"], recv["pol_stats"])

    def policy_ring():
        yield from pol_scatter.steps(r.result.at[1])

    def after_ref():
        columns = columns_to_rows(r.table, token_sums(0, r.ref_hidden))
        r.ref_stats[pl.ds(aligned(8 * mine, 8), 8), :] = columns
        ref_stats.start()
        yield

    def fill(steps, count):
        for _ in range(count):
            next(steps, None)

    ref_ring, policy_work, policy_steps = ref_scatter.steps(r.result.at[0]), policy(), policy_ring()
    fill(policy_work, 3)
    for count in (2, 2, 2, 2, 4):
        fill(ref_ring, 1)
        fill(policy_work, count)
    for _ in policy_work:
        pass
    fill(ref_ring, 3)
    for _ in range(5):
        fill(ref_ring, 1)
        fill(policy_steps, 1)
    together(policy_steps, after_ref(), (1,) + (0,) * 12)
    columns = columns_to_rows(r.table, token_sums(1, r.pol_hidden))
    packed = [columns[k : k + 1, 128 * c : 128 * c + 128] for k in range(3) for c in range(3)]
    packed = jnp.concatenate(packed + [jnp.zeros((7, 128), F32)], axis=0)
    r.pol_stats[pl.ds(aligned(16 * mine, 8), 16), :] = packed
    pol_stats.start()
    pol_stats.wait()
    packed = pol_stats.total()
    pol_total = [
        jnp.concatenate([packed[3 * k + c : 3 * k + c + 1] for c in range(3)], axis=1) for k in range(3)
    ]
    scale_pol = lax.rsqrt(pol_total[0] / WIDTH + NORM_EPS)
    rows_to_columns(r.table, [scale_pol, scale_pol * scale_pol * scale_pol * pol_total[1] / WIDTH])
    readout = r.readout[...].astype(F32)
    bare = r.table[0:TOK, 0:1] * post_gain * readout - r.summed[1] * r.table[0:TOK, 1:2]
    pack_hidden(bare, r.grad_buf, mine * SHARD)
    back_gather = Gather(r.grad_buf, SHARD, send["gather_back"], recv["gather_back"])
    back_gather.begin()

    lane = lax.broadcasted_iota(jnp.int32, (1, 384), 1)
    lengths = [r.lengths[s] for s in range(3)]
    living = jnp.zeros((1, 384), F32)
    for s in range(3):
        living = jnp.where((lane >= 96 * s) & (lane < 96 * s + lengths[s]), 1.0, living)
    ref_stats.wait()
    ref_total = ref_stats.total()
    scale_ref = lax.rsqrt(ref_total[0:1] / WIDTH + NORM_EPS)
    token_scores = (
        (ref_total[2:3] + scale_ref * ref_total[1:2]) * living,
        (pol_total[2] + scale_pol * pol_total[1]) * living,
    )
    row8 = lax.broadcasted_iota(jnp.int32, (8, 128), 0)
    lane8 = lax.broadcasted_iota(jnp.int32, (8, 128), 1)
    tile = jnp.zeros((8, 128), F32)
    for m in range(2):
        for s in range(3):
            inside = (lane >= 96 * s) & (lane < 96 * s + 96)
            score = jnp.sum(jnp.where(inside, token_scores[m], 0.0), axis=1, keepdims=True)
            tile = jnp.where((row8 == m) & (lane8 == 3 * rank + s), score, tile)
    scores = Exchange(r.scores, 8, 8, rank, in_data, send["scores"], recv["scores"])
    r.scores[pl.ds(aligned(8 * rank, 8), 8), :] = tile
    scores.start()

    def outputs():
        rows_to_columns(r.coefficient, [scale_ref, scale_pol])
        for m, (hidden, out) in enumerate(((r.ref_hidden, r.ref_out), (r.pol_hidden, r.pol_out))):
            scale = r.coefficient[0:TOK, m : m + 1]
            out[...] = (hidden[...].astype(F32) + r.summed[m] * scale * post_gain).astype(BF16)
            yield

    def preference():
        scores.wait()
        everyone = scores.total()
        ratio = everyone[1:2] - everyone[0:1]
        row32 = lax.broadcasted_iota(jnp.int32, (32, 128), 0)
        lane32 = lax.broadcasted_iota(jnp.int32, (32, 128), 1)
        named = jnp.full((32, 128), -1, jnp.int32)
        for k in range(24):
            named = jnp.where(row32 == k, r.pairing[k], named)
        chosen = named == lane32
        even = lax.rem(row32, 2) == 0
        picked = jnp.sum(jnp.where(chosen, ratio, 0.0), axis=1, keepdims=True)
        picked = jnp.broadcast_to(picked, (32, 128))
        other = jnp.where(even, pltpu.roll(picked, 31, 0), pltpu.roll(picked, 1, 0))
        margin = DPO_BETA * jnp.where(even, picked - other, other - picked)
        loss = jnp.maximum(-margin, 0.0) + jnp.log1p(jnp.exp(-jnp.abs(margin)))
        counted = even & (row32 < 24) & (lane32 == 0)
        total_loss = jnp.sum(jnp.where(counted, loss, 0.0), axis=(0, 1), keepdims=True)
        r.loss[...] = jnp.broadcast_to(total_loss, (8, 128))
        pull = DPO_BETA * LOSS_SCALE / (1.0 + jnp.exp(margin))
        signed = jnp.where(even, -pull, pull)
        coefficients = jnp.sum(jnp.where(chosen, signed, 0.0), axis=0, keepdims=True)
        lane128 = lax.broadcasted_iota(jnp.int32, (1, 128), 1)
        coefficient = jnp.zeros((1, 384), F32)
        for s in range(3):
            own = jnp.sum(jnp.where(lane128 == 3 * rank + s, coefficients, 0.0), axis=1, keepdims=True)
            coefficient = jnp.where((lane >= 96 * s) & (lane < 96 * s + 96), own, coefficient)
        rows_to_columns(r.coefficient, [coefficient * living])
        yield

    def meanwhile():
        yield from outputs()
        yield from preference()

    together(back_gather.steps(), meanwhile(), (1, 1, 0, 0, 0, 0, 0, 1, 0, 0, 0, 0, 0, 0, 0))
    unpack_features(r.grad_buf, SHARD, 0, r.normed, 0)

    for i in range(3):
        total = None
        for c in range(3 * i, 3 * i + 3):
            term = dot(r.normed[0:TOK, 512 * c : 512 * c + 512], r.w_back[512 * c : 512 * c + 512, :])
            total = term if total is None else total + term
        r.grad_mixed[...] = total if i == 0 else r.grad_mixed[...] + total
    r.grad_mixed[...] *= r.coefficient[0:TOK, 0:1]

    for i in range(3):
        here = slice(96 * i, 96 * i + 96)
        at = slice(TOK + 96 * i, TOK + 96 * i + 96)
        cos, sin = r.cosine[...], r.sine[...]
        key, value = r.heads[at, 256:384], r.heads[at, 384:512]
        key_grad = jnp.zeros((96, HEAD), F32)
        value_grad = jnp.zeros((96, HEAD), F32)
        for g in range(2):
            query = r.heads[at, 128 * g : 128 * g + 128]
            incoming = r.grad_mixed[here, 128 * g : 128 * g + 128].astype(BF16)
            prob = r.probs[at, 128 * g : 128 * g + 96]
            cap = r.capped[at, 128 * g : 128 * g + 96] / SOFT_CAP
            grad_probs = dot(incoming, value, NT)
            value_grad = value_grad + dot(prob.astype(BF16), incoming, TN)
            centered = grad_probs - jnp.sum(grad_probs * prob, axis=1, keepdims=True)
            grad_scores = (prob * centered * (1.0 - cap * cap) * QUERY_SCALE).astype(BF16)
            query_grad = dot(grad_scores, key)
            key_grad = key_grad + dot(grad_scores, query, TN)
            r.grads[here, 128 * g : 128 * g + 128] = rope(query_grad, cos, -sin).astype(BF16)
        r.grads[here, 256:384] = rope(key_grad, cos, -sin).astype(BF16)
        r.grads[here, 384:512] = value_grad.astype(BF16)

    query_factor = jnp.concatenate([r.b_query[...], jnp.zeros((RANK, 256), BF16)], axis=0)
    value_factor = jnp.concatenate([jnp.zeros((RANK, 128), BF16), r.b_value[...]], axis=0)
    hook = dot(r.grads[:, 0:256], query_factor, NT) + dot(r.grads[:, 384:512], value_factor, NT)
    r.grads[:, 512:640] = (ADAPTER_SCALE * hook).astype(BF16)
    r.hooks[0:TOK, :] = r.grads[:, 512:640].astype(F32)
    r.hooks[TOK:384, :] = jnp.zeros((384 - TOK, 128), F32)
    hooks = Exchange(r.hook_parts, 24, 16, mine, in_tensor, send["hooks"], recv["hooks"], r.hooks, True)
    own_rows = pl.ds(aligned(24 * mine, 8), 24)
    r.hook_parts[own_rows, :] = r.hooks[own_rows, :]
    hooks.start()
    pull_back = jnp.sum(r.grads[...].astype(F32) * r.linear[...], axis=1, keepdims=True)
    stats_back = Exchange(r.stats_back, 8, 16, mine, in_tensor, send["stats_back"], recv["stats_back"])
    r.stats_back[pl.ds(aligned(8 * mine, 8), 8), :] = columns_to_rows(r.table, [pull_back])
    stats_back.start()
    factor_terms = ADAPTER_SCALE * dot(r.low[...], r.grads[:, 0:512], TN)
    own_factor = pl.ds(aligned(64 * rank, 64), 64)
    r.factors[own_factor, 0:256] = factor_terms[0:64, 0:256].astype(BF16)
    r.factors[own_factor, 256:384] = factor_terms[64:128, 384:512].astype(BF16)
    factors = Exchange(r.factors, 64, 8, rank, in_data, send["factors"], recv["factors"])
    factors.start()
    for _ in partial_products(r.grads, r.w_in, r.partial_back):
        pass
    back_scatter = Scatter(
        r.partial_back, r.landing_back, SHARD, send["scatter_back"], recv["scatter_back"]
    )
    hook_whole = Exchange(
        r.hook_whole, 24, 16, mine, in_tensor, send["hook_whole"], recv["hook_whole"]
    )
    hooks.wait()
    r.hook_whole[own_rows, :] = hooks.total()
    hook_whole.start()
    back_scatter.begin()

    def across(i):
        return pltpu.make_async_remote_copy(
            src_ref=r.a_terms.at[pl.ds(aligned(576 * (2 * i + 1 - core), 64), 576), :],
            dst_ref=r.a_across.at[pl.ds(576 * i, 576), :],
            send_sem=send["across"].at[i],
            recv_sem=recv["across"].at[i],
            device_id={"dp_1": 1 - core},
            device_id_type=MESH,
        )

    def round_y(i):
        to = lax.rem(y + i, 4)
        return pltpu.make_async_remote_copy(
            src_ref=r.a_pairs.at[pl.ds(aligned(576 * to, 64), 576), :],
            dst_ref=r.a_round.at[pl.ds(576 * i, 576), :],
            send_sem=send["round"].at[i],
            recv_sem=recv["round"].at[i],
            device_id={"dp_0": to},
            device_id_type=MESH,
        )

    def adapters_back():
        hook_whole.wait()
        hook_low = r.hook_whole[0:TOK, :].astype(BF16)
        for q in range(4):
            at = MAIN + 128 * q
            tail = dot(r.normed[TOK : 2 * TOK, at : at + 128], hook_low, TN).astype(BF16)
            for t in range(4 * q, 4 * q + 4):
                term = dot(r.normed[TOK : 2 * TOK, 256 * t : 256 * t + 256], hook_low, TN)
                r.a_terms[288 * t : 288 * t + 256, :] = term.astype(BF16)
                j = t - 4 * q
                r.a_terms[288 * t + 256 : 288 * t + 288, :] = tail[32 * j : 32 * j + 32, :]
            across(q).start()
            yield
        for i in range(4):
            across(i).wait_recv()
            own = r.a_terms[pl.ds(aligned(576 * (2 * i + core), 64), 576), :].astype(F32)
            pair = own + r.a_across[576 * i : 576 * i + 576, :].astype(F32)
            r.a_pairs[576 * i : 576 * i + 576, :] = pair.astype(BF16)
        for i in range(1, 4):
            round_y(i).start()
        yield

    together(back_scatter.steps(r.result.at[0]), adapters_back(), (0, 0, 1, 1, 1, 1, 0, 1, 0, 0, 0, 0, 0))

    stats_back.wait()
    rows_to_columns(r.table, [stats_back.total()])
    unpack_result(r.result.at[0], 0, r.summed.at[1])
    pre_scale = r.scale[TOK : 2 * TOK, 0:1]
    shrink_back = pre_scale * pre_scale * r.table[0:TOK, 0:1] / WIDTH
    grad_result = r.coefficient[0:TOK, 0:1] * r.readout[...].astype(F32)
    hidden = r.pol_hidden[...].astype(F32)
    r.grad_hidden[...] = (
        grad_result + pre_scale * pre_gain * r.summed[1] - hidden * shrink_back
    ).astype(BF16)
    factors.wait()
    factor_total = factors.total()
    r.query_grad[...] = factor_total[:, 0:256]
    r.value_grad[...] = factor_total[:, 256:384]
    whole = r.a_pairs[pl.ds(aligned(576 * y, 64), 576), :].astype(F32)
    for i in range(1, 4):
        round_y(i).wait_recv()
        whole = whole + r.a_round[576 * i : 576 * i + 576, :].astype(F32)
    r.grad_a[...] = whole
    for ring in (gather, weights, ref_scatter, pol_scatter, back_gather, back_scatter):
        ring.drain()
    for exchange in (ref_stats, pol_stats, scores, hooks, hook_whole, stats_back, factors):
        exchange.drain()
    for i in range(4):
        across(i).wait_send()
    for i in range(1, 4):
        round_y(i).wait_send()


def partial_products(rows, matrix, partial):
    for block in range(4):
        left = rows[...]
        for t in range(4 * block, 4 * block + 4):
            product = dot(left, matrix[256 * t : 256 * t + 256, :], NT).astype(BF16)
            for half in range(2):
                at = t * SHARD + TOK * half
                partial[at : at + TOK, :] = product[:, 128 * half : 128 * half + 128]
        at = MAIN + 128 * block
        product = dot(left, matrix[at : at + 128, :], NT).astype(BF16)
        for j in range(4):
            at = (4 * block + j) * SHARD + 2 * TOK
            partial[at : at + GROUP, :] = pack_tail(product[:, 32 * j : 32 * j + 32])
        yield


def rotation_tables():
    spacing = ROPE_BASE ** (-2.0 * np.arange(64, dtype=np.float32) / HEAD)
    angles = np.arange(LENGTH, dtype=np.float32)[:, None] * spacing.astype(np.float32)[None, :]
    cosine, sine = np.cos(angles), np.sin(angles)
    return (
        np.concatenate([cosine, cosine], axis=1).astype(np.float32),
        np.concatenate([-sine, sine], axis=1).astype(np.float32),
    )


INPUTS = [
    "lengths", "pairing", "ref_hidden", "pol_hidden", "readout", "w_query", "w_key", "w_value", "w_out", "a_query",
    "a_value", "b_query", "b_value", "pre_gain", "post_gain", "cosine", "sine",
]
OUTPUTS = ["pol_out", "ref_out", "loss", "grad_hidden", "grad_a", "query_grad", "value_grad"]


def hand_out(*refs):
    for source, target in zip(refs[: len(OUTPUTS)], refs[len(OUTPUTS) :]):
        target[...] = source[0 : target.shape[0], 0 : target.shape[1]]


def body(
    ref_hidden,
    pol_hidden,
    readout,
    lengths,
    pairing,
    pre_gain,
    post_gain,
    w_query,
    w_key,
    value_projection,
    w_out,
    a_query,
    a_value,
    query_second_factor,
    value_second_factor,
):
    vmem, smem = pl.BlockSpec(memory_space=pltpu.VMEM), pl.BlockSpec(memory_space=pltpu.SMEM)
    cosine, sine = rotation_tables()
    semaphores = [pltpu.SemaphoreType.DMA(shape) for shape in SEMAPHORES.values() for _ in range(2)]
    tile = jax.ShapeDtypeStruct((TOK, TOK), BF16)
    results = pl.pallas_call(
        step_body,
        out_shape=(
            tile,
            tile,
            jax.ShapeDtypeStruct((8, 128), F32),
            tile,
            jax.ShapeDtypeStruct((576, 128), F32),
            jax.ShapeDtypeStruct((RANK, 256), F32),
            jax.ShapeDtypeStruct((RANK, 128), F32),
        ),
        in_specs=[smem, smem] + [vmem] * (len(INPUTS) - 2),
        out_specs=(vmem,) * len(OUTPUTS),
        scratch_shapes=[pltpu.VMEM(shape, kind) for shape, kind in SCRATCH.values()] + semaphores,
        compiler_params=pltpu.CompilerParams(
            collective_id=0, has_side_effects=True, vmem_limit_bytes=62 * 1024 * 1024
        ),
    )(
        lengths,
        pairing,
        ref_hidden,
        pol_hidden,
        readout,
        w_query,
        w_key,
        value_projection,
        w_out,
        a_query.T,
        a_value.T,
        query_second_factor,
        value_second_factor,
        pre_gain.reshape(36, 128),
        post_gain.reshape(36, 128),
        jnp.asarray(cosine),
        jnp.asarray(sine),
    )
    shapes = [jax.ShapeDtypeStruct(a.shape, a.dtype) for a in results]
    shapes[2] = jax.ShapeDtypeStruct((1, 1), F32)
    pol_out, ref_out, loss, grad_hidden, grad_a, query_grad, value_grad = pl.pallas_call(
        hand_out,
        out_shape=tuple(shapes),
        in_specs=[vmem] * len(OUTPUTS),
        out_specs=(vmem,) * len(OUTPUTS),
    )(*results)
    return (pol_out, ref_out, loss.reshape(()), grad_hidden, grad_a, query_grad, value_grad)


def solution(mesh):
    torus = Mesh(mesh.devices.reshape(4, 2, 4, 4), ("dp_0", "dp_1", "tensor_0", "tensor_1"))
    split, rows, columns = P(DP, TENSOR), P(DP, None), P(None, TENSOR)
    return jax.shard_map(
        body,
        mesh=torus,
        in_specs=(split, split, split, P(DP), P(), P(), P(), split, split, split, split, rows, rows, columns, columns),
        out_specs=(split, split, P(), split, rows, columns, columns),
        check_vma=False,
    )
```

```python
import jax
import jax.numpy as jnp
import numpy as np
from jax import lax
from jax.experimental import pallas as pl
from jax.experimental.pallas import tpu as pltpu
from jax.sharding import Mesh
from jax.sharding import PartitionSpec as P

Y, CORE, X, Z = "dp_0", "dp_1", "tensor_0", "tensor_1"
DP, TENSOR = (Y, CORE), (X, Z)
MESH = pl.DeviceIdType.MESH

WIDTH = 4608
TOK = 288
LENGTH = 96
HEAD = 128
RANK = 64
NORM_EPS = 1e-06
SOFT_CAP = 50.0
ADAPTER_SCALE = 0.5
DPO_BETA = 0.5
LOSS_SCALE = 256.0
ROPE_BASE = 10000.0
QUERY_SCALE = float(WIDTH // 32) ** (-0.5)

GROUP = 80
SHARD = 2 * TOK + GROUP
MAIN = 4096
RINGS = ((0, 1), (0, -1), (1, 1), (1, -1))

ORDER = (2, 1, 3, 0)

F32 = jnp.float32
BF16 = jnp.bfloat16
NT = (((1,), (1,)), ((), ()))
TN = (((0,), (0,)), ((), ()))


def dot(a, b, dims=(((1,), (0,)), ((), ())), precision=None):
    return lax.dot_general(a, b, dims, preferred_element_type=F32, precision=precision)


def aligned(start, multiple):
    return start if isinstance(start, int) else pl.multiple_of(start, multiple)


def back(position, hops, direction):
    return lax.rem(position - hops * direction + 8, 4)


def chunks_of(rows):
    tiles = rows // 16
    sizes = [16 * (tiles // 4 + (1 if k < tiles % 4 else 0)) for k in range(4)]
    return sizes, [sum(sizes[:k]) for k in range(4)]


class Ring:
    def __init__(self, rows, send, recv):
        self.rows = rows
        self.sizes, self.starts = chunks_of(rows)
        self.send, self.recv = send, recv
        self.at = (lax.axis_index(X), lax.axis_index(Z))

    def place(self, k, first, second):
        primary, way = RINGS[k]
        a = back(self.at[primary], first, way)
        b = back(self.at[1 - primary], second, way)
        px, pz = (a, b) if primary == 0 else (b, a)
        return aligned((4 * px + pz) * self.rows + self.starts[k], 16)

    def next_on(self, k, secondary, behind=False):
        primary, way = RINGS[k]
        axis = 1 - primary if secondary else primary
        return {TENSOR[axis]: back(self.at[axis], 1 if behind else -1, way)}

    def remote(self, source, target, number, device):
        return pltpu.make_async_remote_copy(
            src_ref=source,
            dst_ref=target,
            send_sem=self.send.at[0],
            recv_sem=self.recv.at[number],
            device_id=device,
            device_id_type=MESH,
        )

    def arrived(self, number):
        whole = self.memory.at[pl.ds(0, self.rows), :]
        self.remote(whole, whole, number, self.next_on(0, False)).wait_recv()

    def drain(self):
        whole = self.memory.at[pl.ds(0, 15 * self.rows), :]
        self.remote(whole, whole, 0, self.next_on(0, False)).wait_send()


class Gather(Ring):
    def __init__(self, buffer, rows, send, recv):
        super().__init__(rows, send, recv)
        self.memory = buffer

    def piece(self, k, j, s):
        return self.memory.at[pl.ds(self.place(k, j, s), self.sizes[k]), :]

    def first(self, k, number):
        piece = self.piece(k, 1 if number == 1 else 0, 0)
        return self.remote(piece, piece, number, self.next_on(k, False, number == 2))

    def second(self, k, j, s):
        piece = self.piece(k, j, s)
        return self.remote(piece, piece, 3 + 3 * j + s, self.next_on(k, True))

    def begin(self):
        for k in range(4):
            self.first(k, 0).start()
            self.first(k, 2).start()
        for k in range(4):
            self.second(k, 0, 0).start()

    def await_first(self, number):
        self.arrived(number)
        for k in range(4):
            if number == 0:
                self.first(k, 1).start()
            self.second(k, number + 1, 0).start()

    def await_second(self, j, s):
        self.arrived(3 + 3 * j + s)
        if s < 2:
            for k in range(4):
                self.second(k, j, s + 1).start()

    def steps(self):
        self.await_first(0)
        yield
        self.await_first(2)
        yield
        self.await_second(0, 0)
        yield
        self.await_first(1)
        yield
        for j, s in ((1, 0), (3, 0), (0, 1), (2, 0), (1, 1), (3, 1), (0, 2), (2, 1), (1, 2), (3, 2), (2, 2)):
            self.await_second(j, s)
            yield


class Scatter(Ring):
    def __init__(self, partial, landing, rows, send, recv):
        super().__init__(rows, send, recv)
        self.partial, self.landing, self.memory = partial, landing, landing

    def piece(self, k, first, second):
        return self.partial.at[pl.ds(self.place(k, first, second), self.sizes[k]), :]

    def slot(self, k, number):
        return self.landing.at[pl.ds(15 * self.starts[k] + number * self.sizes[k], self.sizes[k]), :]

    def outer(self, k, j, s):
        number = 3 * j + s
        return self.remote(self.piece(k, ORDER[j], s + 1), self.slot(k, number), number, self.next_on(k, True))

    def inner(self, k, number):
        piece = self.piece(k, (2, 3, 1)[number - 12], 0)
        return self.remote(piece, self.slot(k, number), number, self.next_on(k, False, number == 14))

    def add(self, k, number, first, second):
        piece, slot = self.piece(k, first, second), self.slot(k, number)
        piece[...] = (piece[...].astype(F32) + slot[...].astype(F32)).astype(BF16)

    def begin(self, parts=range(4)):
        for j in parts:
            for k in range(4):
                self.outer(k, j, 0).start()

    def steps(self, result):
        for s in range(3):
            for j in range(4):
                self.arrived(3 * j + s)
                if s == 2 and j == 2:
                    self.arrived(12)
                for k in range(4):
                    self.add(k, 3 * j + s, ORDER[j], s + 2)
                    if s < 2:
                        self.outer(k, j, s + 1).start()
                    elif j == 0:
                        self.inner(k, 12).start()
                    elif j == 1:
                        self.inner(k, 14).start()
                    elif j == 2:
                        self.add(k, 12, 3, 0)
                        self.inner(k, 13).start()
                yield
        self.arrived(14)
        self.arrived(13)
        for k in range(4):
            own = self.piece(k, 0, 0)[...].astype(F32)
            for number in (14, 13):
                own = own + self.slot(k, number)[...].astype(F32)
            result[pl.ds(self.starts[k], self.sizes[k]), :] = own
        yield


class Weights:
    def __init__(self, w_in, w_back, y_send, y_recv, d_send, d_recv):
        self.w_in, self.w_back = w_in, w_back
        self.sems = (y_send, y_recv, d_send, d_recv)
        self.y, self.core = lax.axis_index(Y), lax.axis_index(CORE)

    def block(self, hops, half, part, core):
        way = 1 - 2 * half
        tile = 2 * (2 * back(self.y, hops, way) + core) + half
        if part < 2:
            return self.w_in.at[pl.ds(aligned(256 * tile + 128 * part, 128), 128), :]
        if part == 3:
            return self.w_back.at[pl.ds(aligned(256 * tile, 256), 256), :]
        ref = self.w_in if part == 2 else self.w_back
        return ref.at[pl.ds(aligned(MAIN + 32 * tile, 32), 32), :]

    def round(self, s, half, part):
        ref = self.block(s, half, part, self.core)
        return self.copy(ref, 0, part, 5 * s + part, {Y: back(self.y, -1, 1 - 2 * half)})

    def across(self, i, half, part):
        return self.copy(self.block(i, half, part, self.core), 2, part, part // 3, {CORE: 1 - self.core})

    def copy(self, ref, way, part, number, device):
        return pltpu.make_async_remote_copy(
            src_ref=ref,
            dst_ref=ref,
            send_sem=self.sems[way].at[part // 3],
            recv_sem=self.sems[way + 1].at[number],
            device_id=device,
            device_id_type=MESH,
        )

    def rows(self, part, count):
        return (self.w_in if part < 3 else self.w_back).at[pl.ds(0, count), :]

    def step(self, s, parts):
        for part in parts:
            if s > 0:
                both = self.rows(part, 2 * (128, 128, 32, 256, 32)[part])
                self.copy(both, 0, part, 5 * (s - 1) + part, {CORE: 1 - self.core}).wait_recv()
            for half in range(2):
                if s < 3:
                    self.round(s, half, part).start()
                self.across(s, half, part).start()

    def arrive(self, part):
        self.copy(self.rows(part, 8 * TOK), 2, part, part // 3, {CORE: 1 - self.core}).wait_recv()

    def drain(self):
        for part in (0, 3):
            self.copy(self.rows(part, 6 * TOK), 0, part, 0, {CORE: 1 - self.core}).wait_send()
            self.copy(self.rows(part, 8 * TOK), 2, part, 0, {CORE: 1 - self.core}).wait_send()


class Exchange:
    def __init__(self, buffer, rows, count, me, device_of, send, recv):
        self.buffer, self.rows, self.count, self.me = buffer, rows, count, me
        self.device_of, self.send, self.recv = device_of, send, recv

    def part(self, buffer, i):
        return buffer.at[pl.ds(aligned(i * self.rows, self.rows), self.rows), :]

    def copy(self, source, target, peer):
        return pltpu.make_async_remote_copy(
            src_ref=source,
            dst_ref=target,
            send_sem=self.send.at[0],
            recv_sem=self.recv.at[0],
            device_id=self.device_of(peer),
            device_id_type=MESH,
        )

    def start(self):
        own = self.part(self.buffer, self.me)
        for delta in range(1, self.count):
            self.copy(own, own, lax.rem(self.me + delta, self.count)).start()

    def slots(self, count):
        whole = self.buffer.at[pl.ds(0, count * self.rows), :]
        return self.copy(whole, whole, lax.rem(self.me + 1, self.count))

    def wait(self):
        self.slots(self.count - 1).wait_recv()

    def total(self):
        value = self.buffer[0 : self.rows, :].astype(F32)
        for i in range(1, self.count):
            value = value + self.buffer[self.rows * i : self.rows * i + self.rows, :].astype(F32)
        return value

    def drain(self):
        self.slots(self.count - 1).wait_send()


OWNERS = 9


class HookSum:
    def __init__(self, terms, parts, sums, me, send_parts, recv_parts, send_sums, recv_sums):
        self.terms, self.parts, self.sums, self.me = terms, parts, sums, me
        self.there = Exchange(parts, 32, 16, me, in_tensor, send_parts, recv_parts)
        self.home = Exchange(parts, 32, 16, me, in_tensor, send_sums, recv_sums)
        self.owner = me < OWNERS

    def start(self):
        @pl.when(self.owner)
        def _():
            own = pl.ds(aligned(32 * self.me, 32), 32)
            self.parts[own, :] = self.terms[own, :]

        for delta in range(1, 16):
            peer = lax.rem(self.me + delta, 16)

            @pl.when(peer < OWNERS)
            def _():
                self.there.copy(self.there.part(self.terms, peer), self.there.part(self.parts, self.me), peer).start()

    def reduce(self):
        @pl.when(self.owner)
        def _():
            self.there.wait()
            self.sums[pl.ds(aligned(32 * self.me, 32), 32), :] = self.there.total().astype(BF16)
            own = self.home.part(self.sums, self.me)
            for delta in range(1, 16):
                self.home.copy(own, own, lax.rem(self.me + delta, 16)).start()

    def wait(self):
        @pl.when(self.owner)
        def _():
            self.home.slots(OWNERS - 1).wait_recv()

        @pl.when(jnp.logical_not(self.owner))
        def _():
            self.home.slots(OWNERS).wait_recv()

    def drain(self):
        @pl.when(self.owner)
        def _():
            self.there.slots(OWNERS - 1).wait_send()
            self.home.slots(15).wait_send()

        @pl.when(jnp.logical_not(self.owner))
        def _():
            self.there.slots(OWNERS).wait_send()


def in_tensor(i):
    return {X: lax.div(i, 4), Z: lax.rem(i, 4)}


def in_data(i):
    return {Y: lax.div(i, 2), CORE: lax.rem(i, 2)}


def together(main, filler, ratio):
    for number, _ in enumerate(main):
        for _ in range(ratio if isinstance(ratio, int) else ratio[number]):
            next(filler, None)
    for _ in filler:
        pass


def signal(peers):
    barrier = pltpu.get_barrier_semaphore()
    for peer in peers:
        pl.semaphore_signal(barrier, inc=1, device_id=peer, device_id_type=MESH)


def pack_tail(tail):
    last = jnp.concatenate([tail[240:288], jnp.zeros((32, 32), tail.dtype)], axis=0)
    return jnp.concatenate([tail[0:80], tail[80:160], tail[160:240], last], axis=1)


GROUPS = ((0, 80), (80, 80), (160, 80), (240, 48))


def unpack_features(buffer, rows, offset, target, row_offset):
    def main(t, carry):
        base = aligned(t * rows + offset, 16)
        for half in range(2):
            target[pl.ds(row_offset, TOK), pl.ds(aligned(256 * t + 128 * half, 128), 128)] = buffer[
                pl.ds(aligned(base + TOK * half, 16), TOK), :
            ]
        return carry

    lax.fori_loop(0, 16, main, 0)

    def tail(q, carry):
        tails = [
            buffer[pl.ds(aligned((4 * q + j) * rows + offset + 2 * TOK, 16), GROUP), :] for j in range(4)
        ]
        for g, (start, size) in enumerate(GROUPS):
            joined = jnp.concatenate([t[:size, 32 * g : 32 * g + 32] for t in tails], axis=1)
            target[pl.ds(row_offset + start, size), pl.ds(aligned(MAIN + 128 * q, 128), 128)] = joined
        return carry

    lax.fori_loop(0, 4, tail, 0)


def unpack_result(packed, offset, target):
    for half in range(2):
        target[:, 128 * half : 128 * half + 128] = packed[offset + TOK * half : offset + TOK * half + TOK, :]
    for g, (start, size) in enumerate(GROUPS):
        base = offset + 2 * TOK
        target[start : start + size, 256:288] = packed[base : base + size, 32 * g : 32 * g + 32]


def pack_hidden(hidden, buffer, base):
    for half in range(2):
        buffer[pl.ds(aligned(base + TOK * half, 16), TOK), :] = hidden[:, 128 * half : 128 * half + 128].astype(
            BF16
        )
    buffer[pl.ds(aligned(base + 2 * TOK, 16), GROUP), :] = pack_tail(hidden[:, 256:288]).astype(BF16)


def feature_lanes(gain, start, count):
    pieces = []
    while count:
        row, lane = divmod(start, 128)
        size = min(count, 128 - lane)
        pieces.append(gain[row : row + 1, lane : lane + size])
        start, count = start + size, count - size
    return pieces[0] if len(pieces) == 1 else jnp.concatenate(pieces, axis=1)


def order_gain(gain, target):
    for c in range(32):
        target[c : c + 1, :] = feature_lanes(gain, 288 * (c // 2) + 128 * (c % 2), 128)
    for q in range(4):
        tails = [feature_lanes(gain, 288 * (4 * q + j) + 256, 32) for j in range(4)]
        target[32 + q : 33 + q, :] = jnp.concatenate(tails, axis=1)


def own_gain(ordered, mine):
    tail = ordered[pl.ds(32 + lax.div(mine, 4), 1), :]
    picked = jnp.zeros((1, 32), F32)
    for j in range(4):
        picked = jnp.where(lax.rem(mine, 4) == j, tail[:, 32 * j : 32 * j + 32], picked)
    return jnp.concatenate([ordered[pl.ds(2 * mine, 1), :], ordered[pl.ds(2 * mine + 1, 1), :], picked], axis=1)


def normalize(normed, scale_ref, gain_ref, offset):
    def rows(i, carry):
        at = pl.ds(aligned(offset + 96 * i, 96), 96)
        squares = jnp.zeros((96, 128), F32)
        for c in range(36):
            x = normed[at, 128 * c : 128 * c + 128].astype(F32)
            squares = squares + x * x
        scale = lax.rsqrt(jnp.sum(squares, axis=1, keepdims=True) / WIDTH + NORM_EPS)
        scale_ref[at, :] = jnp.broadcast_to(scale, (96, 128))
        for c in range(36):
            x = normed[at, 128 * c : 128 * c + 128].astype(F32)
            normed[at, 128 * c : 128 * c + 128] = (x * scale * gain_ref[c : c + 1, :]).astype(BF16)
        return carry

    lax.fori_loop(0, 3, rows, 0)


def rope(x, cosine, sine):
    return x * cosine + pltpu.roll(x, 64, 1) * sine


def allowed_here(length):
    query = lax.broadcasted_iota(jnp.int32, (LENGTH, LENGTH), 0)
    key = lax.broadcasted_iota(jnp.int32, (LENGTH, LENGTH), 1)
    return (key <= query) & (key < length)


def columns_to_rows(scratch, columns):
    lane = lax.broadcasted_iota(jnp.int32, (TOK, 128), 1)
    table = jnp.zeros((TOK, 128), F32)
    for k, column in enumerate(columns):
        table = jnp.where(lane == k, column, table)
    scratch[0:TOK, :] = table
    scratch[TOK:384, :] = jnp.zeros((384 - TOK, 128), F32)
    return jnp.transpose(scratch[...])[0:8, :]


def rows_to_columns(scratch, rows):
    missing = 128 - sum(row.shape[0] for row in rows)
    filled = jnp.concatenate(list(rows) + [jnp.zeros((missing, 384), F32)], axis=0)
    scratch[...] = jnp.transpose(filled)


SCRATCH = dict(
    hidden_buf=((32 * SHARD, 128), BF16),
    w_in=((WIDTH, 640), BF16),
    w_back=((WIDTH, 256), BF16),
    normed=((2 * TOK, WIDTH), BF16),
    scale=((2 * TOK, 128), F32),
    acc=((2 * TOK, 640), F32),
    linear=((TOK, 640), F32),
    low=((TOK, 128), BF16),
    heads=((2 * TOK, 512), BF16),
    mixed=((2 * TOK, 256), BF16),
    probs=((2 * TOK, 256), F32),
    capped=((2 * TOK, 256), F32),
    partial=((16 * SHARD, 128), BF16),
    partial_pol=((16 * SHARD, 128), BF16),
    landing=((15 * SHARD, 128), BF16),
    landing_pol=((15 * SHARD, 128), BF16),
    result=((2, SHARD, 128), F32),
    summed=((2, TOK, TOK), F32),
    table=((384, 128), F32),
    coefficient=((384, 128), F32),
    ref_stats=((16 * 8, 384), F32),
    pol_stats=((16 * 16, 128), F32),
    pre_ordered=((40, 128), F32),
    post_ordered=((40, 128), F32),
    scores=((8 * 8, 128), F32),
    grad_buf=((16 * SHARD, 128), BF16),
    grad_mixed=((TOK, 256), F32),
    grads=((TOK, 640), BF16),
    partial_back=((16 * SHARD, 128), BF16),
    landing_back=((15 * SHARD, 128), BF16),
    hooks=((TOK, 128), BF16),
    hook_parts=((16 * 32, 128), BF16),
    hook_sums=((TOK, 128), BF16),
    stats_back=((16 * 8, 128), F32),
    factors=((8 * 64, 384), BF16),
    a_terms=((WIDTH, 128), BF16),
    a_across=((4 * 576, 128), BF16),
    a_pairs=((4 * 576, 128), BF16),
    a_round=((4 * 576, 128), BF16),
)
SEMAPHORES = dict(
    gather=(1, 15),
    scatter_ref=(1, 15),
    scatter_pol=(1, 15),
    gather_back=(1, 15),
    scatter_back=(1, 15),
    y=(2, 15),
    d=(2, 2),
    ref_stats=(1, 1),
    pol_stats=(1, 1),
    scores=(1, 1),
    hooks=(1, 1),
    hook_sums=(1, 1),
    stats_back=(1, 1),
    factors=(1, 1),
    across=(1, 1),
    round=(1, 1),
)


class Refs:
    pass


def step_body(*refs):
    inputs, outputs = list(INPUTS), list(OUTPUTS)
    outside, refs = refs[: len(inputs + outputs)], refs[len(inputs + outputs) :]
    names = inputs + outputs + list(SCRATCH)
    r, send, recv = Refs(), Refs(), Refs()
    for name, ref in zip(names, refs):
        setattr(r, name, ref)
    load_sems, store_sems, *sems = refs[len(names) :]
    for number, name in enumerate(SEMAPHORES):
        setattr(send, name, sems[2 * number])
        setattr(recv, name, sems[2 * number + 1])

    x, z = lax.axis_index(X), lax.axis_index(Z)
    y, core = lax.axis_index(Y), lax.axis_index(CORE)
    mine, rank = 4 * x + z, 2 * y + core
    def load(number):
        return pltpu.make_async_copy(outside[number], refs[number], load_sems.at[number])

    def store(number):
        at = len(inputs) + number
        return pltpu.make_async_copy(refs[at], outside[at], store_sems.at[number])

    signal(
        [in_tensor(lax.rem(mine + i, 16)) for i in range(1, 16)]
        + [in_data(lax.rem(rank + i, 8)) for i in range(1, 8)]
    )
    for number in range(len(inputs)):
        load(number).start()
    for number in range(10):
        load(number).wait()
    pack_hidden(r.ref_hidden[...], r.hidden_buf, mine * 2 * SHARD)
    pack_hidden(r.pol_hidden[...], r.hidden_buf, mine * 2 * SHARD + SHARD)
    a_both = jnp.concatenate([r.a_query[...].astype(F32), r.a_value[...].astype(F32)], axis=0)
    a_both = jnp.transpose(jnp.concatenate([a_both, jnp.zeros((128, 64), F32)], axis=1))
    for half in range(2):
        tile = 2 * rank + half
        for start, size, to in ((0, 256, 256 * tile), (256, 32, MAIN + 32 * tile)):
            here, there = pl.ds(288 * half + start, size), pl.ds(aligned(to, 32), size)
            r.w_in[there, 0:256] = r.w_query[here, :]
            r.w_in[there, 256:384] = r.w_key[here, :]
            r.w_in[there, 384:512] = r.w_value[here, :]
            r.w_in[there, 512:640] = a_both[288 * half + start : 288 * half + start + size, :].astype(BF16)
            r.w_back[there, :] = r.w_out[here, :]
    pl.semaphore_wait(pltpu.get_barrier_semaphore(), 22)

    gather = Gather(r.hidden_buf, 2 * SHARD, send.gather, recv.gather)
    weights = Weights(r.w_in, r.w_back, send.y, recv.y, send.d, recv.d)

    def weight_steps():
        for s in range(1, 3):
            weights.step(s, (0,))
            yield
            weights.step(s, (1,))
            if s == 1:
                weights.step(s, (2,))
            yield
        weights.step(2, (2,))
        weights.step(0, (3, 4))
        yield
        for part in range(3):
            weights.step(3, (part,))
            yield
        weights.step(1, (3, 4))
        yield

    gather.begin()
    weights.step(0, (0, 1, 2))
    for number in range(10, len(inputs)):
        load(number).wait()
    gain = r.pre_ordered
    order_gain(r.pre_gain, gain)
    order_gain(r.post_gain, r.post_ordered)
    pre_gain, post_gain = own_gain(gain, mine), own_gain(r.post_ordered, mine)
    together(gather.steps(), weight_steps(), (0, 1, 1, 0, 1, 1, 0, 1, 1, 0, 1, 1, 0, 1, 0))

    def project(m):
        rows = slice(m * TOK, m * TOK + TOK)
        for i in range(3):
            total = None
            for c in range(3 * i, 3 * i + 3):
                term = dot(r.normed[rows, 512 * c : 512 * c + 512], r.w_in[512 * c : 512 * c + 512, :])
                total = term if total is None else total + term
            r.acc[rows, :] = total if i == 0 else r.acc[rows, :] + total
            yield

    def attend(m):
        for i in range(3):
            at = slice(m * TOK + 96 * i, m * TOK + 96 * i + 96)
            cos, sin = r.cosine[...], r.sine[...]
            key = rope(r.acc[at, 256:384], cos, sin).astype(BF16)
            value = r.acc[at, 384:512].astype(BF16)
            allowed = allowed_here(r.lengths[i])
            r.heads[at, 256:384] = key
            r.heads[at, 384:512] = value
            for g in range(2):
                query = rope(r.acc[at, 128 * g : 128 * g + 128], cos, sin).astype(BF16)
                r.heads[at, 128 * g : 128 * g + 128] = query
                scores = dot(query, key, NT) * QUERY_SCALE
                cap = SOFT_CAP * jnp.tanh(scores / SOFT_CAP)
                weight = jnp.where(allowed, jnp.exp(cap), 0.0)
                prob = weight / jnp.sum(weight, axis=1, keepdims=True)
                r.probs[at, 128 * g : 128 * g + 96] = prob
                r.capped[at, 128 * g : 128 * g + 96] = cap
                r.mixed[at, 128 * g : 128 * g + 128] = dot(prob.astype(BF16), value).astype(BF16)
            yield

    unpack_features(r.hidden_buf, 2 * SHARD, 0, r.normed, 0)
    normalize(r.normed, r.scale, gain, 0)
    weights.arrive(0)
    weights.step(2, (3, 4))
    for _ in project(0):
        pass
    for _ in attend(0):
        pass
    weights.step(3, (3, 4))
    weights.arrive(3)
    for _ in partial_products(r.mixed.at[0:TOK], r.w_back, r.partial):
        pass
    ref_scatter = Scatter(r.partial, r.landing, SHARD, send.scatter_ref, recv.scatter_ref)
    ref_scatter.begin()
    pol_scatter = Scatter(r.partial_pol, r.landing_pol, SHARD, send.scatter_pol, recv.scatter_pol)

    def policy():
        unpack_features(r.hidden_buf, 2 * SHARD, SHARD, r.normed, TOK)
        yield
        normalize(r.normed, r.scale, gain, TOK)
        yield
        yield from project(1)
        r.linear[...] = r.acc[TOK : 2 * TOK, :]
        r.low[...] = r.acc[TOK : 2 * TOK, 512:640].astype(BF16)
        query_factor = jnp.concatenate([r.b_query[...], jnp.zeros((RANK, 256), BF16)], axis=0)
        value_factor = jnp.concatenate([jnp.zeros((RANK, 128), BF16), r.b_value[...]], axis=0)
        r.acc[TOK : 2 * TOK, 0:256] += ADAPTER_SCALE * dot(r.low[...], query_factor)
        r.acc[TOK : 2 * TOK, 384:512] += ADAPTER_SCALE * dot(r.low[...], value_factor)
        yield
        yield from attend(1)
        yield from partial_products(r.mixed.at[TOK : 2 * TOK], r.w_back, r.partial_pol)

    def token_sums(m, hidden):
        unpack_result(r.result.at[m], 0, r.summed.at[m])
        summed, readout = r.summed[m], r.readout[...].astype(F32)
        return [
            jnp.sum(summed * summed, axis=1, keepdims=True),
            jnp.sum(summed * post_gain * readout, axis=1, keepdims=True),
            jnp.sum(hidden[...].astype(F32) * readout, axis=1, keepdims=True),
        ]

    ref_stats = Exchange(r.ref_stats, 8, 16, mine, in_tensor, send.ref_stats, recv.ref_stats)
    pol_stats = Exchange(r.pol_stats, 16, 16, mine, in_tensor, send.pol_stats, recv.pol_stats)

    def policy_ring():
        yield from pol_scatter.steps(r.result.at[1])

    def after_ref():
        columns = columns_to_rows(r.table, token_sums(0, r.ref_hidden))
        r.ref_stats[pl.ds(aligned(8 * mine, 8), 8), :] = columns
        ref_stats.start()
        yield

    def fill(steps, count):
        for _ in range(count):
            next(steps, None)

    ref_ring, policy_work, policy_steps = ref_scatter.steps(r.result.at[0]), policy(), policy_ring()
    fill(policy_work, 3)
    for count in (2, 2, 2, 2, 2):
        fill(ref_ring, 1)
        fill(policy_work, count)
    for _ in policy_work:
        pass
    fill(ref_ring, 3)
    pol_scatter.begin((0,))
    fill(ref_ring, 1)
    pol_scatter.begin((1,))
    fill(ref_ring, 1)
    pol_scatter.begin((2, 3))
    for count in (2, 2, 1):
        fill(ref_ring, 1)
        fill(policy_steps, count)
    together(policy_steps, after_ref(), (1,) + (0,) * 12)
    columns = columns_to_rows(r.table, token_sums(1, r.pol_hidden))
    packed = [columns[k : k + 1, 128 * c : 128 * c + 128] for k in range(3) for c in range(3)]
    packed = jnp.concatenate(packed + [jnp.zeros((7, 128), F32)], axis=0)
    r.pol_stats[pl.ds(aligned(16 * mine, 8), 16), :] = packed
    pol_stats.start()
    pol_stats.wait()
    packed = pol_stats.total()
    pol_total = [
        jnp.concatenate([packed[3 * k + c : 3 * k + c + 1] for c in range(3)], axis=1) for k in range(3)
    ]
    scale_pol = lax.rsqrt(pol_total[0] / WIDTH + NORM_EPS)
    rows_to_columns(r.table, [scale_pol, scale_pol * scale_pol * scale_pol * pol_total[1] / WIDTH])
    readout = r.readout[...].astype(F32)
    bare = r.table[0:TOK, 0:1] * post_gain * readout - r.summed[1] * r.table[0:TOK, 1:2]
    pack_hidden(bare, r.grad_buf, mine * SHARD)
    back_gather = Gather(r.grad_buf, SHARD, send.gather_back, recv.gather_back)
    back_gather.begin()

    lane = lax.broadcasted_iota(jnp.int32, (1, 384), 1)
    lengths = [r.lengths[s] for s in range(3)]
    living = jnp.zeros((1, 384), F32)
    for s in range(3):
        living = jnp.where((lane >= 96 * s) & (lane < 96 * s + lengths[s]), 1.0, living)
    ref_stats.wait()
    ref_total = ref_stats.total()
    scale_ref = lax.rsqrt(ref_total[0:1] / WIDTH + NORM_EPS)
    token_scores = (
        (ref_total[2:3] + scale_ref * ref_total[1:2]) * living,
        (pol_total[2] + scale_pol * pol_total[1]) * living,
    )
    row8 = lax.broadcasted_iota(jnp.int32, (8, 128), 0)
    lane8 = lax.broadcasted_iota(jnp.int32, (8, 128), 1)
    tile = jnp.zeros((8, 128), F32)
    for m in range(2):
        for s in range(3):
            inside = (lane >= 96 * s) & (lane < 96 * s + 96)
            score = jnp.sum(jnp.where(inside, token_scores[m], 0.0), axis=1, keepdims=True)
            tile = jnp.where((row8 == m) & (lane8 == 3 * rank + s), score, tile)
    scores = Exchange(r.scores, 8, 8, rank, in_data, send.scores, recv.scores)
    r.scores[pl.ds(aligned(8 * rank, 8), 8), :] = tile
    scores.start()

    def layer_outputs():
        rows_to_columns(r.coefficient, [scale_ref, scale_pol])
        for m, (hidden, out) in enumerate(((r.ref_hidden, r.ref_out), (r.pol_hidden, r.pol_out))):
            scale = r.coefficient[0:TOK, m : m + 1]
            out[...] = (hidden[...].astype(F32) + r.summed[m] * scale * post_gain).astype(BF16)
            yield
            store(1 - m).start()

    def preference():
        scores.wait()
        everyone = scores.total()
        ratio = everyone[1:2] - everyone[0:1]
        row32 = lax.broadcasted_iota(jnp.int32, (32, 128), 0)
        lane32 = lax.broadcasted_iota(jnp.int32, (32, 128), 1)
        named = jnp.full((32, 128), -1, jnp.int32)
        for k in range(24):
            named = jnp.where(row32 == k, r.pairing[k], named)
        chosen = named == lane32
        even = lax.rem(row32, 2) == 0
        picked = jnp.sum(jnp.where(chosen, ratio, 0.0), axis=1, keepdims=True)
        picked = jnp.broadcast_to(picked, (32, 128))
        other = jnp.where(even, pltpu.roll(picked, 31, 0), pltpu.roll(picked, 1, 0))
        margin = DPO_BETA * jnp.where(even, picked - other, other - picked)
        loss = jnp.maximum(-margin, 0.0) + jnp.log1p(jnp.exp(-jnp.abs(margin)))
        counted = even & (row32 < 24) & (lane32 == 0)
        total_loss = jnp.sum(jnp.where(counted, loss, 0.0), axis=(0, 1), keepdims=True)
        r.loss[...] = jnp.broadcast_to(total_loss, (8, 128))
        store(2).start()
        pull = DPO_BETA * LOSS_SCALE / (1.0 + jnp.exp(margin))
        signed = jnp.where(even, -pull, pull)
        coefficients = jnp.sum(jnp.where(chosen, signed, 0.0), axis=0, keepdims=True)
        lane128 = lax.broadcasted_iota(jnp.int32, (1, 128), 1)
        coefficient = jnp.zeros((1, 384), F32)
        for s in range(3):
            own = jnp.sum(jnp.where(lane128 == 3 * rank + s, coefficients, 0.0), axis=1, keepdims=True)
            coefficient = jnp.where((lane >= 96 * s) & (lane < 96 * s + 96), own, coefficient)
        rows_to_columns(r.coefficient, [coefficient * living])
        yield

    def meanwhile():
        yield from layer_outputs()
        yield from preference()

    together(back_gather.steps(), meanwhile(), (1, 1, 0, 0, 0, 0, 0, 1, 0, 0, 0, 0, 0, 0, 0))
    unpack_features(r.grad_buf, SHARD, 0, r.normed, 0)

    for i in range(3):
        total = None
        for c in range(3 * i, 3 * i + 3):
            term = dot(r.normed[0:TOK, 512 * c : 512 * c + 512], r.w_back[512 * c : 512 * c + 512, :])
            total = term if total is None else total + term
        r.grad_mixed[...] = total if i == 0 else r.grad_mixed[...] + total
    r.grad_mixed[...] *= r.coefficient[0:TOK, 0:1]

    for i in range(3):
        here = slice(96 * i, 96 * i + 96)
        at = slice(TOK + 96 * i, TOK + 96 * i + 96)
        cos, sin = r.cosine[...], r.sine[...]
        key, value = r.heads[at, 256:384], r.heads[at, 384:512]
        key_grad = jnp.zeros((96, HEAD), F32)
        value_grad = jnp.zeros((96, HEAD), F32)
        for g in range(2):
            query = r.heads[at, 128 * g : 128 * g + 128]
            incoming = r.grad_mixed[here, 128 * g : 128 * g + 128].astype(BF16)
            prob = r.probs[at, 128 * g : 128 * g + 96]
            cap = r.capped[at, 128 * g : 128 * g + 96] / SOFT_CAP
            grad_probs = dot(incoming, value, NT)
            value_grad = value_grad + dot(prob.astype(BF16), incoming, TN)
            centered = grad_probs - jnp.sum(grad_probs * prob, axis=1, keepdims=True)
            grad_scores = (prob * centered * (1.0 - cap * cap) * QUERY_SCALE).astype(BF16)
            query_grad = dot(grad_scores, key)
            key_grad = key_grad + dot(grad_scores, query, TN)
            r.grads[here, 128 * g : 128 * g + 128] = rope(query_grad, cos, -sin).astype(BF16)
        r.grads[here, 256:384] = rope(key_grad, cos, -sin).astype(BF16)
        r.grads[here, 384:512] = value_grad.astype(BF16)

    query_factor = jnp.concatenate([r.b_query[...], jnp.zeros((RANK, 256), BF16)], axis=0)
    value_factor = jnp.concatenate([jnp.zeros((RANK, 128), BF16), r.b_value[...]], axis=0)
    hook = dot(r.grads[:, 0:256], query_factor, NT) + dot(r.grads[:, 384:512], value_factor, NT)
    r.grads[:, 512:640] = (ADAPTER_SCALE * hook).astype(BF16)
    r.hooks[...] = r.grads[:, 512:640]
    hooks = HookSum(
        r.hooks,
        r.hook_parts,
        r.hook_sums,
        mine,
        send.hooks,
        recv.hooks,
        send.hook_sums,
        recv.hook_sums,
    )
    hooks.start()
    stats_back = Exchange(r.stats_back, 8, 16, mine, in_tensor, send.stats_back, recv.stats_back)
    factors = Exchange(r.factors, 64, 8, rank, in_data, send.factors, recv.factors)
    for _ in partial_products(r.grads, r.w_in, r.partial_back):
        pass
    back_scatter = Scatter(
        r.partial_back, r.landing_back, SHARD, send.scatter_back, recv.scatter_back
    )
    back_scatter.begin((0,))
    hooks.reduce()
    back_scatter.begin((1, 2, 3))

    def across(i):
        return pltpu.make_async_remote_copy(
            src_ref=r.a_terms.at[pl.ds(aligned(576 * (2 * i + 1 - core), 64), 576), :],
            dst_ref=r.a_across.at[pl.ds(576 * i, 576), :],
            send_sem=send.across.at[0],
            recv_sem=recv.across.at[0],
            device_id={CORE: 1 - core},
            device_id_type=MESH,
        )

    def round_y(i):
        to = lax.rem(y + i, 4)
        return pltpu.make_async_remote_copy(
            src_ref=r.a_pairs.at[pl.ds(aligned(576 * to, 64), 576), :],
            dst_ref=r.a_round.at[pl.ds(576 * i, 576), :],
            send_sem=send.round.at[0],
            recv_sem=recv.round.at[0],
            device_id={Y: to},
            device_id_type=MESH,
        )

    def all_bytes(sent, arrived, buffer, count):
        whole = buffer.at[pl.ds(0, 576 * count), :]
        return pltpu.make_async_remote_copy(
            src_ref=whole,
            dst_ref=whole,
            send_sem=sent.at[0],
            recv_sem=arrived.at[0],
            device_id={CORE: 1 - core},
            device_id_type=MESH,
        )

    def adapters_back():
        pull_back = jnp.sum(r.grads[...].astype(F32) * r.linear[...], axis=1, keepdims=True)
        row = columns_to_rows(r.table, [pull_back])[0:1]
        row = [row[:, 128 * c : 128 * c + 128] for c in range(3)] + [jnp.zeros((5, 128), F32)]
        r.stats_back[pl.ds(aligned(8 * mine, 8), 8), :] = jnp.concatenate(row, axis=0)
        stats_back.start()
        factor_terms = ADAPTER_SCALE * dot(r.low[...], r.grads[:, 0:512], TN)
        own_factor = pl.ds(aligned(64 * rank, 64), 64)
        r.factors[own_factor, 0:256] = factor_terms[0:64, 0:256].astype(BF16)
        r.factors[own_factor, 256:384] = factor_terms[64:128, 384:512].astype(BF16)
        factors.start()
        yield
        hooks.wait()
        hook_low = r.hook_sums[...]
        for q in range(4):
            at = MAIN + 128 * q
            tail = dot(r.normed[TOK : 2 * TOK, at : at + 128], hook_low, TN).astype(BF16)
            for t in range(4 * q, 4 * q + 4):
                term = dot(r.normed[TOK : 2 * TOK, 256 * t : 256 * t + 256], hook_low, TN)
                r.a_terms[288 * t : 288 * t + 256, :] = term.astype(BF16)
                j = t - 4 * q
                r.a_terms[288 * t + 256 : 288 * t + 288, :] = tail[32 * j : 32 * j + 32, :]
            across(q).start()
            yield
        all_bytes(send.across, recv.across, r.a_across, 4).wait_recv()
        for i in range(4):
            own = r.a_terms[pl.ds(aligned(576 * (2 * i + core), 64), 576), :].astype(F32)
            pair = own + r.a_across[576 * i : 576 * i + 576, :].astype(F32)
            r.a_pairs[576 * i : 576 * i + 576, :] = pair.astype(BF16)
        for i in range(1, 4):
            round_y(i).start()
        yield

    adapters = adapters_back()
    fill(adapters, 1)
    together(back_scatter.steps(r.result.at[0]), adapters, (0, 0, 1, 1, 1, 1, 0, 1, 0, 0, 0, 0, 0))

    stats_back.wait()
    row = stats_back.total()
    rows_to_columns(r.table, [jnp.concatenate([row[c : c + 1] for c in range(3)], axis=1)])
    unpack_result(r.result.at[0], 0, r.summed.at[1])
    pre_scale = r.scale[TOK : 2 * TOK, 0:1]
    shrink_back = pre_scale * pre_scale * r.table[0:TOK, 0:1] / WIDTH
    grad_result = r.coefficient[0:TOK, 0:1] * r.readout[...].astype(F32)
    hidden = r.pol_hidden[...].astype(F32)
    r.grad_hidden[...] = (
        grad_result + pre_scale * pre_gain * r.summed[1] - hidden * shrink_back
    ).astype(BF16)
    store(3).start()
    factors.wait()
    factor_total = factors.total()
    r.query_grad[...] = factor_total[:, 0:256]
    r.value_grad[...] = factor_total[:, 256:384]
    store(5).start()
    store(6).start()
    whole = r.a_pairs[pl.ds(aligned(576 * y, 64), 576), :].astype(F32)
    all_bytes(send.round, recv.round, r.a_round, 3).wait_recv()
    for i in range(1, 4):
        whole = whole + r.a_round[576 * i : 576 * i + 576, :].astype(F32)
    r.grad_a[...] = whole
    store(4).start()
    for ring in (gather, weights, ref_scatter, pol_scatter, back_gather, back_scatter):
        ring.drain()
    for exchange in (ref_stats, pol_stats, scores, hooks, stats_back, factors):
        exchange.drain()
    all_bytes(send.across, recv.across, r.a_across, 4).wait_send()
    all_bytes(send.round, recv.round, r.a_round, 3).wait_send()
    for number in range(len(outputs)):
        store(number).wait()


def partial_products(rows, matrix, partial):
    for block in range(4):
        left = rows[...]
        for t in range(4 * block, 4 * block + 4):
            product = dot(left, matrix[256 * t : 256 * t + 256, :], NT).astype(BF16)
            for half in range(2):
                at = t * SHARD + TOK * half
                partial[at : at + TOK, :] = product[:, 128 * half : 128 * half + 128]
        at = MAIN + 128 * block
        product = dot(left, matrix[at : at + 128, :], NT).astype(BF16)
        for j in range(4):
            at = (4 * block + j) * SHARD + 2 * TOK
            partial[at : at + GROUP, :] = pack_tail(product[:, 32 * j : 32 * j + 32])
        yield


def rotation_tables():
    spacing = ROPE_BASE ** (-2.0 * np.arange(64, dtype=np.float32) / HEAD)
    angles = np.arange(LENGTH, dtype=np.float32)[:, None] * spacing.astype(np.float32)[None, :]
    cosine, sine = np.cos(angles), np.sin(angles)
    return (
        np.concatenate([cosine, cosine], axis=1).astype(np.float32),
        np.concatenate([-sine, sine], axis=1).astype(np.float32),
    )


INPUTS = dict(
    lengths=None,
    pairing=None,
    ref_hidden=((TOK, TOK), BF16),
    pol_hidden=((TOK, TOK), BF16),
    w_query=((576, 256), BF16),
    w_key=((576, 128), BF16),
    w_value=((576, 128), BF16),
    w_out=((576, 256), BF16),
    a_query=((RANK, 576), BF16),
    a_value=((RANK, 576), BF16),
    readout=((TOK, TOK), BF16),
    b_query=((RANK, 256), BF16),
    b_value=((RANK, 128), BF16),
    pre_gain=((36, 128), F32),
    post_gain=((36, 128), F32),
    cosine=((LENGTH, HEAD), F32),
    sine=((LENGTH, HEAD), F32),
)
OUTPUTS = dict(
    pol_out=((TOK, TOK), BF16),
    ref_out=((TOK, TOK), BF16),
    loss=((8, 128), F32),
    grad_hidden=((TOK, TOK), BF16),
    grad_a=((576, 128), F32),
    query_grad=((RANK, 256), F32),
    value_grad=((RANK, 128), F32),
)


def hand_out(*refs):
    for source, target in zip(refs[: len(OUTPUTS)], refs[len(OUTPUTS) :]):
        target[...] = source[0 : target.shape[0], 0 : target.shape[1]]


def body(
    ref_hidden,
    pol_hidden,
    readout,
    lengths,
    pairing,
    pre_gain,
    post_gain,
    w_query,
    w_key,
    value_projection,
    w_out,
    a_query,
    a_value,
    query_second_factor,
    value_second_factor,
):
    vmem, whole = pl.BlockSpec(memory_space=pltpu.VMEM), pl.BlockSpec(memory_space=pl.ANY)
    cosine, sine = rotation_tables()
    dma = pltpu.SemaphoreType.DMA
    staged = [pltpu.VMEM(*kind) if kind else None for kind in list(INPUTS.values()) + list(OUTPUTS.values())]
    staged[0:2] = [pltpu.SMEM((3,), jnp.int32), pltpu.SMEM((24,), jnp.int32)]
    results = pl.pallas_call(
        step_body,
        out_shape=tuple(jax.ShapeDtypeStruct(*kind) for kind in OUTPUTS.values()),
        in_specs=[whole] * len(INPUTS),
        out_specs=(whole,) * len(OUTPUTS),
        scratch_shapes=staged
        + [pltpu.VMEM(shape, kind) for shape, kind in SCRATCH.values()]
        + [dma((len(INPUTS),)), dma((len(OUTPUTS),))]
        + [dma((count,)) for pair in SEMAPHORES.values() for count in pair],
        compiler_params=pltpu.CompilerParams(
            collective_id=0, has_side_effects=True, vmem_limit_bytes=62 * 1024 * 1024
        ),
    )(
        lengths,
        pairing,
        ref_hidden,
        pol_hidden,
        w_query,
        w_key,
        value_projection,
        w_out,
        a_query.T,
        a_value.T,
        readout,
        query_second_factor,
        value_second_factor,
        pre_gain.reshape(36, 128),
        post_gain.reshape(36, 128),
        jnp.asarray(cosine),
        jnp.asarray(sine),
    )
    shapes = [jax.ShapeDtypeStruct(a.shape, a.dtype) for a in results]
    shapes[2] = jax.ShapeDtypeStruct((1, 1), F32)
    pol_out, ref_out, loss, grad_hidden, grad_a, query_grad, value_grad = pl.pallas_call(
        hand_out,
        out_shape=tuple(shapes),
        in_specs=[vmem] * len(OUTPUTS),
        out_specs=(vmem,) * len(OUTPUTS),
    )(*results)
    return (pol_out, ref_out, loss.reshape(()), grad_hidden, grad_a, query_grad, value_grad)


def solution(mesh):
    torus = Mesh(mesh.devices.reshape(4, 2, 4, 4), (Y, CORE, X, Z))
    split, rows, columns = P(DP, TENSOR), P(DP, None), P(None, TENSOR)
    return jax.shard_map(
        body,
        mesh=torus,
        in_specs=(split, split, split, P(DP), P(), P(), P(), split, split, split, split, rows, rows, columns, columns),
        out_specs=(split, split, P(), split, rows, columns, columns),
        check_vma=False,
    )
```

```python
import jax
import jax.numpy as jnp
import numpy as np
from jax import lax
from jax.experimental import pallas as pl
from jax.experimental.pallas import tpu as pltpu
from jax.sharding import Mesh
from jax.sharding import PartitionSpec as P

Y, CORE, X, Z = "dp_0", "dp_1", "tensor_0", "tensor_1"
DP, TENSOR = (Y, CORE), (X, Z)
MESH = pl.DeviceIdType.MESH

WIDTH = 4608
TOK = 288
LENGTH = 96
HEAD = 128
RANK = 64
NORM_EPS = 1e-06
SOFT_CAP = 50.0
ADAPTER_SCALE = 0.5
DPO_BETA = 0.5
LOSS_SCALE = 256.0
ROPE_BASE = 10000.0
QUERY_SCALE = float(WIDTH // 32) ** (-0.5)

GROUP = 80
SHARD = 2 * TOK + GROUP
MAIN = 4096
RINGS = ((0, 1), (0, -1), (1, 1), (1, -1))

ORDER = (2, 1, 3, 0)

F32 = jnp.float32
BF16 = jnp.bfloat16
NT = (((1,), (1,)), ((), ()))
TN = (((0,), (0,)), ((), ()))


def dot(a, b, dims=(((1,), (0,)), ((), ())), precision=None):
    return lax.dot_general(a, b, dims, preferred_element_type=F32, precision=precision)


def aligned(start, multiple):
    return start if isinstance(start, int) else pl.multiple_of(start, multiple)


def back(position, hops, direction):
    return lax.rem(position - hops * direction + 8, 4)


def chunks_of(rows):
    tiles = rows // 16
    sizes = [16 * (tiles // 4 + (1 if k < tiles % 4 else 0)) for k in range(4)]
    return sizes, [sum(sizes[:k]) for k in range(4)]


class Ring:
    def __init__(self, rows, send, recv):
        self.rows = rows
        self.sizes, self.starts = chunks_of(rows)
        self.send, self.recv = send, recv
        self.at = (lax.axis_index(X), lax.axis_index(Z))

    def place(self, k, first, second):
        primary, way = RINGS[k]
        a = back(self.at[primary], first, way)
        b = back(self.at[1 - primary], second, way)
        px, pz = (a, b) if primary == 0 else (b, a)
        return aligned((4 * px + pz) * self.rows + self.starts[k], 16)

    def next_on(self, k, secondary, behind=False):
        primary, way = RINGS[k]
        axis = 1 - primary if secondary else primary
        return {TENSOR[axis]: back(self.at[axis], 1 if behind else -1, way)}

    def remote(self, source, target, number, device):
        return pltpu.make_async_remote_copy(
            src_ref=source,
            dst_ref=target,
            send_sem=self.send.at[0],
            recv_sem=self.recv.at[number],
            device_id=device,
            device_id_type=MESH,
        )

    def arrived(self, number):
        whole = self.memory.at[pl.ds(0, self.rows), :]
        self.remote(whole, whole, number, self.next_on(0, False)).wait_recv()

    def drain(self):
        whole = self.memory.at[pl.ds(0, 15 * self.rows), :]
        self.remote(whole, whole, 0, self.next_on(0, False)).wait_send()


class Gather(Ring):
    def __init__(self, buffer, rows, send, recv):
        super().__init__(rows, send, recv)
        self.memory = buffer

    def piece(self, k, j, s):
        return self.memory.at[pl.ds(self.place(k, j, s), self.sizes[k]), :]

    def first(self, k, number):
        piece = self.piece(k, 1 if number == 1 else 0, 0)
        return self.remote(piece, piece, number, self.next_on(k, False, number == 2))

    def second(self, k, j, s):
        piece = self.piece(k, j, s)
        return self.remote(piece, piece, 3 + 3 * j + s, self.next_on(k, True))

    def begin(self):
        for k in range(4):
            self.first(k, 0).start()
            self.first(k, 2).start()
        for k in range(4):
            self.second(k, 0, 0).start()

    def await_first(self, number):
        self.arrived(number)
        for k in range(4):
            if number == 0:
                self.first(k, 1).start()
            self.second(k, number + 1, 0).start()

    def await_second(self, j, s):
        self.arrived(3 + 3 * j + s)
        if s < 2:
            for k in range(4):
                self.second(k, j, s + 1).start()

    def steps(self):
        self.await_first(0)
        yield
        self.await_first(2)
        yield
        self.await_second(0, 0)
        yield
        self.await_first(1)
        yield
        for j, s in ((1, 0), (3, 0), (0, 1), (2, 0), (1, 1), (3, 1), (0, 2), (2, 1), (1, 2), (3, 2), (2, 2)):
            self.await_second(j, s)
            yield


class Scatter(Ring):
    def __init__(self, partial, landing, rows, send, recv):
        super().__init__(rows, send, recv)
        self.partial, self.landing, self.memory = partial, landing, landing

    def piece(self, k, first, second):
        return self.partial.at[pl.ds(self.place(k, first, second), self.sizes[k]), :]

    def slot(self, k, number):
        return self.landing.at[pl.ds(15 * self.starts[k] + number * self.sizes[k], self.sizes[k]), :]

    def outer(self, k, j, s):
        number = 3 * j + s
        return self.remote(self.piece(k, ORDER[j], s + 1), self.slot(k, number), number, self.next_on(k, True))

    def inner(self, k, number):
        piece = self.piece(k, (2, 3, 1)[number - 12], 0)
        return self.remote(piece, self.slot(k, number), number, self.next_on(k, False, number == 14))

    def add(self, k, number, first, second):
        piece, slot = self.piece(k, first, second), self.slot(k, number)
        piece[...] = (piece[...].astype(F32) + slot[...].astype(F32)).astype(BF16)

    def begin(self, parts=range(4)):
        for j in parts:
            for k in range(4):
                self.outer(k, j, 0).start()

    def steps(self, result):
        for s in range(3):
            for j in range(4):
                self.arrived(3 * j + s)
                if s == 2 and j == 2:
                    self.arrived(12)
                for k in range(4):
                    self.add(k, 3 * j + s, ORDER[j], s + 2)
                    if s < 2:
                        self.outer(k, j, s + 1).start()
                    elif j == 0:
                        self.inner(k, 12).start()
                    elif j == 1:
                        self.inner(k, 14).start()
                    elif j == 2:
                        self.add(k, 12, 3, 0)
                        self.inner(k, 13).start()
                yield
        self.arrived(14)
        self.arrived(13)
        for k in range(4):
            own = self.piece(k, 0, 0)[...].astype(F32)
            for number in (14, 13):
                own = own + self.slot(k, number)[...].astype(F32)
            result[pl.ds(self.starts[k], self.sizes[k]), :] = own
        yield


class Weights:
    def __init__(self, w_in, w_back, y_send, y_recv, d_send, d_recv):
        self.w_in, self.w_back = w_in, w_back
        self.sems = (y_send, y_recv, d_send, d_recv)
        self.y, self.core = lax.axis_index(Y), lax.axis_index(CORE)

    def block(self, hops, half, part, core):
        way = 1 - 2 * half
        tile = 2 * (2 * back(self.y, hops, way) + core) + half
        if part < 2:
            return self.w_in.at[pl.ds(aligned(256 * tile + 128 * part, 128), 128), :]
        if part == 3:
            return self.w_back.at[pl.ds(aligned(256 * tile, 256), 256), :]
        ref = self.w_in if part == 2 else self.w_back
        return ref.at[pl.ds(aligned(MAIN + 32 * tile, 32), 32), :]

    def round(self, s, half, part):
        ref = self.block(s, half, part, self.core)
        return self.copy(ref, 0, part, 5 * s + part, {Y: back(self.y, -1, 1 - 2 * half)})

    def across(self, i, half, part):
        return self.copy(self.block(i, half, part, self.core), 2, part, part // 3, {CORE: 1 - self.core})

    def copy(self, ref, way, part, number, device):
        return pltpu.make_async_remote_copy(
            src_ref=ref,
            dst_ref=ref,
            send_sem=self.sems[way].at[part // 3],
            recv_sem=self.sems[way + 1].at[number],
            device_id=device,
            device_id_type=MESH,
        )

    def rows(self, part, count):
        return (self.w_in if part < 3 else self.w_back).at[pl.ds(0, count), :]

    def step(self, s, parts):
        for part in parts:
            if s > 0:
                both = self.rows(part, 2 * (128, 128, 32, 256, 32)[part])
                self.copy(both, 0, part, 5 * (s - 1) + part, {CORE: 1 - self.core}).wait_recv()
            for half in range(2):
                if s < 3:
                    self.round(s, half, part).start()
                self.across(s, half, part).start()

    def arrive(self, part):
        self.copy(self.rows(part, 8 * TOK), 2, part, part // 3, {CORE: 1 - self.core}).wait_recv()

    def drain(self):
        for part in (0, 3):
            self.copy(self.rows(part, 6 * TOK), 0, part, 0, {CORE: 1 - self.core}).wait_send()
            self.copy(self.rows(part, 8 * TOK), 2, part, 0, {CORE: 1 - self.core}).wait_send()


class Exchange:
    def __init__(self, buffer, rows, count, me, device_of, send, recv):
        self.buffer, self.rows, self.count, self.me = buffer, rows, count, me
        self.device_of, self.send, self.recv = device_of, send, recv

    def part(self, buffer, i):
        return buffer.at[pl.ds(aligned(i * self.rows, self.rows), self.rows), :]

    def copy(self, source, target, peer):
        return pltpu.make_async_remote_copy(
            src_ref=source,
            dst_ref=target,
            send_sem=self.send.at[0],
            recv_sem=self.recv.at[0],
            device_id=self.device_of(peer),
            device_id_type=MESH,
        )

    def start(self):
        own = self.part(self.buffer, self.me)
        for delta in range(1, self.count):
            self.copy(own, own, lax.rem(self.me + delta, self.count)).start()

    def slots(self, count):
        whole = self.buffer.at[pl.ds(0, count * self.rows), :]
        return self.copy(whole, whole, lax.rem(self.me + 1, self.count))

    def wait(self):
        self.slots(self.count - 1).wait_recv()

    def total(self):
        value = self.buffer[0 : self.rows, :].astype(F32)
        for i in range(1, self.count):
            value = value + self.buffer[self.rows * i : self.rows * i + self.rows, :].astype(F32)
        return value

    def drain(self):
        self.slots(self.count - 1).wait_send()


OWNERS = 9


class HookSum:
    def __init__(self, terms, parts, sums, me, send_parts, recv_parts, send_sums, recv_sums):
        self.terms, self.parts, self.sums, self.me = terms, parts, sums, me
        self.there = Exchange(parts, 32, 16, me, in_tensor, send_parts, recv_parts)
        self.home = Exchange(parts, 32, 16, me, in_tensor, send_sums, recv_sums)
        self.owner = me < OWNERS

    def start(self):
        @pl.when(self.owner)
        def _():
            own = pl.ds(aligned(32 * self.me, 32), 32)
            self.parts[own, :] = self.terms[own, :]

        for delta in range(1, 16):
            peer = lax.rem(self.me + delta, 16)

            @pl.when(peer < OWNERS)
            def _():
                self.there.copy(self.there.part(self.terms, peer), self.there.part(self.parts, self.me), peer).start()

    def reduce(self):
        @pl.when(self.owner)
        def _():
            self.there.wait()
            self.sums[pl.ds(aligned(32 * self.me, 32), 32), :] = self.there.total().astype(BF16)
            own = self.home.part(self.sums, self.me)
            for delta in range(1, 16):
                self.home.copy(own, own, lax.rem(self.me + delta, 16)).start()

    def wait(self):
        @pl.when(self.owner)
        def _():
            self.home.slots(OWNERS - 1).wait_recv()

        @pl.when(jnp.logical_not(self.owner))
        def _():
            self.home.slots(OWNERS).wait_recv()

    def drain(self):
        @pl.when(self.owner)
        def _():
            self.there.slots(OWNERS - 1).wait_send()
            self.home.slots(15).wait_send()

        @pl.when(jnp.logical_not(self.owner))
        def _():
            self.there.slots(OWNERS).wait_send()


def in_tensor(i):
    return {X: lax.div(i, 4), Z: lax.rem(i, 4)}


def in_data(i):
    return {Y: lax.div(i, 2), CORE: lax.rem(i, 2)}


def together(main, filler, ratio):
    for number, _ in enumerate(main):
        for _ in range(ratio if isinstance(ratio, int) else ratio[number]):
            next(filler, None)
    for _ in filler:
        pass


def signal(peers):
    barrier = pltpu.get_barrier_semaphore()
    for peer in peers:
        pl.semaphore_signal(barrier, inc=1, device_id=peer, device_id_type=MESH)


def pack_tail(tail):
    last = jnp.concatenate([tail[240:288], jnp.zeros((32, 32), tail.dtype)], axis=0)
    return jnp.concatenate([tail[0:80], tail[80:160], tail[160:240], last], axis=1)


GROUPS = ((0, 80), (80, 80), (160, 80), (240, 48))


def unpack_features(buffer, rows, offset, target, row_offset):
    def main(t, carry):
        base = aligned(t * rows + offset, 16)
        for half in range(2):
            target[pl.ds(row_offset, TOK), pl.ds(aligned(256 * t + 128 * half, 128), 128)] = buffer[
                pl.ds(aligned(base + TOK * half, 16), TOK), :
            ]
        return carry

    lax.fori_loop(0, 16, main, 0)

    def tail(q, carry):
        tails = [
            buffer[pl.ds(aligned((4 * q + j) * rows + offset + 2 * TOK, 16), GROUP), :] for j in range(4)
        ]
        for g, (start, size) in enumerate(GROUPS):
            joined = jnp.concatenate([t[:size, 32 * g : 32 * g + 32] for t in tails], axis=1)
            target[pl.ds(row_offset + start, size), pl.ds(aligned(MAIN + 128 * q, 128), 128)] = joined
        return carry

    lax.fori_loop(0, 4, tail, 0)


def unpack_result(packed, offset, target):
    for half in range(2):
        target[:, 128 * half : 128 * half + 128] = packed[offset + TOK * half : offset + TOK * half + TOK, :]
    for g, (start, size) in enumerate(GROUPS):
        base = offset + 2 * TOK
        target[start : start + size, 256:288] = packed[base : base + size, 32 * g : 32 * g + 32]


def pack_hidden(hidden, buffer, base):
    for half in range(2):
        buffer[pl.ds(aligned(base + TOK * half, 16), TOK), :] = hidden[:, 128 * half : 128 * half + 128].astype(
            BF16
        )
    buffer[pl.ds(aligned(base + 2 * TOK, 16), GROUP), :] = pack_tail(hidden[:, 256:288]).astype(BF16)


def feature_lanes(gain, start, count):
    pieces = []
    while count:
        row, lane = divmod(start, 128)
        size = min(count, 128 - lane)
        pieces.append(gain[row : row + 1, lane : lane + size])
        start, count = start + size, count - size
    return pieces[0] if len(pieces) == 1 else jnp.concatenate(pieces, axis=1)


def order_gain(gain, target):
    for c in range(32):
        target[c : c + 1, :] = feature_lanes(gain, 288 * (c // 2) + 128 * (c % 2), 128)
    for q in range(4):
        tails = [feature_lanes(gain, 288 * (4 * q + j) + 256, 32) for j in range(4)]
        target[32 + q : 33 + q, :] = jnp.concatenate(tails, axis=1)


def own_gain(ordered, mine):
    tail = ordered[pl.ds(32 + lax.div(mine, 4), 1), :]
    picked = jnp.zeros((1, 32), F32)
    for j in range(4):
        picked = jnp.where(lax.rem(mine, 4) == j, tail[:, 32 * j : 32 * j + 32], picked)
    return jnp.concatenate([ordered[pl.ds(2 * mine, 1), :], ordered[pl.ds(2 * mine + 1, 1), :], picked], axis=1)


def normalize(normed, scale_ref, gain_ref, offset):
    def rows(i, carry):
        at = pl.ds(aligned(offset + 96 * i, 96), 96)
        squares = jnp.zeros((96, 128), F32)
        for c in range(36):
            x = normed[at, 128 * c : 128 * c + 128].astype(F32)
            squares = squares + x * x
        scale = lax.rsqrt(jnp.sum(squares, axis=1, keepdims=True) / WIDTH + NORM_EPS)
        scale_ref[at, :] = jnp.broadcast_to(scale, (96, 128))
        for c in range(36):
            x = normed[at, 128 * c : 128 * c + 128].astype(F32)
            normed[at, 128 * c : 128 * c + 128] = (x * scale * gain_ref[c : c + 1, :]).astype(BF16)
        return carry

    lax.fori_loop(0, 3, rows, 0)


def rope(x, cosine, sine):
    return x * cosine + pltpu.roll(x, 64, 1) * sine


def allowed_here(length):
    query = lax.broadcasted_iota(jnp.int32, (LENGTH, LENGTH), 0)
    key = lax.broadcasted_iota(jnp.int32, (LENGTH, LENGTH), 1)
    return (key <= query) & (key < length)


def columns_to_rows(scratch, columns):
    lane = lax.broadcasted_iota(jnp.int32, (TOK, 128), 1)
    table = jnp.zeros((TOK, 128), F32)
    for k, column in enumerate(columns):
        table = jnp.where(lane == k, column, table)
    scratch[0:TOK, :] = table
    scratch[TOK:384, :] = jnp.zeros((384 - TOK, 128), F32)
    return jnp.transpose(scratch[...])[0:8, :]


def as_tile(row):
    pieces = [row[:, 128 * c : 128 * c + 128] for c in range(3)]
    return jnp.concatenate(pieces + [jnp.zeros((5, 128), F32)], axis=0)


def as_row(tile):
    return jnp.concatenate([tile[c : c + 1] for c in range(3)], axis=1)


def rows_to_columns(scratch, rows):
    missing = 128 - sum(row.shape[0] for row in rows)
    filled = jnp.concatenate(list(rows) + [jnp.zeros((missing, 384), F32)], axis=0)
    scratch[...] = jnp.transpose(filled)


SCRATCH = dict(
    ref_gathered=((16 * SHARD, 128), BF16),
    pol_gathered=((16 * SHARD, 128), BF16),
    w_in=((WIDTH, 512), BF16),
    a_all=((640, 128), BF16),
    a_own=((TOK, 128), BF16),
    w_back=((WIDTH, 256), BF16),
    normed=((2 * TOK, WIDTH), BF16),
    scale=((2 * TOK, 128), F32),
    acc=((2 * TOK, 512), F32),
    linear=((TOK, 512), F32),
    pre_stats=((16 * 8, 128), F32),
    own_normed=((TOK, TOK), BF16),
    low_terms=((TOK, 128), BF16),
    low_parts=((16 * 32, 128), BF16),
    low=((TOK, 128), BF16),
    heads=((2 * TOK, 512), BF16),
    mixed=((2 * TOK, 256), BF16),
    probs=((2 * TOK, 256), F32),
    capped=((2 * TOK, 256), F32),
    partial=((16 * SHARD, 128), BF16),
    partial_pol=((16 * SHARD, 128), BF16),
    landing=((15 * SHARD, 128), BF16),
    landing_pol=((15 * SHARD, 128), BF16),
    result=((2, SHARD, 128), F32),
    summed=((2, TOK, TOK), F32),
    table=((384, 128), F32),
    coefficient=((384, 128), F32),
    ref_stats=((16 * 8, 384), F32),
    pol_stats=((16 * 16, 128), F32),
    pre_ordered=((40, 128), F32),
    post_ordered=((40, 128), F32),
    scores=((8 * 8, 128), F32),
    grad_buf=((16 * SHARD, 128), BF16),
    grad_mixed=((TOK, 256), F32),
    grads=((TOK, 512), BF16),
    partial_back=((16 * SHARD, 128), BF16),
    landing_back=((15 * SHARD, 128), BF16),
    hooks=((TOK, 128), BF16),
    hook_parts=((16 * 32, 128), BF16),
    hook_sums=((TOK, 128), BF16),
    stats_back=((16 * 8, 128), F32),
    factors=((8 * 64, 384), BF16),
    a_terms=((WIDTH, 128), BF16),
    a_across=((4 * 576, 128), BF16),
    a_pairs=((4 * 576, 128), BF16),
    a_round=((4 * 576, 128), BF16),
)
SEMAPHORES = dict(
    gather_ref=(1, 15),
    gather_pol=(1, 15),
    a=(1, 1),
    pre_stats=(1, 1),
    low_terms=(1, 1),
    low=(1, 1),
    scatter_ref=(1, 15),
    scatter_pol=(1, 15),
    gather_back=(1, 15),
    scatter_back=(1, 15),
    y=(2, 15),
    d=(2, 2),
    ref_stats=(1, 1),
    pol_stats=(1, 1),
    scores=(1, 1),
    hooks=(1, 1),
    hook_sums=(1, 1),
    stats_back=(1, 1),
    factors=(1, 1),
    across=(4, 4),
    round=(1, 1),
)


class Refs:
    pass


def step_body(*refs):
    inputs, outputs = list(INPUTS), list(OUTPUTS)
    outside, refs = refs[: len(inputs + outputs)], refs[len(inputs + outputs) :]
    names = inputs + outputs + list(SCRATCH)
    r, send, recv = Refs(), Refs(), Refs()
    for name, ref in zip(names, refs):
        setattr(r, name, ref)
    load_sems, store_sems, *sems = refs[len(names) :]
    for number, name in enumerate(SEMAPHORES):
        setattr(send, name, sems[2 * number])
        setattr(recv, name, sems[2 * number + 1])

    x, z = lax.axis_index(X), lax.axis_index(Z)
    y, core = lax.axis_index(Y), lax.axis_index(CORE)
    mine, rank = 4 * x + z, 2 * y + core
    def load(number):
        return pltpu.make_async_copy(outside[number], refs[number], load_sems.at[number])

    def store(number):
        at = len(inputs) + number
        return pltpu.make_async_copy(refs[at], outside[at], store_sems.at[number])

    signal(
        [in_tensor(lax.rem(mine + i, 16)) for i in range(1, 16)]
        + [in_data(lax.rem(rank + i, 8)) for i in range(1, 8)]
    )
    for number in range(len(inputs)):
        load(number).start()
    for number in range(10):
        load(number).wait()
    pack_hidden(r.ref_hidden[...], r.ref_gathered, mine * SHARD)
    pack_hidden(r.pol_hidden[...], r.pol_gathered, mine * SHARD)
    a_both = jnp.concatenate([r.a_query[...].astype(F32), r.a_value[...].astype(F32)], axis=0)
    r.a_all[...] = jnp.transpose(jnp.concatenate([a_both, jnp.zeros((128, 64), F32)], axis=1)).astype(BF16)
    a_rank = lax.div(mine, 2)
    a_here, a_core = rank == a_rank, core == lax.rem(a_rank, 2)
    a_relay = a_core & (y != lax.div(a_rank, 2))
    a_rows = pl.ds(aligned(TOK * lax.rem(mine, 2), 32), TOK)

    @pl.when(a_here)
    def _():
        r.a_own[...] = r.a_all[a_rows, :]

    def a_copy(source, target, device):
        return pltpu.make_async_remote_copy(
            src_ref=source,
            dst_ref=target,
            send_sem=send.a.at[0],
            recv_sem=recv.a.at[0],
            device_id=device,
            device_id_type=MESH,
        )

    def send_a():
        @pl.when(a_here)
        def _():
            for device in [{Y: lax.rem(y + i, 4)} for i in (1, 3, 2)] + [{CORE: 1 - core}]:
                a_copy(r.a_all.at[a_rows, :], r.a_own, device).start()

    def relay_a():
        @pl.when(a_relay)
        def _():
            a_copy(r.a_own, r.a_own, {CORE: 1 - core}).wait_recv()
            a_copy(r.a_own, r.a_own, {CORE: 1 - core}).start()

    def await_a():
        @pl.when(jnp.logical_not(a_core))
        def _():
            a_copy(r.a_own, r.a_own, {CORE: 1 - core}).wait_recv()

    def drain_a():
        @pl.when(a_here)
        def _():
            whole = r.ref_gathered.at[pl.ds(0, 4 * TOK), :]
            a_copy(whole, whole, {CORE: 1 - core}).wait_send()

        @pl.when(a_relay)
        def _():
            a_copy(r.a_own, r.a_own, {CORE: 1 - core}).wait_send()

    pre_stats = Exchange(r.pre_stats, 8, 16, mine, in_tensor, send.pre_stats, recv.pre_stats)
    own_hidden = r.pol_hidden[...].astype(F32)
    row = columns_to_rows(r.table, [jnp.sum(own_hidden * own_hidden, axis=1, keepdims=True)])[0:1]
    r.pre_stats[pl.ds(aligned(8 * mine, 8), 8), :] = as_tile(row)
    for half in range(2):
        tile = 2 * rank + half
        for start, size, to in ((0, 256, 256 * tile), (256, 32, MAIN + 32 * tile)):
            here, there = pl.ds(288 * half + start, size), pl.ds(aligned(to, 32), size)
            r.w_in[there, 0:256] = r.w_query[here, :]
            r.w_in[there, 256:384] = r.w_key[here, :]
            r.w_in[there, 384:512] = r.w_value[here, :]
            r.w_back[there, :] = r.w_out[here, :]
    pl.semaphore_wait(pltpu.get_barrier_semaphore(), 22)

    ref_gather = Gather(r.ref_gathered, SHARD, send.gather_ref, recv.gather_ref)
    pol_gather = Gather(r.pol_gathered, SHARD, send.gather_pol, recv.gather_pol)
    weights = Weights(r.w_in, r.w_back, send.y, recv.y, send.d, recv.d)

    def weight_steps():
        for s in range(1, 3):
            weights.step(s, (0,))
            yield
            weights.step(s, (1,))
            if s == 1:
                weights.step(s, (2,))
            yield
        weights.step(2, (2,))
        weights.step(0, (3, 4))
        yield
        for part in range(3):
            weights.step(3, (part,))
            yield
        for s in range(1, 4):
            weights.step(s, (3, 4))
            yield

    pre_stats.start()
    ref_gather.begin()
    weights.step(0, (0, 1, 2))
    for number in range(10, len(inputs)):
        load(number).wait()
    gain = r.pre_ordered
    order_gain(r.pre_gain, gain)
    order_gain(r.post_gain, r.post_ordered)
    pre_gain, post_gain = own_gain(gain, mine), own_gain(r.post_ordered, mine)
    def project(m):
        rows = slice(m * TOK, m * TOK + TOK)
        for i in range(3):
            total = None
            for c in range(3 * i, 3 * i + 3):
                term = dot(r.normed[rows, 512 * c : 512 * c + 512], r.w_in[512 * c : 512 * c + 512, :])
                total = term if total is None else total + term
            r.acc[rows, :] = total if i == 0 else r.acc[rows, :] + total
            yield

    def attend(m):
        for i in range(3):
            at = slice(m * TOK + 96 * i, m * TOK + 96 * i + 96)
            cos, sin = r.cosine[...], r.sine[...]
            key = rope(r.acc[at, 256:384], cos, sin).astype(BF16)
            value = r.acc[at, 384:512].astype(BF16)
            allowed = allowed_here(r.lengths[i])
            r.heads[at, 256:384] = key
            r.heads[at, 384:512] = value
            for g in range(2):
                query = rope(r.acc[at, 128 * g : 128 * g + 128], cos, sin).astype(BF16)
                r.heads[at, 128 * g : 128 * g + 128] = query
                scores = dot(query, key, NT) * QUERY_SCALE
                cap = SOFT_CAP * jnp.tanh(scores / SOFT_CAP)
                weight = jnp.where(allowed, jnp.exp(cap), 0.0)
                prob = weight / jnp.sum(weight, axis=1, keepdims=True)
                r.probs[at, 128 * g : 128 * g + 96] = prob
                r.capped[at, 128 * g : 128 * g + 96] = cap
                r.mixed[at, 128 * g : 128 * g + 128] = dot(prob.astype(BF16), value).astype(BF16)
            yield

    def fill(steps, count):
        for _ in range(count):
            next(steps, None)

    def ref_work():
        unpack_features(r.ref_gathered, SHARD, 0, r.normed, 0)
        yield
        normalize(r.normed, r.scale, gain, 0)
        yield
        weights.arrive(0)
        yield from project(0)
        yield from attend(0)

    lows = HookSum(
        r.low_terms, r.low_parts, r.low, mine, send.low_terms, recv.low_terms, send.low, recv.low
    )

    def low_work():
        send_a()
        pre_stats.wait()
        rows_to_columns(r.table, [lax.rsqrt(as_row(pre_stats.total()) / WIDTH + NORM_EPS)])
        own = r.pol_hidden[...].astype(F32) * r.table[0:TOK, 0:1] * pre_gain
        r.own_normed[...] = own.astype(BF16)
        yield
        relay_a()
        yield
        await_a()
        r.low_terms[...] = dot(r.own_normed[...], r.a_own[...]).astype(BF16)
        lows.start()
        yield
        lows.reduce()
        yield

    low = low_work()
    first, second, passing, work = ref_gather.steps(), pol_gather.steps(), weight_steps(), ref_work()
    arrivals = dict(G=first, Q=second, V=passing, C=work, X=low)
    for letter in "GGGVPGGGVQGVQGVXQGVQGVXQGQGVXQVGQGVQGCQVCQCQCCQCQXCQCV":
        if letter == "P":
            pol_gather.begin()
        else:
            fill(arrivals[letter], 1)
    weights.arrive(3)
    for _ in partial_products(r.mixed.at[0:TOK], r.w_back, r.partial):
        pass
    ref_scatter = Scatter(r.partial, r.landing, SHARD, send.scatter_ref, recv.scatter_ref)
    ref_scatter.begin()
    pol_scatter = Scatter(r.partial_pol, r.landing_pol, SHARD, send.scatter_pol, recv.scatter_pol)

    def policy():
        unpack_features(r.pol_gathered, SHARD, 0, r.normed, TOK)
        yield
        normalize(r.normed, r.scale, gain, TOK)
        yield
        yield from project(1)
        r.linear[...] = r.acc[TOK : 2 * TOK, :]
        lows.wait()
        query_factor = jnp.concatenate([r.b_query[...], jnp.zeros((RANK, 256), BF16)], axis=0)
        value_factor = jnp.concatenate([jnp.zeros((RANK, 128), BF16), r.b_value[...]], axis=0)
        r.acc[TOK : 2 * TOK, 0:256] += ADAPTER_SCALE * dot(r.low[...], query_factor)
        r.acc[TOK : 2 * TOK, 384:512] += ADAPTER_SCALE * dot(r.low[...], value_factor)
        yield
        yield from attend(1)
        yield from partial_products(r.mixed.at[TOK : 2 * TOK], r.w_back, r.partial_pol)

    def token_sums(m, hidden):
        unpack_result(r.result.at[m], 0, r.summed.at[m])
        summed, readout = r.summed[m], r.readout[...].astype(F32)
        return [
            jnp.sum(summed * summed, axis=1, keepdims=True),
            jnp.sum(summed * post_gain * readout, axis=1, keepdims=True),
            jnp.sum(hidden[...].astype(F32) * readout, axis=1, keepdims=True),
        ]

    ref_stats = Exchange(r.ref_stats, 8, 16, mine, in_tensor, send.ref_stats, recv.ref_stats)
    pol_stats = Exchange(r.pol_stats, 16, 16, mine, in_tensor, send.pol_stats, recv.pol_stats)

    def policy_ring():
        yield from pol_scatter.steps(r.result.at[1])

    def after_ref():
        columns = columns_to_rows(r.table, token_sums(0, r.ref_hidden))
        r.ref_stats[pl.ds(aligned(8 * mine, 8), 8), :] = columns
        ref_stats.start()
        yield

    ref_ring, policy_work, policy_steps = ref_scatter.steps(r.result.at[0]), policy(), policy_ring()
    fill(policy_work, 3)
    for count in (2, 2, 2, 2, 2, 0, 0, 0):
        fill(ref_ring, 1)
        fill(policy_work, count)
    for _ in policy_work:
        pass
    pol_scatter.begin((0,))
    fill(ref_ring, 1)
    pol_scatter.begin((1,))
    fill(ref_ring, 1)
    pol_scatter.begin((2, 3))
    for count in (2, 2, 1):
        fill(ref_ring, 1)
        fill(policy_steps, count)
    together(policy_steps, after_ref(), (1,) + (0,) * 12)
    columns = columns_to_rows(r.table, token_sums(1, r.pol_hidden))
    packed = [columns[k : k + 1, 128 * c : 128 * c + 128] for k in range(3) for c in range(3)]
    packed = jnp.concatenate(packed + [jnp.zeros((7, 128), F32)], axis=0)
    r.pol_stats[pl.ds(aligned(16 * mine, 8), 16), :] = packed
    pol_stats.start()
    pol_stats.wait()
    packed = pol_stats.total()
    pol_total = [
        jnp.concatenate([packed[3 * k + c : 3 * k + c + 1] for c in range(3)], axis=1) for k in range(3)
    ]
    scale_pol = lax.rsqrt(pol_total[0] / WIDTH + NORM_EPS)
    rows_to_columns(r.table, [scale_pol, scale_pol * scale_pol * scale_pol * pol_total[1] / WIDTH])
    readout = r.readout[...].astype(F32)
    bare = r.table[0:TOK, 0:1] * post_gain * readout - r.summed[1] * r.table[0:TOK, 1:2]
    pack_hidden(bare, r.grad_buf, mine * SHARD)
    back_gather = Gather(r.grad_buf, SHARD, send.gather_back, recv.gather_back)
    back_gather.begin()

    lane = lax.broadcasted_iota(jnp.int32, (1, 384), 1)
    lengths = [r.lengths[s] for s in range(3)]
    living = jnp.zeros((1, 384), F32)
    for s in range(3):
        living = jnp.where((lane >= 96 * s) & (lane < 96 * s + lengths[s]), 1.0, living)
    ref_stats.wait()
    ref_total = ref_stats.total()
    scale_ref = lax.rsqrt(ref_total[0:1] / WIDTH + NORM_EPS)
    token_scores = (
        (ref_total[2:3] + scale_ref * ref_total[1:2]) * living,
        (pol_total[2] + scale_pol * pol_total[1]) * living,
    )
    row8 = lax.broadcasted_iota(jnp.int32, (8, 128), 0)
    lane8 = lax.broadcasted_iota(jnp.int32, (8, 128), 1)
    tile = jnp.zeros((8, 128), F32)
    for m in range(2):
        for s in range(3):
            inside = (lane >= 96 * s) & (lane < 96 * s + 96)
            score = jnp.sum(jnp.where(inside, token_scores[m], 0.0), axis=1, keepdims=True)
            tile = jnp.where((row8 == m) & (lane8 == 3 * rank + s), score, tile)
    scores = Exchange(r.scores, 8, 8, rank, in_data, send.scores, recv.scores)
    r.scores[pl.ds(aligned(8 * rank, 8), 8), :] = tile
    scores.start()

    def layer_outputs():
        rows_to_columns(r.coefficient, [scale_ref, scale_pol])
        for m, (hidden, out) in enumerate(((r.ref_hidden, r.ref_out), (r.pol_hidden, r.pol_out))):
            scale = r.coefficient[0:TOK, m : m + 1]
            out[...] = (hidden[...].astype(F32) + r.summed[m] * scale * post_gain).astype(BF16)
            yield
            store(1 - m).start()

    def preference():
        scores.wait()
        everyone = scores.total()
        ratio = everyone[1:2] - everyone[0:1]
        row32 = lax.broadcasted_iota(jnp.int32, (32, 128), 0)
        lane32 = lax.broadcasted_iota(jnp.int32, (32, 128), 1)
        named = jnp.full((32, 128), -1, jnp.int32)
        for k in range(24):
            named = jnp.where(row32 == k, r.pairing[k], named)
        chosen = named == lane32
        even = lax.rem(row32, 2) == 0
        picked = jnp.sum(jnp.where(chosen, ratio, 0.0), axis=1, keepdims=True)
        picked = jnp.broadcast_to(picked, (32, 128))
        other = jnp.where(even, pltpu.roll(picked, 31, 0), pltpu.roll(picked, 1, 0))
        margin = DPO_BETA * jnp.where(even, picked - other, other - picked)
        loss = jnp.maximum(-margin, 0.0) + jnp.log1p(jnp.exp(-jnp.abs(margin)))
        counted = even & (row32 < 24) & (lane32 == 0)
        total_loss = jnp.sum(jnp.where(counted, loss, 0.0), axis=(0, 1), keepdims=True)
        r.loss[...] = jnp.broadcast_to(total_loss, (8, 128))
        store(2).start()
        pull = DPO_BETA * LOSS_SCALE / (1.0 + jnp.exp(margin))
        signed = jnp.where(even, -pull, pull)
        coefficients = jnp.sum(jnp.where(chosen, signed, 0.0), axis=0, keepdims=True)
        lane128 = lax.broadcasted_iota(jnp.int32, (1, 128), 1)
        coefficient = jnp.zeros((1, 384), F32)
        for s in range(3):
            own = jnp.sum(jnp.where(lane128 == 3 * rank + s, coefficients, 0.0), axis=1, keepdims=True)
            coefficient = jnp.where((lane >= 96 * s) & (lane < 96 * s + 96), own, coefficient)
        rows_to_columns(r.coefficient, [coefficient * living])
        yield

    def meanwhile():
        yield from layer_outputs()
        yield from preference()

    together(back_gather.steps(), meanwhile(), (1, 1, 0, 0, 0, 0, 0, 1, 0, 0, 0, 0, 0, 0, 0))
    unpack_features(r.grad_buf, SHARD, 0, r.normed, 0)

    for i in range(3):
        total = None
        for c in range(3 * i, 3 * i + 3):
            term = dot(r.normed[0:TOK, 512 * c : 512 * c + 512], r.w_back[512 * c : 512 * c + 512, :])
            total = term if total is None else total + term
        r.grad_mixed[...] = total if i == 0 else r.grad_mixed[...] + total
    r.grad_mixed[...] *= r.coefficient[0:TOK, 0:1]

    for i in range(3):
        here = slice(96 * i, 96 * i + 96)
        at = slice(TOK + 96 * i, TOK + 96 * i + 96)
        cos, sin = r.cosine[...], r.sine[...]
        key, value = r.heads[at, 256:384], r.heads[at, 384:512]
        key_grad = jnp.zeros((96, HEAD), F32)
        value_grad = jnp.zeros((96, HEAD), F32)
        for g in range(2):
            query = r.heads[at, 128 * g : 128 * g + 128]
            incoming = r.grad_mixed[here, 128 * g : 128 * g + 128].astype(BF16)
            prob = r.probs[at, 128 * g : 128 * g + 96]
            cap = r.capped[at, 128 * g : 128 * g + 96] / SOFT_CAP
            grad_probs = dot(incoming, value, NT)
            value_grad = value_grad + dot(prob.astype(BF16), incoming, TN)
            centered = grad_probs - jnp.sum(grad_probs * prob, axis=1, keepdims=True)
            grad_scores = (prob * centered * (1.0 - cap * cap) * QUERY_SCALE).astype(BF16)
            query_grad = dot(grad_scores, key)
            key_grad = key_grad + dot(grad_scores, query, TN)
            r.grads[here, 128 * g : 128 * g + 128] = rope(query_grad, cos, -sin).astype(BF16)
        r.grads[here, 256:384] = rope(key_grad, cos, -sin).astype(BF16)
        r.grads[here, 384:512] = value_grad.astype(BF16)

    query_factor = jnp.concatenate([r.b_query[...], jnp.zeros((RANK, 256), BF16)], axis=0)
    value_factor = jnp.concatenate([jnp.zeros((RANK, 128), BF16), r.b_value[...]], axis=0)
    hook = dot(r.grads[:, 0:256], query_factor, NT) + dot(r.grads[:, 384:512], value_factor, NT)
    r.hooks[...] = (ADAPTER_SCALE * hook).astype(BF16)
    hooks = HookSum(
        r.hooks,
        r.hook_parts,
        r.hook_sums,
        mine,
        send.hooks,
        recv.hooks,
        send.hook_sums,
        recv.hook_sums,
    )
    hooks.start()
    stats_back = Exchange(r.stats_back, 8, 16, mine, in_tensor, send.stats_back, recv.stats_back)
    factors = Exchange(r.factors, 64, 8, rank, in_data, send.factors, recv.factors)
    for _ in partial_products(r.grads, r.w_in, r.partial_back):
        pass
    back_scatter = Scatter(
        r.partial_back, r.landing_back, SHARD, send.scatter_back, recv.scatter_back
    )
    back_scatter.begin((0, 1))

    def across(i):
        return pltpu.make_async_remote_copy(
            src_ref=r.a_terms.at[pl.ds(aligned(576 * (2 * i + 1 - core), 64), 576), :],
            dst_ref=r.a_across.at[pl.ds(576 * i, 576), :],
            send_sem=send.across.at[i],
            recv_sem=recv.across.at[i],
            device_id={CORE: 1 - core},
            device_id_type=MESH,
        )

    def round_y(source, target, to):
        return pltpu.make_async_remote_copy(
            src_ref=source,
            dst_ref=target,
            send_sem=send.round.at[0],
            recv_sem=recv.round.at[0],
            device_id={Y: to},
            device_id_type=MESH,
        )

    three = r.a_round.at[pl.ds(0, 3 * 576), :]
    rounds = round_y(three, three, lax.rem(y + 1, 4))

    def pair_up(i):
        across(i).wait_recv()
        rows = slice(576 * i, 576 * i + 576)
        own = r.a_terms[pl.ds(aligned(576 * (2 * i + core), 64), 576), :].astype(F32)
        r.a_pairs[rows, :] = (own + r.a_across[rows, :].astype(F32)).astype(BF16)

        @pl.when(y != i)
        def _():
            place = pl.ds(aligned(576 * lax.rem(i - y + 4, 4), 64), 576)
            round_y(r.a_pairs.at[pl.ds(576 * i, 576), :], r.a_round.at[place, :], i).start()

    def adapters_back():
        pull_back = jnp.sum(r.grads[...].astype(F32) * r.linear[...], axis=1, keepdims=True)
        pull_back += jnp.sum(r.hooks[...].astype(F32) * r.low[...].astype(F32), axis=1, keepdims=True)
        row = columns_to_rows(r.table, [pull_back])[0:1]
        r.stats_back[pl.ds(aligned(8 * mine, 8), 8), :] = as_tile(row)
        stats_back.start()
        factor_terms = ADAPTER_SCALE * dot(r.low[...], r.grads[:, 0:512], TN)
        own_factor = pl.ds(aligned(64 * rank, 64), 64)
        r.factors[own_factor, 0:256] = factor_terms[0:64, 0:256].astype(BF16)
        r.factors[own_factor, 256:384] = factor_terms[64:128, 384:512].astype(BF16)
        factors.start()
        yield
        hooks.wait()
        hook_low = r.hook_sums[...]
        r.summed[0] = dot(hook_low, r.a_own[...], NT)
        for q in range(4):
            at = MAIN + 128 * q
            tail = dot(r.normed[TOK : 2 * TOK, at : at + 128], hook_low, TN).astype(BF16)
            for t in range(4 * q, 4 * q + 4):
                term = dot(r.normed[TOK : 2 * TOK, 256 * t : 256 * t + 256], hook_low, TN)
                r.a_terms[288 * t : 288 * t + 256, :] = term.astype(BF16)
                j = t - 4 * q
                r.a_terms[288 * t + 256 : 288 * t + 288, :] = tail[32 * j : 32 * j + 32, :]
            across(q).start()
            if q:
                pair_up(q - 1)
            yield
        pair_up(3)
        yield

    adapters = adapters_back()
    fill(adapters, 1)
    back_scatter.begin((2,))
    hooks.reduce()
    back_scatter.begin((3,))
    together(back_scatter.steps(r.result.at[0]), adapters, (0, 0, 0, 1, 1, 1, 1, 1, 0, 0, 0, 0, 0))

    stats_back.wait()
    rows_to_columns(r.table, [as_row(stats_back.total())])
    unpack_result(r.result.at[0], 0, r.summed.at[1])
    pre_scale = r.scale[TOK : 2 * TOK, 0:1]
    shrink_back = pre_scale * pre_scale * r.table[0:TOK, 0:1] / WIDTH
    grad_result = r.coefficient[0:TOK, 0:1] * r.readout[...].astype(F32)
    hidden = r.pol_hidden[...].astype(F32)
    r.grad_hidden[...] = (
        grad_result + pre_scale * pre_gain * (r.summed[1] + r.summed[0]) - hidden * shrink_back
    ).astype(BF16)
    store(3).start()
    factors.wait()
    factor_total = factors.total()
    r.query_grad[...] = factor_total[:, 0:256]
    r.value_grad[...] = factor_total[:, 256:384]
    store(5).start()
    store(6).start()
    whole = r.a_pairs[pl.ds(aligned(576 * y, 64), 576), :].astype(F32)
    rounds.wait_recv()
    for i in range(1, 4):
        whole = whole + r.a_round[576 * i : 576 * i + 576, :].astype(F32)
    r.grad_a[...] = whole
    store(4).start()
    drain_a()
    for ring in (ref_gather, pol_gather, weights, ref_scatter, pol_scatter, back_gather, back_scatter):
        ring.drain()
    for exchange in (pre_stats, ref_stats, pol_stats, scores, lows, hooks, stats_back, factors):
        exchange.drain()
    for i in range(4):
        across(i).wait_send()
    rounds.wait_send()
    for number in range(len(outputs)):
        store(number).wait()


def partial_products(rows, matrix, partial):
    for block in range(4):
        left = rows[...]
        for t in range(4 * block, 4 * block + 4):
            product = dot(left, matrix[256 * t : 256 * t + 256, :], NT).astype(BF16)
            for half in range(2):
                at = t * SHARD + TOK * half
                partial[at : at + TOK, :] = product[:, 128 * half : 128 * half + 128]
        at = MAIN + 128 * block
        product = dot(left, matrix[at : at + 128, :], NT).astype(BF16)
        for j in range(4):
            at = (4 * block + j) * SHARD + 2 * TOK
            partial[at : at + GROUP, :] = pack_tail(product[:, 32 * j : 32 * j + 32])
        yield


def rotation_tables():
    spacing = ROPE_BASE ** (-2.0 * np.arange(64, dtype=np.float32) / HEAD)
    angles = np.arange(LENGTH, dtype=np.float32)[:, None] * spacing.astype(np.float32)[None, :]
    cosine, sine = np.cos(angles), np.sin(angles)
    return (
        np.concatenate([cosine, cosine], axis=1).astype(np.float32),
        np.concatenate([-sine, sine], axis=1).astype(np.float32),
    )


INPUTS = dict(
    lengths=None,
    pairing=None,
    ref_hidden=((TOK, TOK), BF16),
    pol_hidden=((TOK, TOK), BF16),
    w_query=((576, 256), BF16),
    w_key=((576, 128), BF16),
    w_value=((576, 128), BF16),
    w_out=((576, 256), BF16),
    a_query=((RANK, 576), BF16),
    a_value=((RANK, 576), BF16),
    readout=((TOK, TOK), BF16),
    b_query=((RANK, 256), BF16),
    b_value=((RANK, 128), BF16),
    pre_gain=((36, 128), F32),
    post_gain=((36, 128), F32),
    cosine=((LENGTH, HEAD), F32),
    sine=((LENGTH, HEAD), F32),
)
OUTPUTS = dict(
    pol_out=((TOK, TOK), BF16),
    ref_out=((TOK, TOK), BF16),
    loss=((8, 128), F32),
    grad_hidden=((TOK, TOK), BF16),
    grad_a=((576, 128), F32),
    query_grad=((RANK, 256), F32),
    value_grad=((RANK, 128), F32),
)


def hand_out(*refs):
    for source, target in zip(refs[: len(OUTPUTS)], refs[len(OUTPUTS) :]):
        target[...] = source[0 : target.shape[0], 0 : target.shape[1]]


def body(
    ref_hidden,
    pol_hidden,
    readout,
    lengths,
    pairing,
    pre_gain,
    post_gain,
    w_query,
    w_key,
    value_projection,
    w_out,
    a_query,
    a_value,
    query_second_factor,
    value_second_factor,
):
    vmem, whole = pl.BlockSpec(memory_space=pltpu.VMEM), pl.BlockSpec(memory_space=pl.ANY)
    cosine, sine = rotation_tables()
    dma = pltpu.SemaphoreType.DMA
    staged = [pltpu.VMEM(*kind) if kind else None for kind in list(INPUTS.values()) + list(OUTPUTS.values())]
    staged[0:2] = [pltpu.SMEM((3,), jnp.int32), pltpu.SMEM((24,), jnp.int32)]
    results = pl.pallas_call(
        step_body,
        out_shape=tuple(jax.ShapeDtypeStruct(*kind) for kind in OUTPUTS.values()),
        in_specs=[whole] * len(INPUTS),
        out_specs=(whole,) * len(OUTPUTS),
        scratch_shapes=staged
        + [pltpu.VMEM(shape, kind) for shape, kind in SCRATCH.values()]
        + [dma((len(INPUTS),)), dma((len(OUTPUTS),))]
        + [dma((count,)) for pair in SEMAPHORES.values() for count in pair],
        compiler_params=pltpu.CompilerParams(
            collective_id=0, has_side_effects=True, vmem_limit_bytes=62 * 1024 * 1024
        ),
    )(
        lengths,
        pairing,
        ref_hidden,
        pol_hidden,
        w_query,
        w_key,
        value_projection,
        w_out,
        a_query.T,
        a_value.T,
        readout,
        query_second_factor,
        value_second_factor,
        pre_gain.reshape(36, 128),
        post_gain.reshape(36, 128),
        jnp.asarray(cosine),
        jnp.asarray(sine),
    )
    shapes = [jax.ShapeDtypeStruct(a.shape, a.dtype) for a in results]
    shapes[2] = jax.ShapeDtypeStruct((1, 1), F32)
    pol_out, ref_out, loss, grad_hidden, grad_a, query_grad, value_grad = pl.pallas_call(
        hand_out,
        out_shape=tuple(shapes),
        in_specs=[vmem] * len(OUTPUTS),
        out_specs=(vmem,) * len(OUTPUTS),
    )(*results)
    return (pol_out, ref_out, loss.reshape(()), grad_hidden, grad_a, query_grad, value_grad)


def solution(mesh):
    torus = Mesh(mesh.devices.reshape(4, 2, 4, 4), (Y, CORE, X, Z))
    split, rows, columns = P(DP, TENSOR), P(DP, None), P(None, TENSOR)
    return jax.shard_map(
        body,
        mesh=torus,
        in_specs=(split, split, split, P(DP), P(), P(), P(), split, split, split, split, rows, rows, columns, columns),
        out_specs=(split, split, P(), split, rows, columns, columns),
        check_vma=False,
    )
```

```python
import jax
import jax.numpy as jnp
import numpy as np
from jax import lax
from jax.experimental import pallas as pl
from jax.experimental.pallas import tpu as pltpu
from jax.sharding import Mesh
from jax.sharding import PartitionSpec as P

Y, CORE, X, Z = "dp_0", "dp_1", "tensor_0", "tensor_1"
DP, TENSOR = (Y, CORE), (X, Z)
MESH = pl.DeviceIdType.MESH

WIDTH = 4608
TOK = 288
LENGTH = 96
HEAD = 128
RANK = 64
NORM_EPS = 1e-06
SOFT_CAP = 50.0
ADAPTER_SCALE = 0.5
DPO_BETA = 0.5
LOSS_SCALE = 256.0
ROPE_BASE = 10000.0
QUERY_SCALE = float(WIDTH // 32) ** (-0.5)

GROUP = 80
SHARD = 2 * TOK + GROUP
MAIN = 4096
RINGS = ((0, 1), (0, -1), (1, 1), (1, -1))

ORDER = (2, 1, 3, 0)

F32 = jnp.float32
BF16 = jnp.bfloat16
NT = (((1,), (1,)), ((), ()))
TN = (((0,), (0,)), ((), ()))


def dot(a, b, dims=(((1,), (0,)), ((), ())), precision=None):
    return lax.dot_general(a, b, dims, preferred_element_type=F32, precision=precision)


def aligned(start, multiple):
    return start if isinstance(start, int) else pl.multiple_of(start, multiple)


def back(position, hops, direction):
    return lax.rem(position - hops * direction + 8, 4)


def chunks_of(rows):
    tiles = rows // 16
    sizes = [16 * (tiles // 4 + (1 if k < tiles % 4 else 0)) for k in range(4)]
    return sizes, [sum(sizes[:k]) for k in range(4)]


class Ring:
    def __init__(self, rows, send, recv):
        self.rows = rows
        self.sizes, self.starts = chunks_of(rows)
        self.send, self.recv = send, recv
        self.at = (lax.axis_index(X), lax.axis_index(Z))

    def place(self, k, first, second):
        primary, way = RINGS[k]
        a = back(self.at[primary], first, way)
        b = back(self.at[1 - primary], second, way)
        px, pz = (a, b) if primary == 0 else (b, a)
        return aligned((4 * px + pz) * self.rows + self.starts[k], 16)

    def next_on(self, k, secondary, behind=False):
        primary, way = RINGS[k]
        axis = 1 - primary if secondary else primary
        return {TENSOR[axis]: back(self.at[axis], 1 if behind else -1, way)}

    def remote(self, source, target, number, device):
        return pltpu.make_async_remote_copy(
            src_ref=source,
            dst_ref=target,
            send_sem=self.send.at[0],
            recv_sem=self.recv.at[number],
            device_id=device,
            device_id_type=MESH,
        )

    def arrived(self, number):
        whole = self.memory.at[pl.ds(0, self.rows), :]
        self.remote(whole, whole, number, self.next_on(0, False)).wait_recv()

    def drain(self):
        whole = self.memory.at[pl.ds(0, 15 * self.rows), :]
        self.remote(whole, whole, 0, self.next_on(0, False)).wait_send()


class Gather(Ring):
    def __init__(self, buffer, rows, send, recv):
        super().__init__(rows, send, recv)
        self.memory = buffer

    def piece(self, k, j, s):
        return self.memory.at[pl.ds(self.place(k, j, s), self.sizes[k]), :]

    def first(self, k, number):
        piece = self.piece(k, 1 if number == 1 else 0, 0)
        return self.remote(piece, piece, number, self.next_on(k, False, number == 2))

    def second(self, k, j, s):
        piece = self.piece(k, j, s)
        return self.remote(piece, piece, 3 + 3 * j + s, self.next_on(k, True))

    def begin(self):
        for k in range(4):
            self.first(k, 0).start()
            self.first(k, 2).start()
        for k in range(4):
            self.second(k, 0, 0).start()

    def await_first(self, number):
        self.arrived(number)
        for k in range(4):
            if number == 0:
                self.first(k, 1).start()
            self.second(k, number + 1, 0).start()

    def await_second(self, j, s):
        self.arrived(3 + 3 * j + s)
        if s < 2:
            for k in range(4):
                self.second(k, j, s + 1).start()

    def steps(self):
        self.await_first(0)
        yield
        self.await_first(2)
        yield
        self.await_second(0, 0)
        yield
        self.await_first(1)
        yield
        for j, s in ((1, 0), (3, 0), (0, 1), (2, 0), (1, 1), (3, 1), (0, 2), (2, 1), (1, 2), (3, 2), (2, 2)):
            self.await_second(j, s)
            yield


class ShortGather(Gather):
    def second(self, k, j, number):
        piece = self.piece(k, j, 1 if number == 1 else 0)
        return self.remote(piece, piece, 3 + 3 * j + number, self.next_on(k, True, number == 2))

    def begin(self):
        for k in range(4):
            self.first(k, 0).start()
            self.first(k, 2).start()
        for k in range(4):
            self.second(k, 0, 0).start()
            self.second(k, 0, 2).start()

    def await_first(self, number):
        self.arrived(number)
        for k in range(4):
            if number == 0:
                self.first(k, 1).start()
            self.second(k, number + 1, 0).start()
            self.second(k, number + 1, 2).start()

    def await_second(self, j, number):
        self.arrived(3 + 3 * j + number)
        if number == 0:
            for k in range(4):
                self.second(k, j, 1).start()

    def steps(self):
        self.await_first(0)
        yield
        self.await_first(2)
        yield
        self.await_second(0, 0)
        yield
        self.await_first(1)
        yield
        for j, number in (
            (0, 2), (1, 0), (3, 0), (2, 0), (1, 2), (3, 2), (0, 1), (1, 1), (2, 2), (3, 1), (2, 1)
        ):
            self.await_second(j, number)
            yield


class Scatter(Ring):
    def __init__(self, partial, landing, rows, send, recv):
        super().__init__(rows, send, recv)
        self.partial, self.landing, self.memory = partial, landing, landing

    def piece(self, k, first, second):
        return self.partial.at[pl.ds(self.place(k, first, second), self.sizes[k]), :]

    def slot(self, k, number):
        return self.landing.at[pl.ds(15 * self.starts[k] + number * self.sizes[k], self.sizes[k]), :]

    def outer(self, k, j, s):
        number = 3 * j + s
        return self.remote(self.piece(k, ORDER[j], s + 1), self.slot(k, number), number, self.next_on(k, True))

    def inner(self, k, number):
        piece = self.piece(k, (2, 3, 1)[number - 12], 0)
        return self.remote(piece, self.slot(k, number), number, self.next_on(k, False, number == 14))

    def add(self, k, number, first, second):
        piece, slot = self.piece(k, first, second), self.slot(k, number)
        piece[...] = (piece[...].astype(F32) + slot[...].astype(F32)).astype(BF16)

    def begin(self, parts=range(4)):
        for j in parts:
            for k in range(4):
                self.outer(k, j, 0).start()

    def steps(self, result):
        for s in range(3):
            for j in range(4):
                self.arrived(3 * j + s)
                if s == 2 and j == 2:
                    self.arrived(12)
                for k in range(4):
                    self.add(k, 3 * j + s, ORDER[j], s + 2)
                    if s < 2:
                        self.outer(k, j, s + 1).start()
                    elif j == 0:
                        self.inner(k, 12).start()
                    elif j == 1:
                        self.inner(k, 14).start()
                    elif j == 2:
                        self.add(k, 12, 3, 0)
                        self.inner(k, 13).start()
                yield
        self.arrived(14)
        self.arrived(13)
        for k in range(4):
            own = self.piece(k, 0, 0)[...].astype(F32)
            for number in (14, 13):
                own = own + self.slot(k, number)[...].astype(F32)
            result[pl.ds(self.starts[k], self.sizes[k]), :] = own
        yield


class ShortScatter(Scatter):
    def outer(self, k, j, number):
        piece = self.piece(k, ORDER[j], (2, 3, 1)[number])
        slot = self.slot(k, 3 * j + number)
        return self.remote(piece, slot, 3 * j + number, self.next_on(k, True, number == 2))

    def hand_on(self, j, number):
        for k in range(4):
            self.outer(k, j, number).start()

    def close(self, j):
        self.arrived(3 * j + 1)
        self.arrived(3 * j + 2)
        for k in range(4):
            piece = self.piece(k, ORDER[j], 0)
            value = piece[...].astype(F32)
            for number in (1, 2):
                value = value + self.slot(k, 3 * j + number)[...].astype(F32)
            piece[...] = value.astype(BF16)

    def steps(self, result):
        for j in range(4):
            self.arrived(3 * j)
            for k in range(4):
                self.add(k, 3 * j, ORDER[j], 3)
                self.outer(k, j, 1).start()
            if j < 2:
                self.hand_on(j, 2)
            yield
        self.close(0)
        for k in range(4):
            self.inner(k, 12).start()
        self.hand_on(2, 2)
        self.hand_on(3, 2)
        yield
        self.close(1)
        for k in range(4):
            self.inner(k, 14).start()
        yield
        self.close(2)
        self.arrived(12)
        for k in range(4):
            self.add(k, 12, 3, 0)
            self.inner(k, 13).start()
        yield
        self.close(3)
        yield
        self.arrived(14)
        self.arrived(13)
        for k in range(4):
            own = self.piece(k, 0, 0)[...].astype(F32)
            for number in (14, 13):
                own = own + self.slot(k, number)[...].astype(F32)
            result[pl.ds(self.starts[k], self.sizes[k]), :] = own
        yield


class Weights:
    def __init__(self, w_in, w_back, y_send, y_recv, d_send, d_recv):
        self.w_in, self.w_back = w_in, w_back
        self.sems = (y_send, y_recv, d_send, d_recv)
        self.y, self.core = lax.axis_index(Y), lax.axis_index(CORE)

    def block(self, hops, half, part, core):
        way = 1 - 2 * half
        tile = 2 * (2 * back(self.y, hops, way) + core) + half
        if part < 2:
            return self.w_in.at[pl.ds(aligned(256 * tile + 128 * part, 128), 128), :]
        if part == 3:
            return self.w_back.at[pl.ds(aligned(256 * tile, 256), 256), :]
        ref = self.w_in if part == 2 else self.w_back
        return ref.at[pl.ds(aligned(MAIN + 32 * tile, 32), 32), :]

    def round(self, s, half, part):
        ref = self.block(s, half, part, self.core)
        return self.copy(ref, 0, part, 5 * s + part, {Y: back(self.y, -1, 1 - 2 * half)})

    def across(self, i, half, part):
        return self.copy(self.block(i, half, part, self.core), 2, part, part // 3, {CORE: 1 - self.core})

    def copy(self, ref, way, part, number, device):
        return pltpu.make_async_remote_copy(
            src_ref=ref,
            dst_ref=ref,
            send_sem=self.sems[way].at[part // 3],
            recv_sem=self.sems[way + 1].at[number],
            device_id=device,
            device_id_type=MESH,
        )

    def rows(self, part, count):
        return (self.w_in if part < 3 else self.w_back).at[pl.ds(0, count), :]

    def step(self, s, parts):
        for part in parts:
            if s > 0:
                both = self.rows(part, 2 * (128, 128, 32, 256, 32)[part])
                self.copy(both, 0, part, 5 * (s - 1) + part, {CORE: 1 - self.core}).wait_recv()
            for half in range(2):
                if s < 3:
                    self.round(s, half, part).start()
                self.across(s, half, part).start()

    def arrive(self, part):
        self.copy(self.rows(part, 8 * TOK), 2, part, part // 3, {CORE: 1 - self.core}).wait_recv()

    def drain(self):
        for part in (0, 3):
            self.copy(self.rows(part, 6 * TOK), 0, part, 0, {CORE: 1 - self.core}).wait_send()
            self.copy(self.rows(part, 8 * TOK), 2, part, 0, {CORE: 1 - self.core}).wait_send()


class Exchange:
    def __init__(self, buffer, rows, count, me, device_of, send, recv):
        self.buffer, self.rows, self.count, self.me = buffer, rows, count, me
        self.device_of, self.send, self.recv = device_of, send, recv

    def part(self, buffer, i):
        return buffer.at[pl.ds(aligned(i * self.rows, self.rows), self.rows), :]

    def copy(self, source, target, peer):
        return pltpu.make_async_remote_copy(
            src_ref=source,
            dst_ref=target,
            send_sem=self.send.at[0],
            recv_sem=self.recv.at[0],
            device_id=self.device_of(peer),
            device_id_type=MESH,
        )

    def start(self):
        own = self.part(self.buffer, self.me)
        for delta in range(1, self.count):
            self.copy(own, own, lax.rem(self.me + delta, self.count)).start()

    def slots(self, count):
        whole = self.buffer.at[pl.ds(0, count * self.rows), :]
        return self.copy(whole, whole, lax.rem(self.me + 1, self.count))

    def wait(self):
        self.slots(self.count - 1).wait_recv()

    def total(self):
        value = self.buffer[0 : self.rows, :].astype(F32)
        for i in range(1, self.count):
            value = value + self.buffer[self.rows * i : self.rows * i + self.rows, :].astype(F32)
        return value

    def drain(self):
        self.slots(self.count - 1).wait_send()


OWNERS = 9


class HookSum:
    def __init__(self, terms, parts, sums, me, send_parts, recv_parts, send_sums, recv_sums, narrow):
        self.terms, self.parts, self.sums, self.me = terms, parts, sums, me
        self.there = Exchange(parts, 32, 16, me, in_tensor, send_parts, recv_parts)
        self.home = Exchange(narrow, 32, 16, me, in_tensor, send_sums, recv_sums)
        self.owner = me < OWNERS

    def start(self):
        @pl.when(self.owner)
        def _():
            own = pl.ds(aligned(32 * self.me, 32), 32)
            self.parts[own, :] = self.terms[own, :]

        for delta in range(1, 16):
            peer = lax.rem(self.me + delta, 16)

            @pl.when(peer < OWNERS)
            def _():
                self.there.copy(self.there.part(self.terms, peer), self.there.part(self.parts, self.me), peer).start()

    def reduce(self):
        @pl.when(self.owner)
        def _():
            self.there.wait()
            self.sums[pl.ds(aligned(32 * self.me, 32), 32), :] = self.there.total().astype(BF16)
            own = self.home.part(self.sums, self.me)
            for delta in range(1, 16):
                self.home.copy(own, own, lax.rem(self.me + delta, 16)).start()

    def wait(self):
        @pl.when(self.owner)
        def _():
            self.home.slots(OWNERS - 1).wait_recv()

        @pl.when(jnp.logical_not(self.owner))
        def _():
            self.home.slots(OWNERS).wait_recv()

    def drain(self):
        @pl.when(self.owner)
        def _():
            self.there.slots(OWNERS - 1).wait_send()
            self.home.slots(15).wait_send()

        @pl.when(jnp.logical_not(self.owner))
        def _():
            self.there.slots(OWNERS).wait_send()


def in_tensor(i):
    return {X: lax.div(i, 4), Z: lax.rem(i, 4)}


def in_data(i):
    return {Y: lax.div(i, 2), CORE: lax.rem(i, 2)}


def together(main, filler, ratio):
    for number, _ in enumerate(main):
        for _ in range(ratio if isinstance(ratio, int) else ratio[number]):
            next(filler, None)
    for _ in filler:
        pass


def signal(peers):
    barrier = pltpu.get_barrier_semaphore()
    for peer in peers:
        pl.semaphore_signal(barrier, inc=1, device_id=peer, device_id_type=MESH)


def pack_tail(tail):
    last = jnp.concatenate([tail[240:288], jnp.zeros((32, 32), tail.dtype)], axis=0)
    return jnp.concatenate([tail[0:80], tail[80:160], tail[160:240], last], axis=1)


GROUPS = ((0, 80), (80, 80), (160, 80), (240, 48))


def unpack_features(buffer, rows, offset, target, row_offset):
    def main(t, carry):
        base = aligned(t * rows + offset, 16)
        for half in range(2):
            target[pl.ds(row_offset, TOK), pl.ds(aligned(256 * t + 128 * half, 128), 128)] = buffer[
                pl.ds(aligned(base + TOK * half, 16), TOK), :
            ]
        return carry

    lax.fori_loop(0, 16, main, 0)

    def tail(q, carry):
        tails = [
            buffer[pl.ds(aligned((4 * q + j) * rows + offset + 2 * TOK, 16), GROUP), :] for j in range(4)
        ]
        for g, (start, size) in enumerate(GROUPS):
            joined = jnp.concatenate([t[:size, 32 * g : 32 * g + 32] for t in tails], axis=1)
            target[pl.ds(row_offset + start, size), pl.ds(aligned(MAIN + 128 * q, 128), 128)] = joined
        return carry

    lax.fori_loop(0, 4, tail, 0)


def unpack_result(packed, offset, target):
    for half in range(2):
        target[:, 128 * half : 128 * half + 128] = packed[offset + TOK * half : offset + TOK * half + TOK, :]
    for g, (start, size) in enumerate(GROUPS):
        base = offset + 2 * TOK
        target[start : start + size, 256:288] = packed[base : base + size, 32 * g : 32 * g + 32]


def pack_hidden(hidden, buffer, base):
    for half in range(2):
        buffer[pl.ds(aligned(base + TOK * half, 16), TOK), :] = hidden[:, 128 * half : 128 * half + 128].astype(
            BF16
        )
    buffer[pl.ds(aligned(base + 2 * TOK, 16), GROUP), :] = pack_tail(hidden[:, 256:288]).astype(BF16)


def feature_lanes(gain, start, count):
    pieces = []
    while count:
        row, lane = divmod(start, 128)
        size = min(count, 128 - lane)
        pieces.append(gain[row : row + 1, lane : lane + size])
        start, count = start + size, count - size
    return pieces[0] if len(pieces) == 1 else jnp.concatenate(pieces, axis=1)


def order_gain(gain, target):
    for c in range(32):
        target[c : c + 1, :] = feature_lanes(gain, 288 * (c // 2) + 128 * (c % 2), 128)
    for q in range(4):
        tails = [feature_lanes(gain, 288 * (4 * q + j) + 256, 32) for j in range(4)]
        target[32 + q : 33 + q, :] = jnp.concatenate(tails, axis=1)


def own_gain(ordered, mine):
    tail = ordered[pl.ds(32 + lax.div(mine, 4), 1), :]
    picked = jnp.zeros((1, 32), F32)
    for j in range(4):
        picked = jnp.where(lax.rem(mine, 4) == j, tail[:, 32 * j : 32 * j + 32], picked)
    return jnp.concatenate([ordered[pl.ds(2 * mine, 1), :], ordered[pl.ds(2 * mine + 1, 1), :], picked], axis=1)


def normalize(normed, scale_ref, gain_ref, offset):
    def rows(i, carry):
        at = pl.ds(aligned(offset + 96 * i, 96), 96)
        squares = jnp.zeros((96, 128), F32)
        for c in range(36):
            x = normed[at, 128 * c : 128 * c + 128].astype(F32)
            squares = squares + x * x
        scale = lax.rsqrt(jnp.sum(squares, axis=1, keepdims=True) / WIDTH + NORM_EPS)
        scale_ref[at, :] = jnp.broadcast_to(scale, (96, 128))
        for c in range(36):
            x = normed[at, 128 * c : 128 * c + 128].astype(F32)
            normed[at, 128 * c : 128 * c + 128] = (x * scale * gain_ref[c : c + 1, :]).astype(BF16)
        return carry

    lax.fori_loop(0, 3, rows, 0)


def rope(x, cosine, sine):
    return x * cosine + pltpu.roll(x, 64, 1) * sine


def allowed_here(length):
    query = lax.broadcasted_iota(jnp.int32, (LENGTH, LENGTH), 0)
    key = lax.broadcasted_iota(jnp.int32, (LENGTH, LENGTH), 1)
    return (key <= query) & (key < length)


def columns_to_rows(scratch, columns):
    lane = lax.broadcasted_iota(jnp.int32, (TOK, 128), 1)
    table = jnp.zeros((TOK, 128), F32)
    for k, column in enumerate(columns):
        table = jnp.where(lane == k, column, table)
    scratch[0:TOK, :] = table
    scratch[TOK:384, :] = jnp.zeros((384 - TOK, 128), F32)
    return jnp.transpose(scratch[...])[0:8, :]


def as_tile(row):
    pieces = [row[:, 128 * c : 128 * c + 128] for c in range(3)]
    return jnp.concatenate(pieces + [jnp.zeros((5, 128), F32)], axis=0)


def as_row(tile):
    return jnp.concatenate([tile[c : c + 1] for c in range(3)], axis=1)


def rows_to_columns(scratch, rows):
    missing = 128 - sum(row.shape[0] for row in rows)
    filled = jnp.concatenate(list(rows) + [jnp.zeros((missing, 384), F32)], axis=0)
    scratch[...] = jnp.transpose(filled)


SCRATCH = dict(
    ref_gathered=((16 * SHARD, 128), BF16),
    pol_gathered=((16 * SHARD, 128), BF16),
    w_in=((WIDTH, 512), BF16),
    a_all=((640, 128), BF16),
    a_own=((TOK, 128), BF16),
    w_back=((WIDTH, 256), BF16),
    normed=((2 * TOK, WIDTH), BF16),
    scale=((2 * TOK, 128), F32),
    acc=((2 * TOK, 512), F32),
    linear=((TOK, 512), F32),
    pre_stats=((16 * 8, 128), F32),
    own_normed=((TOK, TOK), BF16),
    low_terms=((TOK, 128), BF16),
    low_parts=((16 * 32, 128), BF16),
    low=((TOK, 128), BF16),
    heads=((2 * TOK, 512), BF16),
    mixed=((2 * TOK, 256), BF16),
    probs=((2 * TOK, 256), F32),
    capped=((2 * TOK, 256), F32),
    partial=((16 * SHARD, 128), BF16),
    partial_pol=((16 * SHARD, 128), BF16),
    landing=((15 * SHARD, 128), BF16),
    landing_pol=((15 * SHARD, 128), BF16),
    result=((2, SHARD, 128), F32),
    summed=((2, TOK, TOK), F32),
    table=((384, 128), F32),
    coefficient=((384, 128), F32),
    ref_stats=((16 * 8, 384), F32),
    pol_stats=((16 * 16, 128), F32),
    pre_ordered=((40, 128), F32),
    post_ordered=((40, 128), F32),
    scores=((8 * 8, 128), F32),
    grad_buf=((16 * SHARD, 128), BF16),
    grad_mixed=((TOK, 256), F32),
    grads=((TOK, 512), BF16),
    partial_back=((16 * SHARD, 128), BF16),
    landing_back=((15 * SHARD, 128), BF16),
    hooks=((TOK, 128), BF16),
    hook_parts=((16 * 32, 128), BF16),
    hook_sums=((TOK, 128), BF16),
    stats_back=((16 * 8, 128), F32),
    factors=((8 * 64, 384), BF16),
    a_terms=((WIDTH, 128), BF16),
    a_across=((4 * 576, 128), BF16),
    a_pairs=((4 * 576, 128), BF16),
    a_round=((4 * 576, 128), BF16),
)
SEMAPHORES = dict(
    gather_ref=(1, 15),
    gather_pol=(1, 15),
    a=(1, 1),
    pre_stats=(1, 1),
    low_terms=(1, 1),
    low=(1, 1),
    scatter_ref=(1, 15),
    scatter_pol=(1, 15),
    gather_back=(1, 15),
    scatter_back=(1, 15),
    y=(2, 15),
    d=(2, 2),
    ref_stats=(1, 1),
    pol_stats=(1, 1),
    scores=(1, 1),
    hooks=(1, 1),
    hook_sums=(1, 1),
    stats_back=(1, 1),
    factors=(1, 1),
    across=(4, 4),
    round=(1, 1),
)


class Refs:
    pass


def step_body(*refs):
    inputs, outputs = list(INPUTS), list(OUTPUTS)
    outside, refs = refs[: len(inputs + outputs)], refs[len(inputs + outputs) :]
    names = inputs + outputs + list(SCRATCH)
    r, send, recv = Refs(), Refs(), Refs()
    for name, ref in zip(names, refs):
        setattr(r, name, ref)
    load_sems, store_sems, *sems = refs[len(names) :]
    for number, name in enumerate(SEMAPHORES):
        setattr(send, name, sems[2 * number])
        setattr(recv, name, sems[2 * number + 1])

    x, z = lax.axis_index(X), lax.axis_index(Z)
    y, core = lax.axis_index(Y), lax.axis_index(CORE)
    mine, rank = 4 * x + z, 2 * y + core
    def load(number):
        return pltpu.make_async_copy(outside[number], refs[number], load_sems.at[number])

    def store(number):
        at = len(inputs) + number
        return pltpu.make_async_copy(refs[at], outside[at], store_sems.at[number])

    signal(
        [in_tensor(lax.rem(mine + i, 16)) for i in range(1, 16)]
        + [in_data(lax.rem(rank + i, 8)) for i in range(1, 8)]
    )
    for number in range(len(inputs)):
        load(number).start()
    for number in range(10):
        load(number).wait()
    pack_hidden(r.ref_hidden[...], r.ref_gathered, mine * SHARD)
    pack_hidden(r.pol_hidden[...], r.pol_gathered, mine * SHARD)
    a_both = jnp.concatenate([r.a_query[...].astype(F32), r.a_value[...].astype(F32)], axis=0)
    r.a_all[...] = jnp.transpose(jnp.concatenate([a_both, jnp.zeros((128, 64), F32)], axis=1)).astype(BF16)
    a_rank = lax.div(mine, 2)
    a_here, a_core = rank == a_rank, core == lax.rem(a_rank, 2)
    a_relay = a_core & (y != lax.div(a_rank, 2))
    a_rows = pl.ds(aligned(TOK * lax.rem(mine, 2), 32), TOK)

    @pl.when(a_here)
    def _():
        r.a_own[...] = r.a_all[a_rows, :]

    def a_copy(source, target, device):
        return pltpu.make_async_remote_copy(
            src_ref=source,
            dst_ref=target,
            send_sem=send.a.at[0],
            recv_sem=recv.a.at[0],
            device_id=device,
            device_id_type=MESH,
        )

    def send_a():
        @pl.when(a_here)
        def _():
            for device in [{Y: lax.rem(y + i, 4)} for i in (1, 3, 2)] + [{CORE: 1 - core}]:
                a_copy(r.a_all.at[a_rows, :], r.a_own, device).start()

    def relay_a():
        @pl.when(a_relay)
        def _():
            a_copy(r.a_own, r.a_own, {CORE: 1 - core}).wait_recv()
            a_copy(r.a_own, r.a_own, {CORE: 1 - core}).start()

    def await_a():
        @pl.when(jnp.logical_not(a_core))
        def _():
            a_copy(r.a_own, r.a_own, {CORE: 1 - core}).wait_recv()

    def drain_a():
        @pl.when(a_here)
        def _():
            whole = r.ref_gathered.at[pl.ds(0, 4 * TOK), :]
            a_copy(whole, whole, {CORE: 1 - core}).wait_send()

        @pl.when(a_relay)
        def _():
            a_copy(r.a_own, r.a_own, {CORE: 1 - core}).wait_send()

    pre_stats = Exchange(r.pre_stats, 8, 16, mine, in_tensor, send.pre_stats, recv.pre_stats)
    own_hidden = r.pol_hidden[...].astype(F32)
    row = columns_to_rows(r.table, [jnp.sum(own_hidden * own_hidden, axis=1, keepdims=True)])[0:1]
    r.pre_stats[pl.ds(aligned(8 * mine, 8), 8), :] = as_tile(row)
    for half in range(2):
        tile = 2 * rank + half
        for start, size, to in ((0, 256, 256 * tile), (256, 32, MAIN + 32 * tile)):
            here, there = pl.ds(288 * half + start, size), pl.ds(aligned(to, 32), size)
            r.w_in[there, 0:256] = r.w_query[here, :]
            r.w_in[there, 256:384] = r.w_key[here, :]
            r.w_in[there, 384:512] = r.w_value[here, :]
            r.w_back[there, :] = r.w_out[here, :]
    pl.semaphore_wait(pltpu.get_barrier_semaphore(), 22)

    ref_gather = Gather(r.ref_gathered, SHARD, send.gather_ref, recv.gather_ref)
    pol_gather = Gather(r.pol_gathered, SHARD, send.gather_pol, recv.gather_pol)
    weights = Weights(r.w_in, r.w_back, send.y, recv.y, send.d, recv.d)

    def weight_steps():
        for s in range(1, 3):
            weights.step(s, (0,))
            yield
            weights.step(s, (1,))
            if s == 1:
                weights.step(s, (2,))
            yield
        weights.step(2, (2,))
        weights.step(0, (3, 4))
        yield
        for part in range(3):
            weights.step(3, (part,))
            yield
        for s in range(1, 4):
            weights.step(s, (3, 4))
            yield

    pre_stats.start()
    ref_gather.begin()
    weights.step(0, (0, 1, 2))
    for number in range(10, len(inputs)):
        load(number).wait()
    gain = r.pre_ordered
    order_gain(r.pre_gain, gain)
    order_gain(r.post_gain, r.post_ordered)
    pre_gain, post_gain = own_gain(gain, mine), own_gain(r.post_ordered, mine)
    def project(m):
        rows = slice(m * TOK, m * TOK + TOK)
        for i in range(3):
            total = None
            for c in range(3 * i, 3 * i + 3):
                term = dot(r.normed[rows, 512 * c : 512 * c + 512], r.w_in[512 * c : 512 * c + 512, :])
                total = term if total is None else total + term
            r.acc[rows, :] = total if i == 0 else r.acc[rows, :] + total
            yield

    def attend(m):
        for i in range(3):
            at = slice(m * TOK + 96 * i, m * TOK + 96 * i + 96)
            cos, sin = r.cosine[...], r.sine[...]
            key = rope(r.acc[at, 256:384], cos, sin).astype(BF16)
            value = r.acc[at, 384:512].astype(BF16)
            allowed = allowed_here(r.lengths[i])
            r.heads[at, 256:384] = key
            r.heads[at, 384:512] = value
            for g in range(2):
                query = rope(r.acc[at, 128 * g : 128 * g + 128], cos, sin).astype(BF16)
                r.heads[at, 128 * g : 128 * g + 128] = query
                scores = dot(query, key, NT) * QUERY_SCALE
                cap = SOFT_CAP * jnp.tanh(scores / SOFT_CAP)
                weight = jnp.where(allowed, jnp.exp(cap), 0.0)
                prob = weight / jnp.sum(weight, axis=1, keepdims=True)
                r.probs[at, 128 * g : 128 * g + 96] = prob
                r.capped[at, 128 * g : 128 * g + 96] = cap
                r.mixed[at, 128 * g : 128 * g + 128] = dot(prob.astype(BF16), value).astype(BF16)
            yield

    def fill(steps, count):
        for _ in range(count):
            next(steps, None)

    def ref_work():
        unpack_features(r.ref_gathered, SHARD, 0, r.normed, 0)
        yield
        normalize(r.normed, r.scale, gain, 0)
        yield
        weights.arrive(0)
        yield from project(0)
        yield from attend(0)

    lows = HookSum(
        r.low_terms, r.low_parts, r.low, mine, send.low_terms, recv.low_terms, send.low, recv.low, r.hook_parts
    )

    def low_work():
        send_a()
        pre_stats.wait()
        rows_to_columns(r.table, [lax.rsqrt(as_row(pre_stats.total()) / WIDTH + NORM_EPS)])
        own = r.pol_hidden[...].astype(F32) * r.table[0:TOK, 0:1] * pre_gain
        r.own_normed[...] = own.astype(BF16)
        yield
        relay_a()
        yield
        await_a()
        r.low_terms[...] = dot(r.own_normed[...], r.a_own[...]).astype(BF16)
        lows.start()
        yield
        lows.reduce()
        yield

    low = low_work()
    first, second, passing, work = ref_gather.steps(), pol_gather.steps(), weight_steps(), ref_work()
    arrivals = dict(G=first, Q=second, V=passing, C=work, X=low)
    for letter in "GGGVPGGGVQGVQGVXQGVQGVXQGQGVXQVGQGVQGCQVCQCQCCQCQXCQCV":
        if letter == "P":
            pol_gather.begin()
        else:
            fill(arrivals[letter], 1)
    weights.arrive(3)
    for _ in partial_products(r.mixed.at[0:TOK], r.w_back, r.partial):
        pass
    ref_scatter = Scatter(r.partial, r.landing, SHARD, send.scatter_ref, recv.scatter_ref)
    ref_scatter.begin()
    pol_scatter = ShortScatter(r.partial_pol, r.landing_pol, SHARD, send.scatter_pol, recv.scatter_pol)

    def policy():
        unpack_features(r.pol_gathered, SHARD, 0, r.normed, TOK)
        yield
        normalize(r.normed, r.scale, gain, TOK)
        yield
        yield from project(1)
        r.linear[...] = r.acc[TOK : 2 * TOK, :]
        lows.wait()
        query_factor = jnp.concatenate([r.b_query[...], jnp.zeros((RANK, 256), BF16)], axis=0)
        value_factor = jnp.concatenate([jnp.zeros((RANK, 128), BF16), r.b_value[...]], axis=0)
        r.acc[TOK : 2 * TOK, 0:256] += ADAPTER_SCALE * dot(r.low[...], query_factor)
        r.acc[TOK : 2 * TOK, 384:512] += ADAPTER_SCALE * dot(r.low[...], value_factor)
        yield
        yield from attend(1)
        yield from partial_products(r.mixed.at[TOK : 2 * TOK], r.w_back, r.partial_pol)

    def token_sums(m, hidden):
        unpack_result(r.result.at[m], 0, r.summed.at[m])
        summed, readout = r.summed[m], r.readout[...].astype(F32)
        return [
            jnp.sum(summed * summed, axis=1, keepdims=True),
            jnp.sum(summed * post_gain * readout, axis=1, keepdims=True),
            jnp.sum(hidden[...].astype(F32) * readout, axis=1, keepdims=True),
        ]

    ref_stats = Exchange(r.ref_stats, 8, 16, mine, in_tensor, send.ref_stats, recv.ref_stats)
    pol_stats = Exchange(r.pol_stats, 16, 16, mine, in_tensor, send.pol_stats, recv.pol_stats)

    def policy_ring():
        yield from pol_scatter.steps(r.result.at[1])

    def after_ref():
        columns = columns_to_rows(r.table, token_sums(0, r.ref_hidden))
        r.ref_stats[pl.ds(aligned(8 * mine, 8), 8), :] = columns
        ref_stats.start()
        yield

    ref_ring, policy_work, policy_steps = ref_scatter.steps(r.result.at[0]), policy(), policy_ring()
    fill(policy_work, 3)
    for count in (2, 2, 2, 2, 2, 0, 0, 0):
        fill(ref_ring, 1)
        fill(policy_work, count)
    for _ in policy_work:
        pass
    pol_scatter.begin((0,))
    fill(ref_ring, 1)
    pol_scatter.begin((1,))
    fill(ref_ring, 1)
    pol_scatter.begin((2, 3))
    for count in (2, 2, 1):
        fill(ref_ring, 1)
        fill(policy_steps, count)
    together(policy_steps, after_ref(), (1,) + (0,) * 8)
    columns = columns_to_rows(r.table, token_sums(1, r.pol_hidden))
    packed = [columns[k : k + 1, 128 * c : 128 * c + 128] for k in range(3) for c in range(3)]
    packed = jnp.concatenate(packed + [jnp.zeros((7, 128), F32)], axis=0)
    r.pol_stats[pl.ds(aligned(16 * mine, 8), 16), :] = packed
    pol_stats.start()
    pol_stats.wait()
    packed = pol_stats.total()
    pol_total = [
        jnp.concatenate([packed[3 * k + c : 3 * k + c + 1] for c in range(3)], axis=1) for k in range(3)
    ]
    scale_pol = lax.rsqrt(pol_total[0] / WIDTH + NORM_EPS)
    rows_to_columns(r.table, [scale_pol, scale_pol * scale_pol * scale_pol * pol_total[1] / WIDTH])
    readout = r.readout[...].astype(F32)
    bare = r.table[0:TOK, 0:1] * post_gain * readout - r.summed[1] * r.table[0:TOK, 1:2]
    pack_hidden(bare, r.grad_buf, mine * SHARD)
    back_gather = ShortGather(r.grad_buf, SHARD, send.gather_back, recv.gather_back)
    back_gather.begin()

    lane = lax.broadcasted_iota(jnp.int32, (1, 384), 1)
    lengths = [r.lengths[s] for s in range(3)]
    living = jnp.zeros((1, 384), F32)
    for s in range(3):
        living = jnp.where((lane >= 96 * s) & (lane < 96 * s + lengths[s]), 1.0, living)
    ref_stats.wait()
    ref_total = ref_stats.total()
    scale_ref = lax.rsqrt(ref_total[0:1] / WIDTH + NORM_EPS)
    token_scores = (
        (ref_total[2:3] + scale_ref * ref_total[1:2]) * living,
        (pol_total[2] + scale_pol * pol_total[1]) * living,
    )
    row8 = lax.broadcasted_iota(jnp.int32, (8, 128), 0)
    lane8 = lax.broadcasted_iota(jnp.int32, (8, 128), 1)
    tile = jnp.zeros((8, 128), F32)
    for m in range(2):
        for s in range(3):
            inside = (lane >= 96 * s) & (lane < 96 * s + 96)
            score = jnp.sum(jnp.where(inside, token_scores[m], 0.0), axis=1, keepdims=True)
            tile = jnp.where((row8 == m) & (lane8 == 3 * rank + s), score, tile)
    scores = Exchange(r.scores, 8, 8, rank, in_data, send.scores, recv.scores)
    r.scores[pl.ds(aligned(8 * rank, 8), 8), :] = tile
    scores.start()

    def layer_outputs():
        rows_to_columns(r.coefficient, [scale_ref, scale_pol])
        for m, (hidden, out) in enumerate(((r.ref_hidden, r.ref_out), (r.pol_hidden, r.pol_out))):
            scale = r.coefficient[0:TOK, m : m + 1]
            out[...] = (hidden[...].astype(F32) + r.summed[m] * scale * post_gain).astype(BF16)
            yield
            store(1 - m).start()

    def preference():
        scores.wait()
        everyone = scores.total()
        ratio = everyone[1:2] - everyone[0:1]
        row32 = lax.broadcasted_iota(jnp.int32, (32, 128), 0)
        lane32 = lax.broadcasted_iota(jnp.int32, (32, 128), 1)
        named = jnp.full((32, 128), -1, jnp.int32)
        for k in range(24):
            named = jnp.where(row32 == k, r.pairing[k], named)
        chosen = named == lane32
        even = lax.rem(row32, 2) == 0
        picked = jnp.sum(jnp.where(chosen, ratio, 0.0), axis=1, keepdims=True)
        picked = jnp.broadcast_to(picked, (32, 128))
        other = jnp.where(even, pltpu.roll(picked, 31, 0), pltpu.roll(picked, 1, 0))
        margin = DPO_BETA * jnp.where(even, picked - other, other - picked)
        loss = jnp.maximum(-margin, 0.0) + jnp.log1p(jnp.exp(-jnp.abs(margin)))
        counted = even & (row32 < 24) & (lane32 == 0)
        total_loss = jnp.sum(jnp.where(counted, loss, 0.0), axis=(0, 1), keepdims=True)
        r.loss[...] = jnp.broadcast_to(total_loss, (8, 128))
        store(2).start()
        pull = DPO_BETA * LOSS_SCALE / (1.0 + jnp.exp(margin))
        signed = jnp.where(even, -pull, pull)
        coefficients = jnp.sum(jnp.where(chosen, signed, 0.0), axis=0, keepdims=True)
        lane128 = lax.broadcasted_iota(jnp.int32, (1, 128), 1)
        coefficient = jnp.zeros((1, 384), F32)
        for s in range(3):
            own = jnp.sum(jnp.where(lane128 == 3 * rank + s, coefficients, 0.0), axis=1, keepdims=True)
            coefficient = jnp.where((lane >= 96 * s) & (lane < 96 * s + 96), own, coefficient)
        rows_to_columns(r.coefficient, [coefficient * living])
        yield

    def meanwhile():
        yield from layer_outputs()
        yield from preference()

    together(back_gather.steps(), meanwhile(), (1, 1, 0, 0, 0, 0, 0, 1, 0, 0, 0, 0, 0, 0, 0))
    unpack_features(r.grad_buf, SHARD, 0, r.normed, 0)

    for i in range(3):
        total = None
        for c in range(3 * i, 3 * i + 3):
            term = dot(r.normed[0:TOK, 512 * c : 512 * c + 512], r.w_back[512 * c : 512 * c + 512, :])
            total = term if total is None else total + term
        r.grad_mixed[...] = total if i == 0 else r.grad_mixed[...] + total
    r.grad_mixed[...] *= r.coefficient[0:TOK, 0:1]

    for i in range(3):
        here = slice(96 * i, 96 * i + 96)
        at = slice(TOK + 96 * i, TOK + 96 * i + 96)
        cos, sin = r.cosine[...], r.sine[...]
        key, value = r.heads[at, 256:384], r.heads[at, 384:512]
        key_grad = jnp.zeros((96, HEAD), F32)
        value_grad = jnp.zeros((96, HEAD), F32)
        for g in range(2):
            query = r.heads[at, 128 * g : 128 * g + 128]
            incoming = r.grad_mixed[here, 128 * g : 128 * g + 128].astype(BF16)
            prob = r.probs[at, 128 * g : 128 * g + 96]
            cap = r.capped[at, 128 * g : 128 * g + 96] / SOFT_CAP
            grad_probs = dot(incoming, value, NT)
            value_grad = value_grad + dot(prob.astype(BF16), incoming, TN)
            centered = grad_probs - jnp.sum(grad_probs * prob, axis=1, keepdims=True)
            grad_scores = (prob * centered * (1.0 - cap * cap) * QUERY_SCALE).astype(BF16)
            query_grad = dot(grad_scores, key)
            key_grad = key_grad + dot(grad_scores, query, TN)
            r.grads[here, 128 * g : 128 * g + 128] = rope(query_grad, cos, -sin).astype(BF16)
        r.grads[here, 256:384] = rope(key_grad, cos, -sin).astype(BF16)
        r.grads[here, 384:512] = value_grad.astype(BF16)

    query_factor = jnp.concatenate([r.b_query[...], jnp.zeros((RANK, 256), BF16)], axis=0)
    value_factor = jnp.concatenate([jnp.zeros((RANK, 128), BF16), r.b_value[...]], axis=0)
    hook = dot(r.grads[:, 0:256], query_factor, NT) + dot(r.grads[:, 384:512], value_factor, NT)
    r.hooks[...] = (ADAPTER_SCALE * hook).astype(BF16)
    hooks = HookSum(
        r.hooks,
        r.hook_parts,
        r.hook_sums,
        mine,
        send.hooks,
        recv.hooks,
        send.hook_sums,
        recv.hook_sums,
        r.hook_parts,
    )
    hooks.start()
    stats_back = Exchange(r.stats_back, 8, 16, mine, in_tensor, send.stats_back, recv.stats_back)
    factors = Exchange(r.factors, 64, 8, rank, in_data, send.factors, recv.factors)
    for _ in partial_products(r.grads, r.w_in, r.partial_back):
        pass
    back_scatter = ShortScatter(
        r.partial_back, r.landing_back, SHARD, send.scatter_back, recv.scatter_back
    )
    back_scatter.begin((0, 1))

    def across(i):
        return pltpu.make_async_remote_copy(
            src_ref=r.a_terms.at[pl.ds(aligned(576 * (2 * i + 1 - core), 64), 576), :],
            dst_ref=r.a_across.at[pl.ds(576 * i, 576), :],
            send_sem=send.across.at[i],
            recv_sem=recv.across.at[i],
            device_id={CORE: 1 - core},
            device_id_type=MESH,
        )

    def round_y(source, target, to):
        return pltpu.make_async_remote_copy(
            src_ref=source,
            dst_ref=target,
            send_sem=send.round.at[0],
            recv_sem=recv.round.at[0],
            device_id={Y: to},
            device_id_type=MESH,
        )

    three = r.a_round.at[pl.ds(0, 3 * 576), :]
    rounds = round_y(three, three, lax.rem(y + 1, 4))

    def pair_up(i):
        across(i).wait_recv()
        rows = slice(576 * i, 576 * i + 576)
        own = r.a_terms[pl.ds(aligned(576 * (2 * i + core), 64), 576), :].astype(F32)
        r.a_pairs[rows, :] = (own + r.a_across[rows, :].astype(F32)).astype(BF16)

        @pl.when(y != i)
        def _():
            place = pl.ds(aligned(576 * lax.rem(i - y + 4, 4), 64), 576)
            round_y(r.a_pairs.at[pl.ds(576 * i, 576), :], r.a_round.at[place, :], i).start()

    def adapters_back():
        pull_back = jnp.sum(r.grads[...].astype(F32) * r.linear[...], axis=1, keepdims=True)
        pull_back += jnp.sum(r.hooks[...].astype(F32) * r.low[...].astype(F32), axis=1, keepdims=True)
        row = columns_to_rows(r.table, [pull_back])[0:1]
        r.stats_back[pl.ds(aligned(8 * mine, 8), 8), :] = as_tile(row)
        stats_back.start()
        factor_terms = ADAPTER_SCALE * dot(r.low[...], r.grads[:, 0:512], TN)
        own_factor = pl.ds(aligned(64 * rank, 64), 64)
        r.factors[own_factor, 0:256] = factor_terms[0:64, 0:256].astype(BF16)
        r.factors[own_factor, 256:384] = factor_terms[64:128, 384:512].astype(BF16)
        factors.start()
        yield
        hooks.wait()
        hook_low = r.hook_sums[...]
        r.summed[0] = dot(hook_low, r.a_own[...], NT)
        for q in range(4):
            at = MAIN + 128 * q
            tail = dot(r.normed[TOK : 2 * TOK, at : at + 128], hook_low, TN).astype(BF16)
            for t in range(4 * q, 4 * q + 4):
                term = dot(r.normed[TOK : 2 * TOK, 256 * t : 256 * t + 256], hook_low, TN)
                r.a_terms[288 * t : 288 * t + 256, :] = term.astype(BF16)
                j = t - 4 * q
                r.a_terms[288 * t + 256 : 288 * t + 288, :] = tail[32 * j : 32 * j + 32, :]
            across(q).start()
            if q:
                pair_up(q - 1)
            yield
        pair_up(3)
        yield

    adapters = adapters_back()
    fill(adapters, 1)
    back_scatter.begin((2,))
    hooks.reduce()
    back_scatter.begin((3,))
    together(back_scatter.steps(r.result.at[0]), adapters, (0, 0, 0, 2, 2, 1, 0, 0, 0))

    stats_back.wait()
    rows_to_columns(r.table, [as_row(stats_back.total())])
    unpack_result(r.result.at[0], 0, r.summed.at[1])
    pre_scale = r.scale[TOK : 2 * TOK, 0:1]
    shrink_back = pre_scale * pre_scale * r.table[0:TOK, 0:1] / WIDTH
    grad_result = r.coefficient[0:TOK, 0:1] * r.readout[...].astype(F32)
    hidden = r.pol_hidden[...].astype(F32)
    r.grad_hidden[...] = (
        grad_result + pre_scale * pre_gain * (r.summed[1] + r.summed[0]) - hidden * shrink_back
    ).astype(BF16)
    store(3).start()
    factors.wait()
    factor_total = factors.total()
    r.query_grad[...] = factor_total[:, 0:256]
    r.value_grad[...] = factor_total[:, 256:384]
    store(5).start()
    store(6).start()
    whole = r.a_pairs[pl.ds(aligned(576 * y, 64), 576), :].astype(F32)
    rounds.wait_recv()
    for i in range(1, 4):
        whole = whole + r.a_round[576 * i : 576 * i + 576, :].astype(F32)
    r.grad_a[...] = whole
    store(4).start()
    drain_a()
    for ring in (ref_gather, pol_gather, weights, ref_scatter, pol_scatter, back_gather, back_scatter):
        ring.drain()
    for exchange in (pre_stats, ref_stats, pol_stats, scores, lows, hooks, stats_back, factors):
        exchange.drain()
    for i in range(4):
        across(i).wait_send()
    rounds.wait_send()
    for number in range(len(outputs)):
        store(number).wait()


def partial_products(rows, matrix, partial):
    for block in range(4):
        left = rows[...]
        for t in range(4 * block, 4 * block + 4):
            product = dot(left, matrix[256 * t : 256 * t + 256, :], NT).astype(BF16)
            for half in range(2):
                at = t * SHARD + TOK * half
                partial[at : at + TOK, :] = product[:, 128 * half : 128 * half + 128]
        at = MAIN + 128 * block
        product = dot(left, matrix[at : at + 128, :], NT).astype(BF16)
        for j in range(4):
            at = (4 * block + j) * SHARD + 2 * TOK
            partial[at : at + GROUP, :] = pack_tail(product[:, 32 * j : 32 * j + 32])
        yield


def rotation_tables():
    spacing = ROPE_BASE ** (-2.0 * np.arange(64, dtype=np.float32) / HEAD)
    angles = np.arange(LENGTH, dtype=np.float32)[:, None] * spacing.astype(np.float32)[None, :]
    cosine, sine = np.cos(angles), np.sin(angles)
    return (
        np.concatenate([cosine, cosine], axis=1).astype(np.float32),
        np.concatenate([-sine, sine], axis=1).astype(np.float32),
    )


INPUTS = dict(
    lengths=None,
    pairing=None,
    ref_hidden=((TOK, TOK), BF16),
    pol_hidden=((TOK, TOK), BF16),
    w_query=((576, 256), BF16),
    w_key=((576, 128), BF16),
    w_value=((576, 128), BF16),
    w_out=((576, 256), BF16),
    a_query=((RANK, 576), BF16),
    a_value=((RANK, 576), BF16),
    readout=((TOK, TOK), BF16),
    b_query=((RANK, 256), BF16),
    b_value=((RANK, 128), BF16),
    pre_gain=((36, 128), F32),
    post_gain=((36, 128), F32),
    cosine=((LENGTH, HEAD), F32),
    sine=((LENGTH, HEAD), F32),
)
OUTPUTS = dict(
    pol_out=((TOK, TOK), BF16),
    ref_out=((TOK, TOK), BF16),
    loss=((8, 128), F32),
    grad_hidden=((TOK, TOK), BF16),
    grad_a=((576, 128), F32),
    query_grad=((RANK, 256), F32),
    value_grad=((RANK, 128), F32),
)


def hand_out(*refs):
    for source, target in zip(refs[: len(OUTPUTS)], refs[len(OUTPUTS) :]):
        target[...] = source[0 : target.shape[0], 0 : target.shape[1]]


def body(
    ref_hidden,
    pol_hidden,
    readout,
    lengths,
    pairing,
    pre_gain,
    post_gain,
    w_query,
    w_key,
    value_projection,
    w_out,
    a_query,
    a_value,
    query_second_factor,
    value_second_factor,
):
    vmem, whole = pl.BlockSpec(memory_space=pltpu.VMEM), pl.BlockSpec(memory_space=pl.ANY)
    cosine, sine = rotation_tables()
    dma = pltpu.SemaphoreType.DMA
    staged = [pltpu.VMEM(*kind) if kind else None for kind in list(INPUTS.values()) + list(OUTPUTS.values())]
    staged[0:2] = [pltpu.SMEM((3,), jnp.int32), pltpu.SMEM((24,), jnp.int32)]
    results = pl.pallas_call(
        step_body,
        out_shape=tuple(jax.ShapeDtypeStruct(*kind) for kind in OUTPUTS.values()),
        in_specs=[whole] * len(INPUTS),
        out_specs=(whole,) * len(OUTPUTS),
        scratch_shapes=staged
        + [pltpu.VMEM(shape, kind) for shape, kind in SCRATCH.values()]
        + [dma((len(INPUTS),)), dma((len(OUTPUTS),))]
        + [dma((count,)) for pair in SEMAPHORES.values() for count in pair],
        compiler_params=pltpu.CompilerParams(
            collective_id=0, has_side_effects=True, vmem_limit_bytes=62 * 1024 * 1024
        ),
    )(
        lengths,
        pairing,
        ref_hidden,
        pol_hidden,
        w_query,
        w_key,
        value_projection,
        w_out,
        a_query.T,
        a_value.T,
        readout,
        query_second_factor,
        value_second_factor,
        pre_gain.reshape(36, 128),
        post_gain.reshape(36, 128),
        jnp.asarray(cosine),
        jnp.asarray(sine),
    )
    shapes = [jax.ShapeDtypeStruct(a.shape, a.dtype) for a in results]
    shapes[2] = jax.ShapeDtypeStruct((1, 1), F32)
    pol_out, ref_out, loss, grad_hidden, grad_a, query_grad, value_grad = pl.pallas_call(
        hand_out,
        out_shape=tuple(shapes),
        in_specs=[vmem] * len(OUTPUTS),
        out_specs=(vmem,) * len(OUTPUTS),
    )(*results)
    return (pol_out, ref_out, loss.reshape(()), grad_hidden, grad_a, query_grad, value_grad)


def solution(mesh):
    torus = Mesh(mesh.devices.reshape(4, 2, 4, 4), (Y, CORE, X, Z))
    split, rows, columns = P(DP, TENSOR), P(DP, None), P(None, TENSOR)
    return jax.shard_map(
        body,
        mesh=torus,
        in_specs=(split, split, split, P(DP), P(), P(), P(), split, split, split, split, rows, rows, columns, columns),
        out_specs=(split, split, P(), split, rows, columns, columns),
        check_vma=False,
    )
```

```python
import jax
import jax.numpy as jnp
import numpy as np
from jax import lax
from jax.experimental import pallas as pl
from jax.experimental.pallas import tpu as pltpu
from jax.sharding import Mesh
from jax.sharding import PartitionSpec as P

Y, CORE, X, Z = "dp_0", "dp_1", "tensor_0", "tensor_1"
DP, TENSOR = (Y, CORE), (X, Z)
MESH = pl.DeviceIdType.MESH

WIDTH = 4608
TOK = 288
LENGTH = 96
HEAD = 128
RANK = 64
NORM_EPS = 1e-06
SOFT_CAP = 50.0
ADAPTER_SCALE = 0.5
DPO_BETA = 0.5
LOSS_SCALE = 256.0
ROPE_BASE = 10000.0
QUERY_SCALE = float(WIDTH // 32) ** (-0.5)

GROUP = 80
SHARD = 2 * TOK + GROUP
MAIN = 4096
RINGS = ((0, 1), (0, -1), (1, 1), (1, -1))

ORDER = (2, 1, 3, 0)

F32 = jnp.float32
BF16 = jnp.bfloat16
NT = (((1,), (1,)), ((), ()))
TN = (((0,), (0,)), ((), ()))


def dot(a, b, dims=(((1,), (0,)), ((), ())), precision=None):
    return lax.dot_general(a, b, dims, preferred_element_type=F32, precision=precision)


def aligned(start, multiple):
    return start if isinstance(start, int) else pl.multiple_of(start, multiple)


def back(position, hops, direction):
    return lax.rem(position - hops * direction + 8, 4)


def chunks_of(rows):
    tiles = rows // 16
    sizes = [16 * (tiles // 4 + (1 if k < tiles % 4 else 0)) for k in range(4)]
    return sizes, [sum(sizes[:k]) for k in range(4)]


class Ring:
    def __init__(self, rows, send, recv):
        self.rows = rows
        self.sizes, self.starts = chunks_of(rows)
        self.send, self.recv = send, recv
        self.at = (lax.axis_index(X), lax.axis_index(Z))

    def place(self, k, first, second):
        primary, way = RINGS[k]
        a = back(self.at[primary], first, way)
        b = back(self.at[1 - primary], second, way)
        px, pz = (a, b) if primary == 0 else (b, a)
        return aligned((4 * px + pz) * self.rows + self.starts[k], 16)

    def next_on(self, k, secondary, behind=False):
        primary, way = RINGS[k]
        axis = 1 - primary if secondary else primary
        return {TENSOR[axis]: back(self.at[axis], 1 if behind else -1, way)}

    def remote(self, source, target, number, device):
        return pltpu.make_async_remote_copy(
            src_ref=source,
            dst_ref=target,
            send_sem=self.send.at[0],
            recv_sem=self.recv.at[number],
            device_id=device,
            device_id_type=MESH,
        )

    def arrived(self, number):
        whole = self.memory.at[pl.ds(0, self.rows), :]
        self.remote(whole, whole, number, self.next_on(0, False)).wait_recv()

    def drain(self):
        whole = self.memory.at[pl.ds(0, 15 * self.rows), :]
        self.remote(whole, whole, 0, self.next_on(0, False)).wait_send()


class Gather(Ring):
    def __init__(self, buffer, rows, send, recv):
        super().__init__(rows, send, recv)
        self.memory = buffer

    def piece(self, k, j, s):
        return self.memory.at[pl.ds(self.place(k, j, s), self.sizes[k]), :]

    def first(self, k, number):
        piece = self.piece(k, 1 if number == 1 else 0, 0)
        return self.remote(piece, piece, number, self.next_on(k, False, number == 2))

    def second(self, k, j, s):
        piece = self.piece(k, j, s)
        return self.remote(piece, piece, 3 + 3 * j + s, self.next_on(k, True))

    def begin(self):
        for k in range(4):
            self.first(k, 0).start()
            self.first(k, 2).start()
        for k in range(4):
            self.second(k, 0, 0).start()

    def await_first(self, number):
        self.arrived(number)
        for k in range(4):
            if number == 0:
                self.first(k, 1).start()
            self.second(k, number + 1, 0).start()

    def await_second(self, j, s):
        self.arrived(3 + 3 * j + s)
        if s < 2:
            for k in range(4):
                self.second(k, j, s + 1).start()

    def steps(self):
        self.await_first(0)
        yield
        self.await_first(2)
        yield
        self.await_second(0, 0)
        yield
        self.await_first(1)
        yield
        for j, s in ((1, 0), (3, 0), (0, 1), (2, 0), (1, 1), (3, 1), (0, 2), (2, 1), (1, 2), (3, 2), (2, 2)):
            self.await_second(j, s)
            yield


class ShortGather(Gather):
    def second(self, k, j, number):
        piece = self.piece(k, j, 1 if number == 1 else 0)
        return self.remote(piece, piece, 3 + 3 * j + number, self.next_on(k, True, number == 2))

    def begin(self):
        for k in range(4):
            self.first(k, 0).start()
            self.first(k, 2).start()
        for k in range(4):
            self.second(k, 0, 0).start()
            self.second(k, 0, 2).start()

    def await_first(self, number):
        self.arrived(number)
        for k in range(4):
            if number == 0:
                self.first(k, 1).start()
            self.second(k, number + 1, 0).start()
            self.second(k, number + 1, 2).start()

    def await_second(self, j, number):
        self.arrived(3 + 3 * j + number)
        if number == 0:
            for k in range(4):
                self.second(k, j, 1).start()

    def steps(self):
        self.await_first(0)
        yield
        self.await_first(2)
        yield
        self.await_second(0, 0)
        yield
        self.await_first(1)
        yield
        for j, number in (
            (0, 2), (1, 0), (3, 0), (2, 0), (1, 2), (3, 2), (0, 1), (1, 1), (2, 2), (3, 1), (2, 1)
        ):
            self.await_second(j, number)
            yield


class Scatter(Ring):
    def __init__(self, partial, landing, rows, send, recv):
        super().__init__(rows, send, recv)
        self.partial, self.landing, self.memory = partial, landing, landing

    def piece(self, k, first, second):
        return self.partial.at[pl.ds(self.place(k, first, second), self.sizes[k]), :]

    def slot(self, k, number):
        return self.landing.at[pl.ds(15 * self.starts[k] + number * self.sizes[k], self.sizes[k]), :]

    def outer(self, k, j, s):
        number = 3 * j + s
        return self.remote(self.piece(k, ORDER[j], s + 1), self.slot(k, number), number, self.next_on(k, True))

    def inner(self, k, number):
        piece = self.piece(k, (2, 3, 1)[number - 12], 0)
        return self.remote(piece, self.slot(k, number), number, self.next_on(k, False, number == 14))

    def add(self, k, number, first, second):
        piece, slot = self.piece(k, first, second), self.slot(k, number)
        piece[...] = (piece[...].astype(F32) + slot[...].astype(F32)).astype(BF16)

    def begin(self, parts=range(4)):
        for j in parts:
            for k in range(4):
                self.outer(k, j, 0).start()

    def steps(self, result):
        for s in range(3):
            for j in range(4):
                self.arrived(3 * j + s)
                if s == 2 and j == 2:
                    self.arrived(12)
                for k in range(4):
                    self.add(k, 3 * j + s, ORDER[j], s + 2)
                    if s < 2:
                        self.outer(k, j, s + 1).start()
                    elif j == 0:
                        self.inner(k, 12).start()
                    elif j == 1:
                        self.inner(k, 14).start()
                    elif j == 2:
                        self.add(k, 12, 3, 0)
                        self.inner(k, 13).start()
                yield
        self.arrived(14)
        self.arrived(13)
        for k in range(4):
            own = self.piece(k, 0, 0)[...].astype(F32)
            for number in (14, 13):
                own = own + self.slot(k, number)[...].astype(F32)
            result[pl.ds(self.starts[k], self.sizes[k]), :] = own
        yield


class ShortScatter(Scatter):
    def outer(self, k, j, number):
        piece = self.piece(k, ORDER[j], (2, 3, 1)[number])
        slot = self.slot(k, 3 * j + number)
        return self.remote(piece, slot, 3 * j + number, self.next_on(k, True, number == 2))

    def hand_on(self, j, number):
        for k in range(4):
            self.outer(k, j, number).start()

    def close(self, j):
        self.arrived(3 * j + 1)
        self.arrived(3 * j + 2)
        for k in range(4):
            piece = self.piece(k, ORDER[j], 0)
            value = piece[...].astype(F32)
            for number in (1, 2):
                value = value + self.slot(k, 3 * j + number)[...].astype(F32)
            piece[...] = value.astype(BF16)

    def steps(self, result):
        for j in range(4):
            self.arrived(3 * j)
            for k in range(4):
                self.add(k, 3 * j, ORDER[j], 3)
                self.outer(k, j, 1).start()
            if j < 2:
                self.hand_on(j, 2)
            yield
        self.close(0)
        for k in range(4):
            self.inner(k, 12).start()
        self.hand_on(2, 2)
        self.hand_on(3, 2)
        yield
        self.close(1)
        for k in range(4):
            self.inner(k, 14).start()
        yield
        self.close(2)
        self.arrived(12)
        for k in range(4):
            self.add(k, 12, 3, 0)
            self.inner(k, 13).start()
        yield
        self.close(3)
        yield
        self.arrived(14)
        self.arrived(13)
        for k in range(4):
            own = self.piece(k, 0, 0)[...].astype(F32)
            for number in (14, 13):
                own = own + self.slot(k, number)[...].astype(F32)
            result[pl.ds(self.starts[k], self.sizes[k]), :] = own
        yield


class Weights:
    def __init__(self, w_in, w_back, y_send, y_recv, d_send, d_recv):
        self.w_in, self.w_back = w_in, w_back
        self.sems = (y_send, y_recv, d_send, d_recv)
        self.y, self.core = lax.axis_index(Y), lax.axis_index(CORE)

    def block(self, hops, half, part, core):
        way = 1 - 2 * half
        tile = 2 * (2 * back(self.y, hops, way) + core) + half
        if part < 2:
            return self.w_in.at[pl.ds(aligned(256 * tile + 128 * part, 128), 128), :]
        if part == 3:
            return self.w_back.at[pl.ds(aligned(256 * tile, 256), 256), :]
        ref = self.w_in if part == 2 else self.w_back
        return ref.at[pl.ds(aligned(MAIN + 32 * tile, 32), 32), :]

    def round(self, s, half, part):
        ref = self.block(s, half, part, self.core)
        return self.copy(ref, 0, part, 5 * s + part, {Y: back(self.y, -1, 1 - 2 * half)})

    def across(self, i, half, part):
        return self.copy(self.block(i, half, part, self.core), 2, part, part // 3, {CORE: 1 - self.core})

    def copy(self, ref, way, part, number, device):
        return pltpu.make_async_remote_copy(
            src_ref=ref,
            dst_ref=ref,
            send_sem=self.sems[way].at[part // 3],
            recv_sem=self.sems[way + 1].at[number],
            device_id=device,
            device_id_type=MESH,
        )

    def rows(self, part, count):
        return (self.w_in if part < 3 else self.w_back).at[pl.ds(0, count), :]

    def step(self, s, parts):
        for part in parts:
            if s > 0:
                both = self.rows(part, 2 * (128, 128, 32, 256, 32)[part])
                self.copy(both, 0, part, 5 * (s - 1) + part, {CORE: 1 - self.core}).wait_recv()
            for half in range(2):
                if s < 3:
                    self.round(s, half, part).start()
                self.across(s, half, part).start()

    def arrive(self, part):
        self.copy(self.rows(part, 8 * TOK), 2, part, part // 3, {CORE: 1 - self.core}).wait_recv()

    def drain(self):
        for part in (0, 3):
            self.copy(self.rows(part, 6 * TOK), 0, part, 0, {CORE: 1 - self.core}).wait_send()
            self.copy(self.rows(part, 8 * TOK), 2, part, 0, {CORE: 1 - self.core}).wait_send()


class Exchange:
    def __init__(self, buffer, rows, count, me, device_of, send, recv):
        self.buffer, self.rows, self.count, self.me = buffer, rows, count, me
        self.device_of, self.send, self.recv = device_of, send, recv

    def part(self, buffer, i):
        return buffer.at[pl.ds(aligned(i * self.rows, self.rows), self.rows), :]

    def copy(self, source, target, peer):
        return pltpu.make_async_remote_copy(
            src_ref=source,
            dst_ref=target,
            send_sem=self.send.at[0],
            recv_sem=self.recv.at[0],
            device_id=self.device_of(peer),
            device_id_type=MESH,
        )

    def start(self):
        own = self.part(self.buffer, self.me)
        for delta in range(1, self.count):
            self.copy(own, own, lax.rem(self.me + delta, self.count)).start()

    def slots(self, count):
        whole = self.buffer.at[pl.ds(0, count * self.rows), :]
        return self.copy(whole, whole, lax.rem(self.me + 1, self.count))

    def wait(self):
        self.slots(self.count - 1).wait_recv()

    def total(self):
        value = self.buffer[0 : self.rows, :].astype(F32)
        for i in range(1, self.count):
            value = value + self.buffer[self.rows * i : self.rows * i + self.rows, :].astype(F32)
        return value

    def drain(self):
        self.slots(self.count - 1).wait_send()


OWNERS = 9


class HookSum:
    def __init__(self, terms, parts, sums, me, send_parts, recv_parts, send_sums, recv_sums, narrow):
        self.terms, self.parts, self.sums, self.me = terms, parts, sums, me
        self.there = Exchange(parts, 32, 16, me, in_tensor, send_parts, recv_parts)
        self.home = Exchange(narrow, 32, 16, me, in_tensor, send_sums, recv_sums)
        self.owner = me < OWNERS

    def start(self):
        @pl.when(self.owner)
        def _():
            own = pl.ds(aligned(32 * self.me, 32), 32)
            self.parts[own, :] = self.terms[own, :]

        for delta in range(1, 16):
            peer = lax.rem(self.me + delta, 16)

            @pl.when(peer < OWNERS)
            def _():
                self.there.copy(self.there.part(self.terms, peer), self.there.part(self.parts, self.me), peer).start()

    def reduce(self):
        @pl.when(self.owner)
        def _():
            self.there.wait()
            self.sums[pl.ds(aligned(32 * self.me, 32), 32), :] = self.there.total().astype(BF16)
            own = self.home.part(self.sums, self.me)
            for delta in range(1, 16):
                self.home.copy(own, own, lax.rem(self.me + delta, 16)).start()

    def wait(self):
        @pl.when(self.owner)
        def _():
            self.home.slots(OWNERS - 1).wait_recv()

        @pl.when(jnp.logical_not(self.owner))
        def _():
            self.home.slots(OWNERS).wait_recv()

    def drain(self):
        @pl.when(self.owner)
        def _():
            self.there.slots(OWNERS - 1).wait_send()
            self.home.slots(15).wait_send()

        @pl.when(jnp.logical_not(self.owner))
        def _():
            self.there.slots(OWNERS).wait_send()


def in_tensor(i):
    return {X: lax.div(i, 4), Z: lax.rem(i, 4)}


def in_data(i):
    return {Y: lax.div(i, 2), CORE: lax.rem(i, 2)}


def together(main, filler, ratio):
    for number, _ in enumerate(main):
        for _ in range(ratio if isinstance(ratio, int) else ratio[number]):
            next(filler, None)
    for _ in filler:
        pass


def signal(peers):
    barrier = pltpu.get_barrier_semaphore()
    for peer in peers:
        pl.semaphore_signal(barrier, inc=1, device_id=peer, device_id_type=MESH)


def pack_tail(tail):
    last = jnp.concatenate([tail[240:288], jnp.zeros((32, 32), tail.dtype)], axis=0)
    return jnp.concatenate([tail[0:80], tail[80:160], tail[160:240], last], axis=1)


GROUPS = ((0, 80), (80, 80), (160, 80), (240, 48))


def unpack_features(buffer, rows, offset, target, row_offset):
    def main(t, carry):
        base = aligned(t * rows + offset, 16)
        for half in range(2):
            target[pl.ds(row_offset, TOK), pl.ds(aligned(256 * t + 128 * half, 128), 128)] = buffer[
                pl.ds(aligned(base + TOK * half, 16), TOK), :
            ]
        return carry

    lax.fori_loop(0, 16, main, 0)

    def tail(q, carry):
        tails = [
            buffer[pl.ds(aligned((4 * q + j) * rows + offset + 2 * TOK, 16), GROUP), :] for j in range(4)
        ]
        for g, (start, size) in enumerate(GROUPS):
            joined = jnp.concatenate([t[:size, 32 * g : 32 * g + 32] for t in tails], axis=1)
            target[pl.ds(row_offset + start, size), pl.ds(aligned(MAIN + 128 * q, 128), 128)] = joined
        return carry

    lax.fori_loop(0, 4, tail, 0)


def unpack_result(packed, offset, target):
    for half in range(2):
        target[:, 128 * half : 128 * half + 128] = packed[offset + TOK * half : offset + TOK * half + TOK, :]
    for g, (start, size) in enumerate(GROUPS):
        base = offset + 2 * TOK
        target[start : start + size, 256:288] = packed[base : base + size, 32 * g : 32 * g + 32]


def pack_hidden(hidden, buffer, base):
    for half in range(2):
        buffer[pl.ds(aligned(base + TOK * half, 16), TOK), :] = hidden[:, 128 * half : 128 * half + 128].astype(
            BF16
        )
    buffer[pl.ds(aligned(base + 2 * TOK, 16), GROUP), :] = pack_tail(hidden[:, 256:288]).astype(BF16)


def feature_lanes(gain, start, count):
    pieces = []
    while count:
        row, lane = divmod(start, 128)
        size = min(count, 128 - lane)
        pieces.append(gain[row : row + 1, lane : lane + size])
        start, count = start + size, count - size
    return pieces[0] if len(pieces) == 1 else jnp.concatenate(pieces, axis=1)


def order_gain(gain, target):
    for c in range(32):
        target[c : c + 1, :] = feature_lanes(gain, 288 * (c // 2) + 128 * (c % 2), 128)
    for q in range(4):
        tails = [feature_lanes(gain, 288 * (4 * q + j) + 256, 32) for j in range(4)]
        target[32 + q : 33 + q, :] = jnp.concatenate(tails, axis=1)


def own_gain(ordered, mine):
    tail = ordered[pl.ds(32 + lax.div(mine, 4), 1), :]
    picked = jnp.zeros((1, 32), F32)
    for j in range(4):
        picked = jnp.where(lax.rem(mine, 4) == j, tail[:, 32 * j : 32 * j + 32], picked)
    return jnp.concatenate([ordered[pl.ds(2 * mine, 1), :], ordered[pl.ds(2 * mine + 1, 1), :], picked], axis=1)


def normalize(normed, scale_ref, gain_ref, offset):
    def rows(i, carry):
        at = pl.ds(aligned(offset + 96 * i, 96), 96)
        squares = jnp.zeros((96, 128), F32)
        for c in range(36):
            x = normed[at, 128 * c : 128 * c + 128].astype(F32)
            squares = squares + x * x
        scale = lax.rsqrt(jnp.sum(squares, axis=1, keepdims=True) / WIDTH + NORM_EPS)
        scale_ref[at, :] = jnp.broadcast_to(scale, (96, 128))
        for c in range(36):
            x = normed[at, 128 * c : 128 * c + 128].astype(F32)
            normed[at, 128 * c : 128 * c + 128] = (x * scale * gain_ref[c : c + 1, :]).astype(BF16)
        return carry

    lax.fori_loop(0, 3, rows, 0)


def rope(x, cosine, sine):
    return x * cosine + pltpu.roll(x, 64, 1) * sine


def allowed_here(length):
    query = lax.broadcasted_iota(jnp.int32, (LENGTH, LENGTH), 0)
    key = lax.broadcasted_iota(jnp.int32, (LENGTH, LENGTH), 1)
    return (key <= query) & (key < length)


def columns_to_rows(scratch, columns):
    lane = lax.broadcasted_iota(jnp.int32, (TOK, 128), 1)
    table = jnp.zeros((TOK, 128), F32)
    for k, column in enumerate(columns):
        table = jnp.where(lane == k, column, table)
    scratch[0:TOK, :] = table
    scratch[TOK:384, :] = jnp.zeros((384 - TOK, 128), F32)
    return jnp.transpose(scratch[...])[0:8, :]


def as_tile(row):
    pieces = [row[:, 128 * c : 128 * c + 128] for c in range(3)]
    return jnp.concatenate(pieces + [jnp.zeros((5, 128), F32)], axis=0)


def as_row(tile):
    return jnp.concatenate([tile[c : c + 1] for c in range(3)], axis=1)


def rows_to_columns(scratch, rows):
    missing = 128 - sum(row.shape[0] for row in rows)
    filled = jnp.concatenate(list(rows) + [jnp.zeros((missing, 384), F32)], axis=0)
    scratch[...] = jnp.transpose(filled)


SCRATCH = dict(
    ref_gathered=((16 * SHARD, 128), BF16),
    pol_gathered=((16 * SHARD, 128), BF16),
    w_in=((WIDTH, 512), BF16),
    a_all=((640, 128), BF16),
    a_own=((TOK, 128), BF16),
    w_back=((WIDTH, 256), BF16),
    normed=((2 * TOK, WIDTH), BF16),
    scale=((2 * TOK, 128), F32),
    acc=((2 * TOK, 512), F32),
    linear=((TOK, 512), F32),
    pre_stats=((16 * 8, 128), F32),
    own_normed=((TOK, TOK), BF16),
    low_terms=((TOK, 128), BF16),
    low_parts=((16 * 32, 128), BF16),
    low=((TOK, 128), BF16),
    heads=((2 * TOK, 512), BF16),
    mixed=((2 * TOK, 256), BF16),
    probs=((2 * TOK, 256), F32),
    capped=((2 * TOK, 256), F32),
    partial=((16 * SHARD, 128), BF16),
    partial_pol=((16 * SHARD, 128), BF16),
    landing=((15 * SHARD, 128), BF16),
    landing_pol=((15 * SHARD, 128), BF16),
    result=((2, SHARD, 128), F32),
    summed=((2, TOK, TOK), F32),
    table=((384, 128), F32),
    coefficient=((384, 128), F32),
    ref_stats=((16 * 8, 384), F32),
    pol_stats=((16 * 16, 128), F32),
    pre_ordered=((40, 128), F32),
    post_ordered=((40, 128), F32),
    scores=((8 * 8, 128), F32),
    grad_buf=((16 * SHARD, 128), BF16),
    grad_mixed=((TOK, 256), F32),
    grads=((TOK, 512), BF16),
    partial_back=((16 * SHARD, 128), BF16),
    landing_back=((15 * SHARD, 128), BF16),
    hooks=((TOK, 128), BF16),
    hook_parts=((16 * 32, 128), BF16),
    hook_sums=((TOK, 128), BF16),
    stats_back=((16 * 8, 128), F32),
    factors=((8 * 64, 384), BF16),
    a_terms=((WIDTH, 128), BF16),
    a_across=((4 * 576, 128), BF16),
    a_pairs=((4 * 576, 128), BF16),
    a_round=((4 * 576, 128), BF16),
)
SEMAPHORES = dict(
    gather_ref=(1, 15),
    gather_pol=(1, 15),
    a=(1, 1),
    pre_stats=(1, 1),
    low_terms=(1, 1),
    low=(1, 1),
    scatter_ref=(1, 15),
    scatter_pol=(1, 15),
    gather_back=(1, 15),
    scatter_back=(1, 15),
    y=(2, 15),
    d=(2, 2),
    ref_stats=(1, 1),
    pol_stats=(1, 1),
    scores=(1, 1),
    hooks=(1, 1),
    hook_sums=(1, 1),
    stats_back=(1, 1),
    factors=(1, 1),
    across=(4, 4),
    round=(1, 1),
)


class Refs:
    pass


def step_body(*refs):
    inputs, outputs = list(INPUTS), list(OUTPUTS)
    outside, refs = refs[: len(inputs + outputs)], refs[len(inputs + outputs) :]
    names = inputs + outputs + list(SCRATCH)
    r, send, recv = Refs(), Refs(), Refs()
    for name, ref in zip(names, refs):
        setattr(r, name, ref)
    load_sems, store_sems, *sems = refs[len(names) :]
    for number, name in enumerate(SEMAPHORES):
        setattr(send, name, sems[2 * number])
        setattr(recv, name, sems[2 * number + 1])

    x, z = lax.axis_index(X), lax.axis_index(Z)
    y, core = lax.axis_index(Y), lax.axis_index(CORE)
    mine, rank = 4 * x + z, 2 * y + core
    def load(number):
        return pltpu.make_async_copy(outside[number], refs[number], load_sems.at[number])

    def store(number):
        at = len(inputs) + number
        return pltpu.make_async_copy(refs[at], outside[at], store_sems.at[number])

    signal(
        [in_tensor(lax.rem(mine + i, 16)) for i in range(1, 16)]
        + [in_data(lax.rem(rank + i, 8)) for i in range(1, 8)]
    )
    for number in range(len(inputs)):
        load(number).start()
    for number in range(10):
        load(number).wait()
    pack_hidden(r.ref_hidden[...], r.ref_gathered, mine * SHARD)
    pack_hidden(r.pol_hidden[...], r.pol_gathered, mine * SHARD)
    a_both = jnp.concatenate([r.a_query[...].astype(F32), r.a_value[...].astype(F32)], axis=0)
    r.a_all[...] = jnp.transpose(jnp.concatenate([a_both, jnp.zeros((128, 64), F32)], axis=1)).astype(BF16)
    a_rank = lax.div(mine, 2)
    a_here, a_core = rank == a_rank, core == lax.rem(a_rank, 2)
    a_relay = a_core & (y != lax.div(a_rank, 2))
    a_rows = pl.ds(aligned(TOK * lax.rem(mine, 2), 32), TOK)

    @pl.when(a_here)
    def _():
        r.a_own[...] = r.a_all[a_rows, :]

    def a_copy(source, target, device):
        return pltpu.make_async_remote_copy(
            src_ref=source,
            dst_ref=target,
            send_sem=send.a.at[0],
            recv_sem=recv.a.at[0],
            device_id=device,
            device_id_type=MESH,
        )

    def send_a():
        @pl.when(a_here)
        def _():
            for device in [{Y: lax.rem(y + i, 4)} for i in (1, 3, 2)] + [{CORE: 1 - core}]:
                a_copy(r.a_all.at[a_rows, :], r.a_own, device).start()

    def relay_a():
        @pl.when(a_relay)
        def _():
            a_copy(r.a_own, r.a_own, {CORE: 1 - core}).wait_recv()
            a_copy(r.a_own, r.a_own, {CORE: 1 - core}).start()

    def await_a():
        @pl.when(jnp.logical_not(a_core))
        def _():
            a_copy(r.a_own, r.a_own, {CORE: 1 - core}).wait_recv()

    def drain_a():
        @pl.when(a_here)
        def _():
            whole = r.ref_gathered.at[pl.ds(0, 4 * TOK), :]
            a_copy(whole, whole, {CORE: 1 - core}).wait_send()

        @pl.when(a_relay)
        def _():
            a_copy(r.a_own, r.a_own, {CORE: 1 - core}).wait_send()

    pre_stats = Exchange(r.pre_stats, 8, 16, mine, in_tensor, send.pre_stats, recv.pre_stats)
    own_hidden = r.pol_hidden[...].astype(F32)
    row = columns_to_rows(r.table, [jnp.sum(own_hidden * own_hidden, axis=1, keepdims=True)])[0:1]
    r.pre_stats[pl.ds(aligned(8 * mine, 8), 8), :] = as_tile(row)
    for half in range(2):
        tile = 2 * rank + half
        for start, size, to in ((0, 256, 256 * tile), (256, 32, MAIN + 32 * tile)):
            here, there = pl.ds(288 * half + start, size), pl.ds(aligned(to, 32), size)
            r.w_in[there, 0:256] = r.w_query[here, :]
            r.w_in[there, 256:384] = r.w_key[here, :]
            r.w_in[there, 384:512] = r.w_value[here, :]
            r.w_back[there, :] = r.w_out[here, :]
    pl.semaphore_wait(pltpu.get_barrier_semaphore(), 22)

    ref_gather = Gather(r.ref_gathered, SHARD, send.gather_ref, recv.gather_ref)
    pol_gather = Gather(r.pol_gathered, SHARD, send.gather_pol, recv.gather_pol)
    weights = Weights(r.w_in, r.w_back, send.y, recv.y, send.d, recv.d)

    def weight_steps():
        for s in range(1, 3):
            weights.step(s, (0,))
            yield
            weights.step(s, (1,))
            if s == 1:
                weights.step(s, (2,))
            yield
        weights.step(2, (2,))
        weights.step(0, (3, 4))
        yield
        for part in range(3):
            weights.step(3, (part,))
            yield
        for s in range(1, 4):
            weights.step(s, (3, 4))
            yield

    pre_stats.start()
    ref_gather.begin()
    weights.step(0, (0, 1, 2))
    for number in range(10, len(inputs)):
        load(number).wait()
    gain = r.pre_ordered
    order_gain(r.pre_gain, gain)
    order_gain(r.post_gain, r.post_ordered)
    pre_gain, post_gain = own_gain(gain, mine), own_gain(r.post_ordered, mine)
    def project(m):
        rows = slice(m * TOK, m * TOK + TOK)
        for i in range(3):
            total = None
            for c in range(3 * i, 3 * i + 3):
                term = dot(r.normed[rows, 512 * c : 512 * c + 512], r.w_in[512 * c : 512 * c + 512, :])
                total = term if total is None else total + term
            r.acc[rows, :] = total if i == 0 else r.acc[rows, :] + total
            yield

    def attend(m):
        for i in range(3):
            at = slice(m * TOK + 96 * i, m * TOK + 96 * i + 96)
            cos, sin = r.cosine[...], r.sine[...]
            key = rope(r.acc[at, 256:384], cos, sin).astype(BF16)
            value = r.acc[at, 384:512].astype(BF16)
            allowed = allowed_here(r.lengths[i])
            r.heads[at, 256:384] = key
            r.heads[at, 384:512] = value
            for g in range(2):
                query = rope(r.acc[at, 128 * g : 128 * g + 128], cos, sin).astype(BF16)
                r.heads[at, 128 * g : 128 * g + 128] = query
                scores = dot(query, key, NT) * QUERY_SCALE
                cap = SOFT_CAP * jnp.tanh(scores / SOFT_CAP)
                weight = jnp.where(allowed, jnp.exp(cap), 0.0)
                prob = weight / jnp.sum(weight, axis=1, keepdims=True)
                r.probs[at, 128 * g : 128 * g + 96] = prob
                r.capped[at, 128 * g : 128 * g + 96] = cap
                r.mixed[at, 128 * g : 128 * g + 128] = dot(prob.astype(BF16), value).astype(BF16)
            yield

    def fill(steps, count):
        for _ in range(count):
            next(steps, None)

    def ref_work():
        unpack_features(r.ref_gathered, SHARD, 0, r.normed, 0)
        yield
        normalize(r.normed, r.scale, gain, 0)
        yield
        weights.arrive(0)
        yield from project(0)
        yield from attend(0)

    lows = HookSum(
        r.low_terms, r.low_parts, r.low, mine, send.low_terms, recv.low_terms, send.low, recv.low, r.hook_parts
    )

    def low_work():
        send_a()
        pre_stats.wait()
        rows_to_columns(r.table, [lax.rsqrt(as_row(pre_stats.total()) / WIDTH + NORM_EPS)])
        own = r.pol_hidden[...].astype(F32) * r.table[0:TOK, 0:1] * pre_gain
        r.own_normed[...] = own.astype(BF16)
        yield
        relay_a()
        yield
        await_a()
        r.low_terms[...] = dot(r.own_normed[...], r.a_own[...]).astype(BF16)
        lows.start()
        yield
        lows.reduce()
        yield

    low = low_work()
    first, second, passing, work = ref_gather.steps(), pol_gather.steps(), weight_steps(), ref_work()
    arrivals = dict(G=first, Q=second, V=passing, C=work, X=low)
    for letter in "GGGVPGGGVQGVQGVXQGVQGVXQGQGVXQVGQGVQGCQVCQCQCCQCQXCQCV":
        if letter == "P":
            pol_gather.begin()
        else:
            fill(arrivals[letter], 1)
    weights.arrive(3)
    for _ in partial_products(r.mixed.at[0:TOK], r.w_back, r.partial):
        pass
    ref_scatter = ShortScatter(r.partial, r.landing, SHARD, send.scatter_ref, recv.scatter_ref)
    ref_scatter.begin()
    pol_scatter = ShortScatter(r.partial_pol, r.landing_pol, SHARD, send.scatter_pol, recv.scatter_pol)

    def policy():
        unpack_features(r.pol_gathered, SHARD, 0, r.normed, TOK)
        yield
        normalize(r.normed, r.scale, gain, TOK)
        yield
        yield from project(1)
        r.linear[...] = r.acc[TOK : 2 * TOK, :]
        lows.wait()
        query_factor = jnp.concatenate([r.b_query[...], jnp.zeros((RANK, 256), BF16)], axis=0)
        value_factor = jnp.concatenate([jnp.zeros((RANK, 128), BF16), r.b_value[...]], axis=0)
        r.acc[TOK : 2 * TOK, 0:256] += ADAPTER_SCALE * dot(r.low[...], query_factor)
        r.acc[TOK : 2 * TOK, 384:512] += ADAPTER_SCALE * dot(r.low[...], value_factor)
        yield
        yield from attend(1)
        yield from partial_products(r.mixed.at[TOK : 2 * TOK], r.w_back, r.partial_pol)

    def token_sums(m, hidden):
        unpack_result(r.result.at[m], 0, r.summed.at[m])
        summed, readout = r.summed[m], r.readout[...].astype(F32)
        return [
            jnp.sum(summed * summed, axis=1, keepdims=True),
            jnp.sum(summed * post_gain * readout, axis=1, keepdims=True),
            jnp.sum(hidden[...].astype(F32) * readout, axis=1, keepdims=True),
        ]

    ref_stats = Exchange(r.ref_stats, 8, 16, mine, in_tensor, send.ref_stats, recv.ref_stats)
    pol_stats = Exchange(r.pol_stats, 16, 16, mine, in_tensor, send.pol_stats, recv.pol_stats)

    def policy_ring():
        yield from pol_scatter.steps(r.result.at[1])

    def after_ref():
        columns = columns_to_rows(r.table, token_sums(0, r.ref_hidden))
        r.ref_stats[pl.ds(aligned(8 * mine, 8), 8), :] = columns
        ref_stats.start()
        yield

    ref_ring, policy_work, policy_steps = ref_scatter.steps(r.result.at[0]), policy(), policy_ring()
    fill(policy_work, 3)
    for count in (2, 2, 2, 2, 2):
        fill(ref_ring, 1)
        fill(policy_work, count)
    for _ in policy_work:
        pass
    pol_scatter.begin((0,))
    fill(ref_ring, 1)
    pol_scatter.begin((1,))
    fill(ref_ring, 1)
    pol_scatter.begin((2, 3))
    for count in (2, 2):
        fill(ref_ring, 1)
        fill(policy_steps, count)
    together(policy_steps, after_ref(), (1,) + (0,) * 8)
    columns = columns_to_rows(r.table, token_sums(1, r.pol_hidden))
    packed = [columns[k : k + 1, 128 * c : 128 * c + 128] for k in range(3) for c in range(3)]
    packed = jnp.concatenate(packed + [jnp.zeros((7, 128), F32)], axis=0)
    r.pol_stats[pl.ds(aligned(16 * mine, 8), 16), :] = packed
    pol_stats.start()
    pol_stats.wait()
    packed = pol_stats.total()
    pol_total = [
        jnp.concatenate([packed[3 * k + c : 3 * k + c + 1] for c in range(3)], axis=1) for k in range(3)
    ]
    scale_pol = lax.rsqrt(pol_total[0] / WIDTH + NORM_EPS)
    rows_to_columns(r.table, [scale_pol, scale_pol * scale_pol * scale_pol * pol_total[1] / WIDTH])
    readout = r.readout[...].astype(F32)
    bare = r.table[0:TOK, 0:1] * post_gain * readout - r.summed[1] * r.table[0:TOK, 1:2]
    pack_hidden(bare, r.grad_buf, mine * SHARD)
    back_gather = ShortGather(r.grad_buf, SHARD, send.gather_back, recv.gather_back)
    back_gather.begin()

    lane = lax.broadcasted_iota(jnp.int32, (1, 384), 1)
    lengths = [r.lengths[s] for s in range(3)]
    living = jnp.zeros((1, 384), F32)
    for s in range(3):
        living = jnp.where((lane >= 96 * s) & (lane < 96 * s + lengths[s]), 1.0, living)
    ref_stats.wait()
    ref_total = ref_stats.total()
    scale_ref = lax.rsqrt(ref_total[0:1] / WIDTH + NORM_EPS)
    token_scores = (
        (ref_total[2:3] + scale_ref * ref_total[1:2]) * living,
        (pol_total[2] + scale_pol * pol_total[1]) * living,
    )
    row8 = lax.broadcasted_iota(jnp.int32, (8, 128), 0)
    lane8 = lax.broadcasted_iota(jnp.int32, (8, 128), 1)
    tile = jnp.zeros((8, 128), F32)
    for m in range(2):
        for s in range(3):
            inside = (lane >= 96 * s) & (lane < 96 * s + 96)
            score = jnp.sum(jnp.where(inside, token_scores[m], 0.0), axis=1, keepdims=True)
            tile = jnp.where((row8 == m) & (lane8 == 3 * rank + s), score, tile)
    scores = Exchange(r.scores, 8, 8, rank, in_data, send.scores, recv.scores)
    r.scores[pl.ds(aligned(8 * rank, 8), 8), :] = tile
    scores.start()

    def layer_outputs():
        rows_to_columns(r.coefficient, [scale_ref, scale_pol])
        for m, (hidden, out) in enumerate(((r.ref_hidden, r.ref_out), (r.pol_hidden, r.pol_out))):
            scale = r.coefficient[0:TOK, m : m + 1]
            out[...] = (hidden[...].astype(F32) + r.summed[m] * scale * post_gain).astype(BF16)
            yield
            store(1 - m).start()

    def preference():
        scores.wait()
        everyone = scores.total()
        ratio = everyone[1:2] - everyone[0:1]
        row32 = lax.broadcasted_iota(jnp.int32, (32, 128), 0)
        lane32 = lax.broadcasted_iota(jnp.int32, (32, 128), 1)
        named = jnp.full((32, 128), -1, jnp.int32)
        for k in range(24):
            named = jnp.where(row32 == k, r.pairing[k], named)
        chosen = named == lane32
        even = lax.rem(row32, 2) == 0
        picked = jnp.sum(jnp.where(chosen, ratio, 0.0), axis=1, keepdims=True)
        picked = jnp.broadcast_to(picked, (32, 128))
        other = jnp.where(even, pltpu.roll(picked, 31, 0), pltpu.roll(picked, 1, 0))
        margin = DPO_BETA * jnp.where(even, picked - other, other - picked)
        loss = jnp.maximum(-margin, 0.0) + jnp.log1p(jnp.exp(-jnp.abs(margin)))
        counted = even & (row32 < 24) & (lane32 == 0)
        total_loss = jnp.sum(jnp.where(counted, loss, 0.0), axis=(0, 1), keepdims=True)
        r.loss[...] = jnp.broadcast_to(total_loss, (8, 128))
        store(2).start()
        pull = DPO_BETA * LOSS_SCALE / (1.0 + jnp.exp(margin))
        signed = jnp.where(even, -pull, pull)
        coefficients = jnp.sum(jnp.where(chosen, signed, 0.0), axis=0, keepdims=True)
        lane128 = lax.broadcasted_iota(jnp.int32, (1, 128), 1)
        coefficient = jnp.zeros((1, 384), F32)
        for s in range(3):
            own = jnp.sum(jnp.where(lane128 == 3 * rank + s, coefficients, 0.0), axis=1, keepdims=True)
            coefficient = jnp.where((lane >= 96 * s) & (lane < 96 * s + 96), own, coefficient)
        rows_to_columns(r.coefficient, [coefficient * living])
        yield

    def meanwhile():
        yield from layer_outputs()
        yield from preference()

    together(back_gather.steps(), meanwhile(), (1, 1, 0, 0, 0, 0, 0, 1, 0, 0, 0, 0, 0, 0, 0))
    unpack_features(r.grad_buf, SHARD, 0, r.normed, 0)

    for i in range(3):
        total = None
        for c in range(3 * i, 3 * i + 3):
            term = dot(r.normed[0:TOK, 512 * c : 512 * c + 512], r.w_back[512 * c : 512 * c + 512, :])
            total = term if total is None else total + term
        r.grad_mixed[...] = total if i == 0 else r.grad_mixed[...] + total
    r.grad_mixed[...] *= r.coefficient[0:TOK, 0:1]

    for i in range(3):
        here = slice(96 * i, 96 * i + 96)
        at = slice(TOK + 96 * i, TOK + 96 * i + 96)
        cos, sin = r.cosine[...], r.sine[...]
        key, value = r.heads[at, 256:384], r.heads[at, 384:512]
        key_grad = jnp.zeros((96, HEAD), F32)
        value_grad = jnp.zeros((96, HEAD), F32)
        for g in range(2):
            query = r.heads[at, 128 * g : 128 * g + 128]
            incoming = r.grad_mixed[here, 128 * g : 128 * g + 128].astype(BF16)
            prob = r.probs[at, 128 * g : 128 * g + 96]
            cap = r.capped[at, 128 * g : 128 * g + 96] / SOFT_CAP
            grad_probs = dot(incoming, value, NT)
            value_grad = value_grad + dot(prob.astype(BF16), incoming, TN)
            centered = grad_probs - jnp.sum(grad_probs * prob, axis=1, keepdims=True)
            grad_scores = (prob * centered * (1.0 - cap * cap) * QUERY_SCALE).astype(BF16)
            query_grad = dot(grad_scores, key)
            key_grad = key_grad + dot(grad_scores, query, TN)
            r.grads[here, 128 * g : 128 * g + 128] = rope(query_grad, cos, -sin).astype(BF16)
        r.grads[here, 256:384] = rope(key_grad, cos, -sin).astype(BF16)
        r.grads[here, 384:512] = value_grad.astype(BF16)

    query_factor = jnp.concatenate([r.b_query[...], jnp.zeros((RANK, 256), BF16)], axis=0)
    value_factor = jnp.concatenate([jnp.zeros((RANK, 128), BF16), r.b_value[...]], axis=0)
    hook = dot(r.grads[:, 0:256], query_factor, NT) + dot(r.grads[:, 384:512], value_factor, NT)
    r.hooks[...] = (ADAPTER_SCALE * hook).astype(BF16)
    hooks = HookSum(
        r.hooks,
        r.hook_parts,
        r.hook_sums,
        mine,
        send.hooks,
        recv.hooks,
        send.hook_sums,
        recv.hook_sums,
        r.hook_parts,
    )
    hooks.start()
    stats_back = Exchange(r.stats_back, 8, 16, mine, in_tensor, send.stats_back, recv.stats_back)
    factors = Exchange(r.factors, 64, 8, rank, in_data, send.factors, recv.factors)
    for _ in partial_products(r.grads, r.w_in, r.partial_back):
        pass
    back_scatter = ShortScatter(
        r.partial_back, r.landing_back, SHARD, send.scatter_back, recv.scatter_back
    )
    back_scatter.begin((0, 1))

    def across(i):
        return pltpu.make_async_remote_copy(
            src_ref=r.a_terms.at[pl.ds(aligned(576 * (2 * i + 1 - core), 64), 576), :],
            dst_ref=r.a_across.at[pl.ds(576 * i, 576), :],
            send_sem=send.across.at[i],
            recv_sem=recv.across.at[i],
            device_id={CORE: 1 - core},
            device_id_type=MESH,
        )

    def round_y(source, target, to):
        return pltpu.make_async_remote_copy(
            src_ref=source,
            dst_ref=target,
            send_sem=send.round.at[0],
            recv_sem=recv.round.at[0],
            device_id={Y: to},
            device_id_type=MESH,
        )

    three = r.a_round.at[pl.ds(0, 3 * 576), :]
    rounds = round_y(three, three, lax.rem(y + 1, 4))

    def pair_up(i):
        across(i).wait_recv()
        rows = slice(576 * i, 576 * i + 576)
        own = r.a_terms[pl.ds(aligned(576 * (2 * i + core), 64), 576), :].astype(F32)
        r.a_pairs[rows, :] = (own + r.a_across[rows, :].astype(F32)).astype(BF16)

        @pl.when(y != i)
        def _():
            place = pl.ds(aligned(576 * lax.rem(i - y + 4, 4), 64), 576)
            round_y(r.a_pairs.at[pl.ds(576 * i, 576), :], r.a_round.at[place, :], i).start()

    def adapters_back():
        pull_back = jnp.sum(r.grads[...].astype(F32) * r.linear[...], axis=1, keepdims=True)
        pull_back += jnp.sum(r.hooks[...].astype(F32) * r.low[...].astype(F32), axis=1, keepdims=True)
        row = columns_to_rows(r.table, [pull_back])[0:1]
        r.stats_back[pl.ds(aligned(8 * mine, 8), 8), :] = as_tile(row)
        stats_back.start()
        factor_terms = ADAPTER_SCALE * dot(r.low[...], r.grads[:, 0:512], TN)
        own_factor = pl.ds(aligned(64 * rank, 64), 64)
        r.factors[own_factor, 0:256] = factor_terms[0:64, 0:256].astype(BF16)
        r.factors[own_factor, 256:384] = factor_terms[64:128, 384:512].astype(BF16)
        factors.start()
        yield
        hooks.wait()
        hook_low = r.hook_sums[...]
        r.summed[0] = dot(hook_low, r.a_own[...], NT)
        for q in range(4):
            at = MAIN + 128 * q
            tail = dot(r.normed[TOK : 2 * TOK, at : at + 128], hook_low, TN).astype(BF16)
            for t in range(4 * q, 4 * q + 4):
                term = dot(r.normed[TOK : 2 * TOK, 256 * t : 256 * t + 256], hook_low, TN)
                r.a_terms[288 * t : 288 * t + 256, :] = term.astype(BF16)
                j = t - 4 * q
                r.a_terms[288 * t + 256 : 288 * t + 288, :] = tail[32 * j : 32 * j + 32, :]
            across(q).start()
            if q:
                pair_up(q - 1)
            yield
        pair_up(3)
        yield

    adapters = adapters_back()
    fill(adapters, 1)
    back_scatter.begin((2,))
    hooks.reduce()
    back_scatter.begin((3,))
    together(back_scatter.steps(r.result.at[0]), adapters, (0, 0, 0, 2, 2, 1, 0, 0, 0))

    stats_back.wait()
    rows_to_columns(r.table, [as_row(stats_back.total())])
    unpack_result(r.result.at[0], 0, r.summed.at[1])
    pre_scale = r.scale[TOK : 2 * TOK, 0:1]
    shrink_back = pre_scale * pre_scale * r.table[0:TOK, 0:1] / WIDTH
    grad_result = r.coefficient[0:TOK, 0:1] * r.readout[...].astype(F32)
    hidden = r.pol_hidden[...].astype(F32)
    r.grad_hidden[...] = (
        grad_result + pre_scale * pre_gain * (r.summed[1] + r.summed[0]) - hidden * shrink_back
    ).astype(BF16)
    store(3).start()
    factors.wait()
    factor_total = factors.total()
    r.query_grad[...] = factor_total[:, 0:256]
    r.value_grad[...] = factor_total[:, 256:384]
    store(5).start()
    store(6).start()
    whole = r.a_pairs[pl.ds(aligned(576 * y, 64), 576), :].astype(F32)
    rounds.wait_recv()
    for i in range(1, 4):
        whole = whole + r.a_round[576 * i : 576 * i + 576, :].astype(F32)
    r.grad_a[...] = whole
    store(4).start()
    drain_a()
    for ring in (ref_gather, pol_gather, weights, ref_scatter, pol_scatter, back_gather, back_scatter):
        ring.drain()
    for exchange in (pre_stats, ref_stats, pol_stats, scores, lows, hooks, stats_back, factors):
        exchange.drain()
    for i in range(4):
        across(i).wait_send()
    rounds.wait_send()
    for number in range(len(outputs)):
        store(number).wait()


def partial_products(rows, matrix, partial):
    for block in range(4):
        left = rows[...]
        for t in range(4 * block, 4 * block + 4):
            product = dot(left, matrix[256 * t : 256 * t + 256, :], NT).astype(BF16)
            for half in range(2):
                at = t * SHARD + TOK * half
                partial[at : at + TOK, :] = product[:, 128 * half : 128 * half + 128]
        at = MAIN + 128 * block
        product = dot(left, matrix[at : at + 128, :], NT).astype(BF16)
        for j in range(4):
            at = (4 * block + j) * SHARD + 2 * TOK
            partial[at : at + GROUP, :] = pack_tail(product[:, 32 * j : 32 * j + 32])
        yield


def rotation_tables():
    spacing = ROPE_BASE ** (-2.0 * np.arange(64, dtype=np.float32) / HEAD)
    angles = np.arange(LENGTH, dtype=np.float32)[:, None] * spacing.astype(np.float32)[None, :]
    cosine, sine = np.cos(angles), np.sin(angles)
    return (
        np.concatenate([cosine, cosine], axis=1).astype(np.float32),
        np.concatenate([-sine, sine], axis=1).astype(np.float32),
    )


INPUTS = dict(
    lengths=None,
    pairing=None,
    ref_hidden=((TOK, TOK), BF16),
    pol_hidden=((TOK, TOK), BF16),
    w_query=((576, 256), BF16),
    w_key=((576, 128), BF16),
    w_value=((576, 128), BF16),
    w_out=((576, 256), BF16),
    a_query=((RANK, 576), BF16),
    a_value=((RANK, 576), BF16),
    readout=((TOK, TOK), BF16),
    b_query=((RANK, 256), BF16),
    b_value=((RANK, 128), BF16),
    pre_gain=((36, 128), F32),
    post_gain=((36, 128), F32),
    cosine=((LENGTH, HEAD), F32),
    sine=((LENGTH, HEAD), F32),
)
OUTPUTS = dict(
    pol_out=((TOK, TOK), BF16),
    ref_out=((TOK, TOK), BF16),
    loss=((8, 128), F32),
    grad_hidden=((TOK, TOK), BF16),
    grad_a=((576, 128), F32),
    query_grad=((RANK, 256), F32),
    value_grad=((RANK, 128), F32),
)


def hand_out(*refs):
    for source, target in zip(refs[: len(OUTPUTS)], refs[len(OUTPUTS) :]):
        target[...] = source[0 : target.shape[0], 0 : target.shape[1]]


def body(
    ref_hidden,
    pol_hidden,
    readout,
    lengths,
    pairing,
    pre_gain,
    post_gain,
    w_query,
    w_key,
    value_projection,
    w_out,
    a_query,
    a_value,
    query_second_factor,
    value_second_factor,
):
    vmem, whole = pl.BlockSpec(memory_space=pltpu.VMEM), pl.BlockSpec(memory_space=pl.ANY)
    cosine, sine = rotation_tables()
    dma = pltpu.SemaphoreType.DMA
    staged = [pltpu.VMEM(*kind) if kind else None for kind in list(INPUTS.values()) + list(OUTPUTS.values())]
    staged[0:2] = [pltpu.SMEM((3,), jnp.int32), pltpu.SMEM((24,), jnp.int32)]
    results = pl.pallas_call(
        step_body,
        out_shape=tuple(jax.ShapeDtypeStruct(*kind) for kind in OUTPUTS.values()),
        in_specs=[whole] * len(INPUTS),
        out_specs=(whole,) * len(OUTPUTS),
        scratch_shapes=staged
        + [pltpu.VMEM(shape, kind) for shape, kind in SCRATCH.values()]
        + [dma((len(INPUTS),)), dma((len(OUTPUTS),))]
        + [dma((count,)) for pair in SEMAPHORES.values() for count in pair],
        compiler_params=pltpu.CompilerParams(
            collective_id=0, has_side_effects=True, vmem_limit_bytes=62 * 1024 * 1024
        ),
    )(
        lengths,
        pairing,
        ref_hidden,
        pol_hidden,
        w_query,
        w_key,
        value_projection,
        w_out,
        a_query.T,
        a_value.T,
        readout,
        query_second_factor,
        value_second_factor,
        pre_gain.reshape(36, 128),
        post_gain.reshape(36, 128),
        jnp.asarray(cosine),
        jnp.asarray(sine),
    )
    shapes = [jax.ShapeDtypeStruct(a.shape, a.dtype) for a in results]
    shapes[2] = jax.ShapeDtypeStruct((1, 1), F32)
    pol_out, ref_out, loss, grad_hidden, grad_a, query_grad, value_grad = pl.pallas_call(
        hand_out,
        out_shape=tuple(shapes),
        in_specs=[vmem] * len(OUTPUTS),
        out_specs=(vmem,) * len(OUTPUTS),
    )(*results)
    return (pol_out, ref_out, loss.reshape(()), grad_hidden, grad_a, query_grad, value_grad)


def solution(mesh):
    torus = Mesh(mesh.devices.reshape(4, 2, 4, 4), (Y, CORE, X, Z))
    split, rows, columns = P(DP, TENSOR), P(DP, None), P(None, TENSOR)
    return jax.shard_map(
        body,
        mesh=torus,
        in_specs=(split, split, split, P(DP), P(), P(), P(), split, split, split, split, rows, rows, columns, columns),
        out_specs=(split, split, P(), split, rows, columns, columns),
        check_vma=False,
    )
```
